32 devices in a mesh: group: 4 (over z), blk: 8 (over y, x, core).
Axes of the slice: x: 2, y: 2, z: 4, core: 2. Of those that a mesh axis runs over, the one named last changes fastest.
Arguments:
- image_a: float32 [3, 1024, 2048], P(None, 'group', 'blk'), may hold values from -6 to 6
- image_b: float32 [3, 1024, 2048], P(None, 'group', 'blk'), may hold values from -6 to 6
- initial: float32 [3, 1024, 2048], P(None, 'group', 'blk'), may hold values from -6 to 6
- coverage: int32 [4, 8], P('group', 'blk'), may hold values 0 or 1
- seam_label: int32 [4, 8], P('group', 'blk'), may hold values from 0 to 1
Outputs:
- blended: float32 [3, 1024, 2048], P(None, 'group', 'blk')
The draws below stay inside these ranges and needn't reach their ends.
All inputs are finite; a program needn't handle non-finite values. No bound on the sum of `coverage` on one device may be relied on, other than what follows from the above.
Results may differ from the reference program's by a relative error of at most 0.00003.
Values sent between devices are 32-bit elements; how exact they have to be, the bound alone decides.
No kernel may reach another device: no remote copies, remote signals or barrier semaphores. Data moves between devices by JAX's collectives and lax.ppermute only.
A program may use at most 128 MiB of HBM per device.

```python
import jax
import jax.numpy as jnp

CHAN = 3
BS = 256
LEVELS = 4
NU = 2
COARSE = 4
NY = 1024
NX = 2048


def place_ends(result, rng, least, high):
    longest = result.shape.index(max(result.shape))
    spots = []
    for shift in (0, 1):
        where = [jax.random.randint(jax.random.fold_in(rng, axis), (), 0, length) for axis, length in enumerate(result.shape)]
        where[longest] = (where[longest] + shift) % result.shape[longest]
        spots.append(tuple(where))
    return result.at[spots[0]].set(least).at[spots[1]].set(high)


def shard_levels(key, dims, cuts, smallest, largest):
    loudness = 1.0
    for dim, shards_of in cuts:
        draws = jax.random.uniform(jax.random.fold_in(jax.random.fold_in(key, 6), dim), (shards_of,), jnp.float32, smallest / len(cuts), largest / len(cuts))
        loudness = loudness * jnp.repeat(jnp.exp(draws), dims[dim] // shards_of).reshape((-1,) + (1,) * (len(dims) - 1 - dim))
    return loudness


def bell_draw(own_key, dims, spread, bound, split=(), held_as=jnp.bfloat16):
    level = shard_levels(own_key, dims, split, -0.22, 0.18) if split else 1.0
    array = jax.random.normal(own_key, dims, jnp.float32) * spread * level
    return jnp.minimum(jnp.maximum(array, -bound), bound).astype(held_as)


def setup_inputs(seed: int = 0) -> dict:
    streams_of = jax.random.split(jax.random.key(seed), 6)
    return {
        "image_a": bell_draw(streams_of[0], (CHAN, NY, NX), 1.0, 6.0, ((1, 4), (2, 8)), jnp.float32),
        "image_b": bell_draw(streams_of[1], (CHAN, NY, NX), 1.0, 6.0, ((1, 4), (2, 8)), jnp.float32),
        "initial": bell_draw(streams_of[2], (CHAN, NY, NX), 1.0, 6.0, ((1, 4), (2, 8)), jnp.float32),
        "coverage": place_ends((jax.random.randint(streams_of[3], (NY // BS, NX // BS), 0, 4) < 3).astype(jnp.int32), jax.random.fold_in(streams_of[3], 1), 0, 1),
        "seam_label": place_ends(jax.random.randint(streams_of[4], (NY // BS, NX // BS), 0, 2), jax.random.fold_in(streams_of[4], 1), 0, 1).astype(jnp.int32),
    }


RELAX = 0.8


def beside_sum(padded):
    return padded[:, :-2, 1:-1] + padded[:, 2:, 1:-1] + padded[:, 1:-1, :-2] + padded[:, 1:-1, 2:]


def zero_rim(field):
    return jnp.pad(field, ((0, 0), (1, 1), (1, 1)))


def cell_map(table, span):
    return jnp.repeat(jnp.repeat(table, span, 0), span, 1)


def smooth(approx, source, active, depth_index, sweeps):
    factor = 0.25 ** depth_index
    for sweep in range(sweeps):
        approx = approx + RELAX * active * (source - factor * (4.0 * approx - beside_sum(zero_rim(approx)))) / (4.0 * factor)
    return approx


def shrink(field):
    chans, rows, cols = field.shape
    return field.reshape(chans, rows // 2, 2, cols // 2, 2).mean(axis=(2, 4))


def expand(field):
    return jnp.repeat(jnp.repeat(field, 2, 1), 2, 2)


def vcycle(source, depth_index, actives):
    active = actives[depth_index]
    zeros = jnp.zeros(source.shape, jnp.float32)
    if depth_index == LEVELS - 1:
        return smooth(zeros, source, active, depth_index, COARSE)
    approx = smooth(zeros, source, active, depth_index, NU)
    factor = 0.25 ** depth_index
    leftover = active * (source - factor * (4.0 * approx - beside_sum(zero_rim(approx))))
    coarse_fix = vcycle(shrink(leftover), depth_index + 1, actives)
    approx = approx + active * expand(coarse_fix)
    return smooth(approx, source, active, depth_index, NU)


def reference(image_a, image_b, initial, coverage, seam_label):
    actives = [cell_map(coverage, BS >> depth_index).astype(jnp.float32)[None] for depth_index in range(LEVELS)]
    laplace_a = 4.0 * image_a - beside_sum(zero_rim(image_a))
    laplace_b = 4.0 * image_b - beside_sum(zero_rim(image_b))
    laplace_x = 4.0 * initial - beside_sum(zero_rim(initial))
    labels = cell_map(seam_label, BS)[None]
    guide = jnp.where(labels == 1, laplace_b, laplace_a)
    source = actives[0] * (guide - laplace_x)
    return initial + vcycle(source, 0, actives)
```

```python
import functools

import jax
import jax.numpy as jnp
from jax import lax
from jax.experimental import pallas as pl
from jax.experimental.pallas import tpu as pltpu
from jax.sharding import PartitionSpec as P

LEVELS = 4
NU = 2
COARSE = 4
RELAX = 0.8

LANES = 128
HALO = 64
SPREAD = 18


def source_reach():
    need = 0
    for _ in range(LEVELS - 1):
        need = -(-(need + NU) // 2)
    need += COARSE - 1
    for _ in range(LEVELS - 1):
        need = 2 * need + NU
    return need


REACH = source_reach()
STRIP = REACH + 2
assert STRIP % 8 == 0 and STRIP <= HALO
A_LEFT, B_LEFT, ACT_LEFT, LAB_LEFT = 60, 61, 62, 63
A_RIGHT, B_RIGHT, ACT_RIGHT, LAB_RIGHT = 64, 65, 66, 67


def lane_ids(rows):
    return lax.broadcasted_iota(jnp.int32, (rows, LANES), 1)


def roll(tile, shift):
    return pltpu.roll(tile, shift % LANES, 1)


def spread_cell(tile, lane):
    return jnp.broadcast_to(tile[:, lane : lane + 1], tile.shape)


def prepare(a_ref, b_ref, x_ref, cover_ref, label_ref, source_ref, column_ref, even_ref, odd_ref, da, db):
    chans, rows, cols = a_ref.shape
    tiles = cols // LANES
    active = cover_ref[0, 0].astype(jnp.float32)
    marked = label_ref[0, 0].astype(jnp.float32)
    second = label_ref[0, 0] == 1
    on_even = lax.rem(lax.axis_index("group"), 2) == 0
    zero_row = jnp.zeros((8, LANES), jnp.float32)
    step = 32
    ids = lane_ids(step)
    for k in range(tiles):
        for buf in (da, db):
            buf[k, 0:8, :] = zero_row
            buf[k, rows + 8 : rows + 16, :] = zero_row

    def flags(n):
        out = jnp.where((ids[:n] == ACT_LEFT) | (ids[:n] == ACT_RIGHT), active, 0.0)
        return jnp.where((ids[:n] == LAB_LEFT) | (ids[:n] == LAB_RIGHT), marked, out)

    flag_lanes = flags(step)

    def channel(c, _):
        for k in range(tiles):
            at = pl.ds(k * LANES, LANES)
            for r in range(0, rows, step):
                x = x_ref[c, r : r + step, at]
                da[k, 8 + r : 8 + r + step, :] = a_ref[c, r : r + step, at] - x
                db[k, 8 + r : 8 + r + step, :] = b_ref[c, r : r + step, at] - x

        def pick(k, low, n):
            return jnp.where(second, db[k, low : low + n, :], da[k, low : low + n, :])

        for r in range(0, rows, step):
            mids = [pick(k, 8 + r, step) for k in range(tiles)]
            rights = [roll(t, 1) for t in mids]
            lefts = [roll(t, -1) for t in mids]
            found = []
            for k in range(tiles):
                below = jnp.where(ids == 0, rights[k - 1] if k else 0.0, rights[k])
                above = jnp.where(ids == LANES - 1, lefts[k + 1] if k + 1 < tiles else 0.0, lefts[k])
                beside = pick(k, 7 + r, step) + pick(k, 9 + r, step) + below + above
                found.append(active * (RELAX * mids[k] - 0.25 * RELAX * beside))
                source_ref[c, k, HALO + r : HALO + r + step, :] = found[k]
            first_a, first_b = da[0, 8 + r : 8 + r + step, :], db[0, 8 + r : 8 + r + step, :]
            last_a, last_b = da[tiles - 1, 8 + r : 8 + r + step, :], db[tiles - 1, 8 + r : 8 + r + step, :]
            cells = flag_lanes
            cells = jnp.where(ids == A_LEFT, spread_cell(first_a, 0), cells)
            cells = jnp.where(ids == B_LEFT, spread_cell(first_b, 0), cells)
            cells = jnp.where(ids == A_RIGHT, spread_cell(last_a, LANES - 1), cells)
            cells = jnp.where(ids == B_RIGHT, spread_cell(last_b, LANES - 1), cells)
            cells = jnp.where(ids < REACH, found[0], cells)
            cells = jnp.where(ids >= LANES - REACH, found[tiles - 1], cells)
            column_ref[c, HALO + r : HALO + r + step, :] = cells
        return 0

    lax.fori_loop(0, chans, channel, 0)

    def message(out, top):
        low = HALO if top else HALO + rows - STRIP
        line = 8 if top else 8 + rows - 1
        spot = STRIP - 2 if top else 0
        packed = zero_row
        eight = ids[:8]
        for t in range(STRIP // 8):
            for c in range(chans):
                lane = SPREAD * t + 6 * c
                moved = roll(column_ref[c, low + 8 * t : low + 8 * t + 8, :], lane - A_LEFT)
                packed = jnp.where((eight >= lane) & (eight < lane + 6), moved, packed)
        out[0, chans * STRIP :, :] = packed
        marks = jnp.where(eight < LANES // 2, active, marked)
        for k in range(1, tiles):
            out[k, chans * STRIP :, :] = marks
        for c in range(chans):
            for k in range(tiles):
                out[k, c * STRIP : (c + 1) * STRIP, :] = source_ref[c, k, low : low + STRIP, :]
                at = pl.ds(k * LANES, LANES)
                row = line - 8
                x = x_ref[c, row : row + 1, at]
                out[k, c * STRIP + spot : c * STRIP + spot + 1, :] = a_ref[c, row : row + 1, at] - x
                out[k, c * STRIP + spot + 1 : c * STRIP + spot + 2, :] = b_ref[c, row : row + 1, at] - x

    @pl.when(on_even)
    def _():
        message(even_ref, False)
        message(odd_ref, True)

    @pl.when(jnp.logical_not(on_even))
    def _():
        message(even_ref, True)
        message(odd_ref, False)


def join_rows(source_in, column_in, sent_even, sent_odd, got_even, got_odd, source_ref, column_ref, even_ref, odd_ref):
    chans, tiles, height, _ = source_ref.shape
    rows = height - 2 * HALO
    tail = chans * STRIP
    row_even = lax.rem(lax.axis_index("group"), 2) == 0
    col_even = lax.rem(lax.axis_index("blk"), 2) == 0
    ids = lane_ids(STRIP)
    one = lane_ids(1)

    def cells_of(c, low, n):
        left, right = source_ref[c, 0, low : low + n, :], source_ref[c, tiles - 1, low : low + n, :]
        return left, right

    def side(top, got, mine):
        low = HALO - STRIP if top else HALO + rows
        their_spot = 0 if top else STRIP - 2
        my_spot = STRIP - 2 if top else 0
        edge = HALO if top else HALO + rows - 1
        other = edge - 1 if top else edge + 1
        packed = got[0, tail:, :]
        marks = got[1, tail:, :]
        their_active, their_mark = spread_cell(marks, 0), spread_cell(marks, LANES // 2)
        own_row = column_ref[0, HALO : HALO + 8, :]
        my_active, my_mark = spread_cell(own_row, ACT_LEFT), spread_cell(own_row, LAB_LEFT)
        eight = ids[:8]
        flags = jnp.where((eight == ACT_LEFT) | (eight == ACT_RIGHT), their_active, their_mark)
        for c in range(chans):
            for k in range(tiles):
                source_ref[c, k, low : low + STRIP, :] = got[k, c * STRIP : (c + 1) * STRIP, :]
                their_a = got[k, c * STRIP + their_spot : c * STRIP + their_spot + 1, :]
                their_b = got[k, c * STRIP + their_spot + 1 : c * STRIP + their_spot + 2, :]
                my_a = mine[k, c * STRIP + my_spot : c * STRIP + my_spot + 1, :]
                my_b = mine[k, c * STRIP + my_spot + 1 : c * STRIP + my_spot + 2, :]
                for_mine = 0.25 * RELAX * my_active[:1] * jnp.where(my_mark[:1] == 1.0, their_b, their_a)
                for_theirs = 0.25 * RELAX * their_active[:1] * jnp.where(their_mark[:1] == 1.0, my_b, my_a)
                source_ref[c, k, edge : edge + 1, :] = source_ref[c, k, edge : edge + 1, :] - for_mine
                source_ref[c, k, other : other + 1, :] = source_ref[c, k, other : other + 1, :] - for_theirs
            for t in range(STRIP // 8):
                cells = roll(packed, A_LEFT - SPREAD * t - 6 * c)
                keep = (eight < ACT_LEFT) | (eight == A_RIGHT) | (eight == B_RIGHT)
                cells = jnp.where(keep, cells, flags)
                left, right = cells_of(c, low + 8 * t, 8)
                cells = jnp.where(eight < REACH, left, cells)
                cells = jnp.where(eight >= LANES - REACH, right, cells)
                column_ref[c, low + 8 * t : low + 8 * t + 8, :] = cells
            left, right = cells_of(c, edge, 1)
            cells = column_ref[c, edge : edge + 1, :]
            cells = jnp.where(one < REACH, left, cells)
            column_ref[c, edge : edge + 1, :] = jnp.where(one >= LANES - REACH, right, cells)

    @pl.when(row_even)
    def _():
        side(True, got_odd, sent_odd)
        side(False, got_even, sent_even)

    @pl.when(jnp.logical_not(row_even))
    def _():
        side(True, got_even, sent_even)
        side(False, got_odd, sent_odd)

    first = HALO - STRIP
    half = even_ref.shape[1]
    low_half = lane_ids(half) < LANES // 2

    def pack(out, right):
        for c in range(chans):
            upper = column_ref[c, first : first + half, :]
            lower = column_ref[c, first + half : first + 2 * half, :]
            if right:
                out[c] = jnp.where(low_half, roll(upper, LANES // 2), lower)
            else:
                out[c] = jnp.where(low_half, upper, roll(lower, LANES // 2))

    @pl.when(col_even)
    def _():
        pack(even_ref, True)
        pack(odd_ref, False)

    @pl.when(jnp.logical_not(col_even))
    def _():
        pack(even_ref, False)
        pack(odd_ref, True)


def bands(height, depth):
    halo = HALO >> depth
    return ((0, halo), (halo, height - halo), (height - halo, height))


def cycle(source_in, column_in, got_even, got_odd, x_ref, out_ref, side, *bufs):
    chans, own_tiles, height, _ = source_in.shape
    rows = height - 2 * HALO
    tiles = own_tiles + 1
    first = HALO - STRIP
    half = got_even.shape[1]
    col_even = lax.rem(lax.axis_index("blk"), 2) == 0
    levels = [bufs[5 * d : 5 * d + 5] for d in range(LEVELS)]

    low_half = lane_ids(half) < LANES // 2
    for c in range(chans):
        even, odd = got_even[c], got_odd[c]
        right = jnp.where(col_even, even, odd)
        left = jnp.where(col_even, odd, even)
        side[c, first : first + half, :] = jnp.where(low_half, right, roll(left, LANES // 2))
        side[c, first + half : first + 2 * half, :] = jnp.where(low_half, roll(right, LANES // 2), left)

    eight = lane_ids(8)
    in_low = eight < LANES // 2
    scale_mid, scale_side, mark_mid, mark_side = [], [], [], []
    for low, _ in ((HALO - 8, 0), (HALO, 0), (HALO + rows, 0)):
        mid, beside = column_in[0, low : low + 8, :], side[0, low : low + 8, :]
        scale_mid.append(spread_cell(mid, ACT_LEFT) * (0.25 * RELAX))
        mark_mid.append(spread_cell(mid, LAB_LEFT) == 1.0)
        scale_side.append(jnp.where(in_low, spread_cell(beside, ACT_LEFT), spread_cell(beside, ACT_RIGHT)) * (0.25 * RELAX))
        mark_side.append(jnp.where(in_low, spread_cell(beside, LAB_RIGHT), spread_cell(beside, LAB_LEFT)) == 1.0)

    def wide(mask, n):
        return jnp.broadcast_to(mask[:1], (n, LANES))

    def scales(band, n):
        return [wide(scale_mid[band], n)] * own_tiles + [wide(scale_side[band], n)]

    def pieces(depth, low, high, step):
        for band, (start, end) in enumerate(bands(height >> depth, depth)):
            start, end = max(start, low), min(end, high)
            while start < end:
                n = min(step, end - start)
                yield band, start, n
                start += n

    def swept(src, add, depth, band, r, n, keep=None):
        shift = 1 << depth
        ids = lane_ids(n)
        mids = [src[k, 8 + r : 8 + r + n, :] for k in range(tiles)]
        rights = [roll(t, shift) for t in mids]
        lefts = [roll(t, -shift) for t in mids]
        scale = scales(band, n)
        found = []
        for k in range(keep or tiles):
            below = jnp.where(ids < shift, rights[k - 1], rights[k])
            above = jnp.where(ids >= LANES - shift, lefts[(k + 1) % tiles], lefts[k])
            beside = (src[k, 7 + r : 7 + r + n, :] + src[k, 9 + r : 9 + r + n, :]) + (below + above)
            found.append(scale[k] * (mids[k] + beside) + add[k, 8 + r : 8 + r + n, :])
        return mids, found

    def restrict(rest, out, depth, low, high):
        shift = 1 << depth
        for r in range(low // 2, high // 2, 32):
            n = min(32, high // 2 - r)
            even = (lane_ids(n) & shift) == 0
            for k in range(tiles):
                total = rest[k, pl.ds(8 + 2 * r, n, stride=2), :] + rest[k, pl.ds(9 + 2 * r, n, stride=2), :]
                other = jnp.where(even, roll(total, -shift), roll(total, shift))
                out[k, 8 + r : 8 + r + n, :] = total + other

    def prolong(fix, out, depth, low, high):
        for band, r, n in pieces(depth + 1, low, high, 32):
            scale = scales(band, n)
            for k in range(tiles):
                value = fix[k, 8 + r : 8 + r + n, :] * (scale[k] * (4.0 / RELAX))
                out[k, pl.ds(8 + 2 * r, n, stride=2), :] = value
                out[k, pl.ds(9 + 2 * r, n, stride=2), :] = value

    def cycle_of(depth, low, high):
        src, one, two, rest, extra = levels[depth]
        step = 32
        if depth == LEVELS - 1:
            held = src
            for sweep in range(1, COARSE):
                into = (one, two)[sweep % 2]
                for band, r, n in pieces(depth, low, high, step):
                    _, found = swept(held, src, depth, band, r, n)
                    for k in range(tiles):
                        into[k, 8 + r : 8 + r + n, :] = found[k]
                held = into
            return held
        for band, r, n in pieces(depth, low, high, step):
            _, found = swept(src, src, depth, band, r, n)
            for k in range(tiles):
                one[k, 8 + r : 8 + r + n, :] = found[k]
        for band, r, n in pieces(depth, low, high, step):
            mids, found = swept(one, src, depth, band, r, n)
            for k in range(tiles):
                rest[k, 8 + r : 8 + r + n, :] = found[k] - mids[k]
        restrict(rest, levels[depth + 1][0], depth, low, high)
        fix = cycle_of(depth + 1, 0, height >> (depth + 1))
        if depth == 0:
            low, high = HALO - 8, HALO + rows + 8
        prolong(fix, extra, depth, low // 2, high // 2)
        for band, r, n in pieces(depth, low, high, step):
            for k in range(tiles):
                two[k, 8 + r : 8 + r + n, :] = one[k, 8 + r : 8 + r + n, :] + extra[k, 8 + r : 8 + r + n, :]
        for band, r, n in pieces(depth, low, high, step):
            _, found = swept(two, src, depth, band, r, n)
            for k in range(tiles):
                one[k, 8 + r : 8 + r + n, :] = found[k]
        if depth == 0:
            return one
        for band, r, n in pieces(depth, low, high, step):
            _, found = swept(one, src, depth, band, r, n)
            for k in range(tiles):
                two[k, 8 + r : 8 + r + n, :] = found[k]
        return two

    def channel(c, _):
        src = levels[0][0]
        for band, r, n in pieces(0, first, height - first, 32):
            ids = lane_ids(n)
            column, beside = column_in[c, r : r + n, :], side[c, r : r + n, :]
            theirs = jnp.where(wide(mark_mid[band], n), roll(beside, -1), beside)
            mine = jnp.where(wide(mark_side[band], n), roll(column, -1), column)
            scale = scales(band, n)
            for k in range(own_tiles):
                value = source_in[c, k, r : r + n, :]
                if k == 0:
                    value = value - jnp.where(ids == 0, scale[k] * roll(theirs, -A_RIGHT), 0.0)
                if k == own_tiles - 1:
                    value = value - jnp.where(ids == LANES - 1, scale[k] * roll(theirs, LANES - 1 - A_LEFT), 0.0)
                src[k, 8 + r : 8 + r + n, :] = value
            value = jnp.where((ids < REACH) | (ids >= LANES - REACH), beside, 0.0)
            value = value - jnp.where(ids == 0, scale[own_tiles] * roll(mine, -A_RIGHT), 0.0)
            value = value - jnp.where(ids == LANES - 1, scale[own_tiles] * roll(mine, LANES - 1 - A_LEFT), 0.0)
            src[own_tiles, 8 + r : 8 + r + n, :] = value
        one = cycle_of(0, first, height - first)
        for r in range(HALO, HALO + rows, 32):
            _, found = swept(one, src, 0, 1, r, 32, own_tiles)
            for k in range(own_tiles):
                at = pl.ds(k * LANES, LANES)
                out_ref[c, r - HALO : r - HALO + 32, at] = x_ref[c, r - HALO : r - HALO + 32, at] + found[k]
        return 0

    lax.fori_loop(0, chans, channel, 0)


def swaps(count, odd):
    pairs = [(i, i + 1) for i in range(odd, count - 1, 2)]
    return pairs + [(j, i) for i, j in pairs]


def shards(image_a, image_b, initial, coverage, seam_label):
    chans, rows, cols = image_a.shape
    tiles = cols // LANES
    height = rows + 2 * HALO
    vmem = pl.BlockSpec(memory_space=pltpu.VMEM)
    smem = pl.BlockSpec(memory_space=pltpu.SMEM)
    sds = functools.partial(jax.ShapeDtypeStruct, dtype=jnp.float32)
    params = pltpu.CompilerParams(vmem_limit_bytes=48 * 1024 * 1024)
    group, blk = lax.axis_size("group"), lax.axis_size("blk")
    central = sds((chans, tiles, height, LANES))
    column = sds((chans, height, LANES))
    upright = sds((tiles, chans * STRIP + 8, LANES))
    beside = sds((chans, (rows + 2 * STRIP) // 2, LANES))

    source, columns, sent_even, sent_odd = pl.pallas_call(
        prepare,
        out_shape=(central, column, upright, upright),
        in_specs=[vmem, vmem, vmem, smem, smem],
        out_specs=(vmem,) * 4,
        scratch_shapes=[pltpu.VMEM((tiles, rows + 16, LANES), jnp.float32)] * 2,
        compiler_params=params,
        name="prepare",
    )(image_a, image_b, initial, coverage, seam_label)
    got_even = lax.ppermute(sent_even, "group", swaps(group, 0))
    got_odd = lax.ppermute(sent_odd, "group", swaps(group, 1))

    source, columns, sent_even, sent_odd = pl.pallas_call(
        join_rows,
        out_shape=(central, column, beside, beside),
        in_specs=[vmem] * 6,
        out_specs=(vmem,) * 4,
        input_output_aliases={0: 0, 1: 1},
        compiler_params=params,
        name="join_rows",
    )(source, columns, sent_even, sent_odd, got_even, got_odd)
    got_even = lax.ppermute(sent_even, "blk", swaps(blk, 0))
    got_odd = lax.ppermute(sent_odd, "blk", swaps(blk, 1))

    scratch = [pltpu.VMEM((chans, height, LANES), jnp.float32)]
    for depth in range(LEVELS):
        scratch += [pltpu.VMEM((tiles + 1, (height >> depth) + 16, LANES), jnp.float32)] * 5
    return pl.pallas_call(
        cycle,
        out_shape=sds((chans, rows, cols)),
        in_specs=[vmem] * 5,
        out_specs=vmem,
        scratch_shapes=scratch,
        compiler_params=params,
        name="cycle",
    )(source, columns, got_even, got_odd, initial)


def solution(mesh):
    placed = (
        P(None, "group", "blk"),
        P(None, "group", "blk"),
        P(None, "group", "blk"),
        P("group", "blk"),
        P("group", "blk"),
    )
    return jax.shard_map(
        shards, mesh=mesh, in_specs=placed, out_specs=P(None, "group", "blk"), check_vma=False
    )
```

```python
import functools

import jax
import jax.numpy as jnp
from jax import lax
from jax.experimental import pallas as pl
from jax.experimental.pallas import tpu as pltpu
from jax.sharding import PartitionSpec as P

LEVELS = 4
NU = 2
COARSE = 4
RELAX = 0.8
NEAR = 0.25 * RELAX

LANES = 128
HALF = LANES // 2
HALO = 64
STEP = 96


def source_reach():
    need = 0
    for _ in range(LEVELS - 1):
        need = -(-(need + NU) // 2)
    need += COARSE - 1
    for _ in range(LEVELS - 1):
        need = 2 * need + NU
    return need


REACH = source_reach()
STRIP = REACH + 2
assert STRIP % 8 == 0 and STRIP <= HALO
FIRST = HALO - STRIP
RIM = 8
SEAM = 6


def lane_ids(rows):
    return lax.broadcasted_iota(jnp.int32, (rows, LANES), 1)


def roll(tile, shift):
    return pltpu.roll(tile, shift % LANES, 1)


def spans(low, high, step=STEP):
    while low < high:
        yield low, min(step, high - low)
        low += step


def even_at(axis):
    return lax.rem(lax.axis_index(axis), 2) == 0


def own_source(mids, ups, downs, active):
    tiles = len(mids)
    rights = [roll(t, 1) for t in mids]
    lefts = [roll(t, -1) for t in mids]
    ids = lane_ids(mids[0].shape[0])
    found = []
    for k in range(tiles):
        before = jnp.where(ids == 0, rights[k - 1] if k else 0.0, rights[k])
        after = jnp.where(ids == LANES - 1, lefts[k + 1] if k + 1 < tiles else 0.0, lefts[k])
        beside = (ups[k] + downs[k]) + (before + after)
        found.append(active * (RELAX * mids[k] - NEAR * beside))
    return found


def staggered(items, begin, end, depth):
    waiting = []
    for item in items:
        waiting.append((item, begin(item)))
        if len(waiting) > depth:
            end(*waiting.pop(0))
    for each in waiting:
        end(*each)


def turn(src, shift, r, n):
    tiles = range(src.shape[0])
    return [roll(src[k, r : r + n, :], shift) for k in tiles], [roll(src[k, r : r + n, :], -shift) for k in tiles]


def swept(src, add, scale, shift, r, n, ring, turned, keep=None):
    tiles = src.shape[0]
    ids = lane_ids(n)
    mids = [src[k, r : r + n, :] for k in range(tiles)]
    rights, lefts = turned
    found = []
    for k in range(keep or tiles):
        before, after = rights[k], lefts[k]
        if tiles > 1 or not ring:
            before = jnp.where(ids < shift, rights[k - 1] if ring or k else 0.0, before)
            after = jnp.where(ids >= LANES - shift, lefts[(k + 1) % tiles] if ring or k + 1 < tiles else 0.0, after)
        beside = (src[k, r - 1 : r - 1 + n, :] + src[k, r + 1 : r + 1 + n, :]) + (before + after)
        more = add(k, r - 8, n) if callable(add) else add[k, r : r + n, :]
        found.append(scale[k] * (mids[k] + beside) + more)
    return mids, found


def restricted(rest, k, r, n, shift):
    total = rest[k, pl.ds(r, n, stride=2), :] + rest[k, pl.ds(r + 1, n, stride=2), :]
    even = (lane_ids(n) & shift) == 0
    return total + jnp.where(even, roll(total, -shift), roll(total, shift))


def strips(a_ref, b_ref, x_ref, cover_ref, label_ref, even_ref, odd_ref, picked, other_a, other_b, built):
    chans, rows, cols = a_ref.shape
    tiles = cols // LANES
    active = cover_ref[0, 0].astype(jnp.float32)
    marked = label_ref[0, 0].astype(jnp.float32)
    second = label_ref[0, 0] == 1
    eight = lane_ids(8)

    top = pl.program_id(0) == 0
    low = jnp.where(top, 0, rows - STRIP)
    line = jnp.where(top, 0, rows - 1)
    spot = jnp.where(top, STRIP - 2, 0)
    for k in range(tiles):
        for edge in (7, 8 + rows):
            picked[k, edge : edge + 1, :] = jnp.zeros((1, LANES), jnp.float32)
    packed = jnp.zeros((8, LANES), jnp.float32)
    for c in range(chans):
        for k in range(tiles):
            at = pl.ds(k * LANES, LANES)
            for r, n in spans(0, rows):
                x = x_ref[c, r : r + n, at]
                from_a, from_b = a_ref[c, r : r + n, at] - x, b_ref[c, r : r + n, at] - x
                other_a[k, r : r + n, :], other_b[k, r : r + n, :] = from_a, from_b
                picked[k, 8 + r : 8 + r + n, :] = jnp.where(second, from_b, from_a)
        start = pl.multiple_of(low, 8)
        parts = [[picked[k, pl.ds(start + 8 + s, STRIP), :] for k in range(tiles)] for s in (0, -1, 1)]
        for k, found in enumerate(own_source(*parts, active)):
            built[k, c * STRIP : (c + 1) * STRIP, :] = found
        for k in range(tiles):
            built[k, pl.ds(c * STRIP + spot, 1), :] = other_a[k, pl.ds(line, 1), :]
            built[k, pl.ds(c * STRIP + spot + 1, 1), :] = other_b[k, pl.ds(line, 1), :]
        for t in range(STRIP // 8):
            lane = 4 * (chans * t + c)
            at = pl.ds(start + 8 * t, 8)
            packed = jnp.where(eight == lane, roll(other_a[0, at, :], lane), packed)
            packed = jnp.where(eight == lane + 1, roll(other_b[0, at, :], lane + 1), packed)
            packed = jnp.where(eight == lane + 2, roll(other_a[tiles - 1, at, :], lane + 3), packed)
            packed = jnp.where(eight == lane + 3, roll(other_b[tiles - 1, at, :], lane + 4), packed)
    built[0, chans * STRIP :, :] = packed
    for k in range(1, tiles):
        built[k, chans * STRIP :, :] = jnp.where(eight < HALF, active, marked)

    by_odd = top == even_at("group")

    @pl.when(by_odd)
    def _():
        odd_ref[...] = built[...]

    @pl.when(jnp.logical_not(by_odd))
    def _():
        even_ref[...] = built[...]


def inside(a_ref, b_ref, x_ref, cover_ref, label_ref, source_ref, once_ref, seam_ref, coarse_ref, da, db, rest):
    chans, rows, cols = a_ref.shape
    tiles = cols // LANES
    active = cover_ref[0, 0].astype(jnp.float32)
    second = label_ref[0, 0] == 1
    for k in range(tiles):
        for buf in (da, db):
            buf[k, 0:8, :] = jnp.zeros((8, LANES), jnp.float32)
            buf[k, rows + 8 : rows + 16, :] = jnp.zeros((8, LANES), jnp.float32)
    scale = [active * NEAR] * tiles
    top, end = HALO, HALO + rows

    def pick(k, low, n):
        return jnp.where(second, db[k, low : low + n, :], da[k, low : low + n, :])

    def channel(c, _):
        for k in range(tiles):
            at = pl.ds(k * LANES, LANES)
            for r, n in spans(0, rows):
                x = x_ref[c, r : r + n, at]
                da[k, 8 + r : 8 + r + n, :] = a_ref[c, r : r + n, at] - x
                db[k, 8 + r : 8 + r + n, :] = b_ref[c, r : r + n, at] - x
        for r, n in spans(0, rows):
            parts = [[pick(k, 8 + s + r, n) for k in range(tiles)] for s in (0, -1, 1)]
            found = own_source(*parts, active)
            for k in range(tiles):
                source_ref[c, k, top + r : top + r + n, :] = found[k]
            ids = lane_ids(n)
            seam = jnp.where(ids < SEAM, found[0], roll(found[tiles - 1], HALF))
            at = pl.ds(8 + r, n)
            seam = jnp.where(ids == HALF, roll(da[tiles - 1, at, :], HALF + 1), seam)
            seam = jnp.where(ids == HALF + 1, roll(db[tiles - 1, at, :], HALF + 2), seam)
            seam = jnp.where(ids == LANES - 1, roll(da[0, at, :], -1), seam)
            seam_ref[c, top + r : top + r + n, :] = jnp.where(ids == LANES - 2, roll(db[0, at, :], -2), seam)
        source, once = source_ref.at[c], once_ref.at[c]

        def first(piece, turned):
            r, n = piece
            _, found = swept(source, source, scale, 1, r, n, False, turned)
            for k in range(tiles):
                once_ref[c, k, r : r + n, :] = found[k]

        def second_sweep(piece, turned):
            r, n = piece
            mids, found = swept(once, source, scale, 1, r, n, False, turned)
            for k in range(tiles):
                rest[k, r : r + n, :] = found[k] - mids[k]

        staggered(spans(top, end), lambda piece: turn(source, 1, *piece), first, 0)
        staggered(spans(top, end), lambda piece: turn(once, 1, *piece), second_sweep, 0)
        for r, n in spans(top // 2, end // 2):
            for k in range(tiles):
                coarse_ref[c, k, r : r + n, :] = restricted(rest, k, 2 * r, n, 1)
        return 0

    lax.fori_loop(0, chans, channel, 0)


def seam_units(chans, height):
    tiles_of = (height - 2 * FIRST) // 8
    for unit in range(chans * tiles_of):
        yield unit // tiles_of, FIRST + 8 * (unit % tiles_of), unit // 16, 8 * (unit % 16)


def message_rows(chans, height):
    quarter = height // 2
    cells = (chans // 2 * quarter + chans % 2 * quarter // 2) // 2
    units = -(-chans * ((height - 2 * FIRST) // 8) // 16) * 8
    return cells, units


def column_rows(chans, height):
    quarter = height // 2
    places = [(c, r, c + 1, r) for c in range(0, chans - 1, 2) for r in range(0, quarter, 8)]
    if chans % 2:
        places += [(chans - 1, r, chans - 1, r + quarter // 2) for r in range(0, quarter // 2, 8)]
    return places


def join_rows(
    source_in, once_in, seam_in, coarse_in, sent_even, sent_odd, got_even, got_odd, cover_ref, label_ref,
    source_ref, once_ref, seam_ref, coarse_ref, even_ref, odd_ref, rest, marks_ref, upper_got, lower_got, lines, left_out, right_out,
):
    chans, tiles, height, _ = source_ref.shape
    rows = height - 2 * HALO
    tail = chans * STRIP
    row_even, col_even = even_at("group"), even_at("blk")
    active = cover_ref[0, 0].astype(jnp.float32)
    marked = label_ref[0, 0].astype(jnp.float32)
    eight = lane_ids(8)

    def take(top, got):
        low = FIRST if top else HALO + rows
        their_spot = 0 if top else STRIP - 2
        my_spot = 0 if top else 2
        edge = HALO if top else HALO + rows - 1
        other = edge - 1 if top else edge + 1
        packed = got[0, tail:, :]
        marks = got[1, tail:, :]
        their_active = jnp.broadcast_to(marks[0:1, 0:1], (1, LANES))
        their_mark = jnp.broadcast_to(marks[0:1, HALF : HALF + 1], (1, LANES))
        band = 0 if top else 2
        marks_ref[band : band + 1, :] = their_active
        marks_ref[band + 3 : band + 4, :] = their_mark
        for c in range(chans):
            for k in range(tiles):
                source_ref[c, k, low : low + STRIP, :] = got[k, c * STRIP : (c + 1) * STRIP, :]
                their_a = got[k, c * STRIP + their_spot : c * STRIP + their_spot + 1, :]
                their_b = got[k, c * STRIP + their_spot + 1 : c * STRIP + their_spot + 2, :]
                my_a = lines[k, 4 * c + my_spot : 4 * c + my_spot + 1, :]
                my_b = lines[k, 4 * c + my_spot + 1 : 4 * c + my_spot + 2, :]
                for_mine = NEAR * active * jnp.where(marked == 1.0, their_b, their_a)
                for_theirs = NEAR * their_active * jnp.where(their_mark == 1.0, my_b, my_a)
                source_ref[c, k, edge : edge + 1, :] = source_ref[c, k, edge : edge + 1, :] - for_mine
                source_ref[c, k, other : other + 1, :] = source_ref[c, k, other : other + 1, :] - for_theirs
            for t in range(STRIP // 8):
                lane = 4 * (chans * t + c)
                last = roll(packed, HALF - lane - 2)
                once_a, once_b = roll(packed, LANES - 1 - lane), roll(packed, LANES - 2 - lane - 1)
                cells = jnp.where(eight == LANES - 1, once_a, jnp.where(eight == LANES - 2, once_b, last))
                r = low + 8 * t
                cells = jnp.where(eight < SEAM, source_ref[c, 0, r : r + 8, :], cells)
                end = roll(source_ref[c, tiles - 1, r : r + 8, :], HALF)
                seam_ref[c, r : r + 8, :] = jnp.where((eight >= HALF - SEAM) & (eight < HALF), end, cells)
            r = edge // 8 * 8
            cells = jnp.where(eight < SEAM, source_ref[c, 0, r : r + 8, :], seam_ref[c, r : r + 8, :])
            end = roll(source_ref[c, tiles - 1, r : r + 8, :], HALF)
            seam_ref[c, r : r + 8, :] = jnp.where((eight >= HALF - SEAM) & (eight < HALF), end, cells)

    def arrange(upper, lower, mine_up, mine_low):
        upper_got[...] = upper[...]
        lower_got[...] = lower[...]
        for c in range(chans):
            for k in range(tiles):
                lines[k, 4 * c : 4 * c + 2, :] = mine_up[k, (c + 1) * STRIP - 2 : (c + 1) * STRIP, :]
                lines[k, 4 * c + 2 : 4 * c + 4, :] = mine_low[k, c * STRIP : c * STRIP + 2, :]

    @pl.when(row_even)
    def _():
        arrange(got_odd, got_even, sent_odd, sent_even)

    @pl.when(jnp.logical_not(row_even))
    def _():
        arrange(got_even, got_odd, sent_even, sent_odd)

    take(True, upper_got)
    take(False, lower_got)
    marks_ref[1:2, :] = jnp.full((1, LANES), active)
    marks_ref[4:5, :] = jnp.full((1, LANES), marked)
    marks_ref[6:8, :] = jnp.zeros((2, LANES), jnp.float32)

    edges = ((FIRST, HALO, 0), (HALO, HALO + RIM, 1), (HALO + rows - RIM, HALO + rows, 1), (HALO + rows, height - FIRST, 2))
    spots = [(c, band, r, n) for c in range(chans) for low, high, band in edges for r, n in spans(low, high)]
    for stage in range(2):
        held = (source_ref, once_ref)[stage]

        def edge_sweep(spot, turned):
            c, band, r, n = spot
            scale = [jnp.broadcast_to(marks_ref[band : band + 1, :] * NEAR, (n, LANES))] * tiles
            mids, found = swept(held.at[c], source_ref.at[c], scale, 1, r, n, False, turned)
            for k in range(tiles):
                if stage == 0:
                    once_ref[c, k, r : r + n, :] = found[k]
                else:
                    rest[c, k, r : r + n, :] = found[k] - mids[k]

        staggered(spots, lambda spot: turn(held.at[spot[0]], 1, *spot[2:]), edge_sweep, 0)
    for c in range(chans):
        for low, high in ((FIRST, HALO + RIM), (HALO + rows - RIM, height - FIRST)):
            for k in range(tiles):
                coarse_ref[c, k, low // 2 : high // 2, :] = restricted(rest.at[c], k, low, (high - low) // 2, 1)
            zeros = jnp.zeros((FIRST // 2, LANES), jnp.float32)
        for k in range(tiles):
            coarse_ref[c, k, 0 : FIRST // 2, :] = zeros
            coarse_ref[c, k, (height - FIRST) // 2 : height // 2, :] = zeros

    cells, units = message_rows(chans, height)
    first_half = eight < HALF
    even_lane = (eight & 1) == 0

    def edge_cells(c, r):
        return jnp.where(first_half, coarse_ref[c, 0, r : r + 8, :], coarse_ref[c, tiles - 1, r : r + 8, :])

    def joined(place):
        c, r, d, s = place
        return jnp.where(even_lane, edge_cells(c, r), edge_cells(d, s))

    def pack(left, right):
        places = column_rows(chans, height)
        for t in range(cells // 8):
            upper, lower = joined(places[t]), joined(places[t + cells // 8])
            left[8 * t : 8 * t + 8, :] = jnp.where(first_half, upper, roll(lower, HALF))
            right[8 * t : 8 * t + 8, :] = jnp.where(first_half, roll(upper, HALF), lower)
        lefts = rights = jnp.zeros((8, LANES), jnp.float32)
        last = None
        for c, r, tile, lane in [*seam_units(chans, height), (None, None, -1, 0)]:
            if tile != last and last is not None:
                at = cells + 8 * last
                left[at : at + 8, :], right[at : at + 8, :] = lefts, rights
            last = tile
            if c is None:
                break
            value = seam_ref[c, r : r + 8, :]
            spot = (eight >= lane) & (eight < lane + 8)
            lefts = jnp.where(spot, roll(value, lane + 2), lefts)
            rights = jnp.where(spot, roll(value, lane - (HALF - SEAM)), rights)
        for out in (left, right):
            out[cells + units : cells + units + 8, :] = marks_ref[...]

    pack(left_out, right_out)

    @pl.when(col_even)
    def _():
        odd_ref[...] = left_out[...]
        even_ref[...] = right_out[...]

    @pl.when(jnp.logical_not(col_even))
    def _():
        even_ref[...] = left_out[...]
        odd_ref[...] = right_out[...]


def cycle(
    source_in, once_in, seam_in, coarse_in, sent_even, got_even, got_odd, x_ref, out_ref,
    right_ref, left_ref, seam_source, seam_once, seam_rest, fine, fine_two, *bufs,
):
    chans, own_tiles, height, _ = source_in.shape
    rows = height - 2 * HALO
    tiles = own_tiles + 1
    cells, units = message_rows(chans, height)
    col_even = even_at("blk")
    eight = lane_ids(8)

    @pl.when(col_even)
    def _():
        right_ref[...] = got_even[...]
        left_ref[...] = got_odd[...]

    @pl.when(jnp.logical_not(col_even))
    def _():
        right_ref[...] = got_odd[...]
        left_ref[...] = got_even[...]

    at = cells + units

    def mark(ref, row):
        return jnp.broadcast_to(ref[at + row : at + row + 1, :], (8, LANES))

    own = [mark(sent_even, i) for i in range(6)]
    right = [mark(right_ref, i) for i in range(6)]
    left = [mark(left_ref, i) for i in range(6)]
    quarter3 = eight < HALF + HALF // 2
    first_half = eight < HALF

    def mixed(i):
        return jnp.where(first_half, own[i], jnp.where(quarter3, right[i], left[i]))

    seam_scale = [mixed(i) * NEAR for i in range(3)]
    seam_mark = [mixed(i + 3) == 1.0 for i in range(3)]
    own_scale = [own[i] * NEAR for i in range(3)]
    side_scale = [jnp.where(first_half, right[i], left[i]) * NEAR for i in range(3)]

    def wide(mask, n):
        return jnp.broadcast_to(mask[:1], (n, LANES))

    def over_rows(kinds, depth, r, n):
        full, halo = height >> depth, HALO >> depth
        ends = ((0, halo), (halo, full - halo), (full - halo, full))
        parts = [(max(a, r), min(b, r + n), kind) for (a, b), kind in zip(ends, kinds)]
        parts = [wide(kind, b - a) for a, b, kind in parts if b > a]
        return parts[0] if len(parts) == 1 else jnp.concatenate(parts, axis=0)

    def scales(depth, r, n):
        return [over_rows(own_scale, depth, r, n)] * own_tiles + [over_rows(side_scale, depth, r, n)]

    inner = (eight < SEAM) | ((eight >= HALF - SEAM) & (eight < HALF))
    outer = ((eight >= HALF) & (eight < HALF + SEAM)) | (eight >= LANES - SEAM)
    from_near = (eight == 0) | (eight == HALF - 1)
    from_own = (eight == HALF) | (eight == LANES - 1)
    up_one = (eight == HALF - 1) | (eight == LANES - 1)
    near_b = (eight == HALF - 2) | (eight == 1)
    right_unit = (eight >= HALF - 2) & (eight < HALF + SEAM)
    def unpack(unit):
        c, r, tile, lane = unit
        rights = roll(right_ref[cells + 8 * tile : cells + 8 * tile + 8, :], HALF - 2 - lane)
        lefts = roll(left_ref[cells + 8 * tile : cells + 8 * tile + 8, :], LANES - SEAM - lane)
        return rights, lefts

    def keep_near(unit, turned):
        c, r, _, _ = unit
        seam_rest[c, 0, r : r + 8, :] = jnp.where(right_unit, *turned)

    def second_cells(unit):
        c, r, _, _ = unit
        cells_b = jnp.where(near_b, seam_rest[c, 0, r : r + 8, :], seam_in[c, r : r + 8, :])
        return roll(cells_b, 1), roll(cells_b, -1)

    def put_seam(unit, turned):
        c, r, _, _ = unit
        band = 0 if r < HALO else 1 if r < HALO + rows else 2
        near, mine = seam_rest[c, 0, r : r + 8, :], seam_in[c, r : r + 8, :]
        value = jnp.where(inner, mine, jnp.where(outer, near, 0.0))
        border = jnp.where(seam_mark[band], jnp.where(up_one, *turned), jnp.where(from_near, near, mine))
        border = jnp.where(from_near | from_own, border, 0.0)
        seam_source[c, 0, r : r + 8, :] = value - seam_scale[band] * border

    units_of = list(seam_units(chans, height))
    staggered(units_of, unpack, keep_near, 24)
    staggered(units_of, second_cells, put_seam, 24)
    spots = [(c, r, n) for c in range(chans) for r, n in spans(FIRST, height - FIRST, 2 * STEP)]

    def seam_first(spot, turned):
        c, r, n = spot
        source = seam_source.at[c]
        _, found = swept(source, source, [over_rows(seam_scale, 0, r, n)], 1, r, n, True, turned)
        seam_once[c, 0, r : r + n, :] = found[0]

    def seam_second(spot, turned):
        c, r, n = spot
        scale = [over_rows(seam_scale, 0, r, n)]
        mids, found = swept(seam_once.at[c], seam_source.at[c], scale, 1, r, n, True, turned)
        seam_rest[c, 0, r : r + n, :] = found[0] - mids[0]

    staggered(spots, lambda spot: turn(seam_source.at[spot[0]], 1, *spot[1:]), seam_first, 0)
    staggered(spots, lambda spot: turn(seam_once.at[spot[0]], 1, *spot[1:]), seam_second, 0)

    one_src, one_once, one_two = bufs[0:3]
    half_rows = height // 2
    eights = lane_ids(8)
    even_lane = (eights & 1) == 0
    places = column_rows(chans, height)
    for t, (c, r, d, s) in enumerate(places):
        low, upper = (8 * t, True) if t < cells // 8 else (8 * t - cells, False)
        from_right, from_left = right_ref[low : low + 8, :], left_ref[low : low + 8, :]
        if upper:
            value = jnp.where(first_half, from_right, roll(from_left, HALF))
        else:
            value = jnp.where(first_half, roll(from_right, HALF), from_left)
        one_src[c, own_tiles, 8 + r : 16 + r, :] = jnp.where(even_lane, value, roll(value, 1))
        one_src[d, own_tiles, 8 + s : 16 + s, :] = jnp.where(even_lane, roll(value, -1), value)
    for c in range(chans):
        for r, n in spans(0, half_rows):
            for k in range(own_tiles):
                one_src[c, k, 8 + r : 8 + r + n, :] = coarse_in[c, k, r : r + n, :]
        for r, n in spans(FIRST // 2, half_rows - FIRST // 2):
            ids = lane_ids(n)
            seam = restricted(seam_rest.at[c], 0, 2 * r, n, 1)
            turned = roll(seam, HALF)
            at = pl.ds(8 + r, n)
            one_src[c, 0, at, :] = jnp.where(ids < 4, seam, one_src[c, 0, at, :])
            one_src[c, own_tiles - 1, at, :] = jnp.where(ids >= LANES - 4, turned, one_src[c, own_tiles - 1, at, :])
            side = jnp.where(ids < 4, turned, one_src[c, own_tiles, at, :])
            one_src[c, own_tiles, at, :] = jnp.where(ids >= LANES - 4, seam, side)

    def smooth(src, once, fields, depth, into, minus=False):
        def one_sweep(spot, turned):
            f, r, n = spot
            mids, found = swept(once.at[f], src.at[f], scales(depth, r, n), 1 << depth, 8 + r, n, True, turned)
            for k in range(tiles):
                into[f, k, 8 + r : 8 + r + n, :] = found[k] - mids[k] if minus else found[k]

        spots = [(f, r, n) for f in range(fields) for r, n in spans(0, height >> depth)]
        staggered(spots, lambda spot: turn(once.at[spot[0]], 1 << depth, 8 + spot[1], spot[2]), one_sweep, 0)

    def expand(fix, fields, depth, out, low, high, spread):
        for f in range(fields):
            for r, n in spans(low, high):
                scale = scales(depth + 1, r, n)
                for k in range(tiles):
                    value = fix[0 if spread else f, k, 8 + r : 8 + r + n, :]
                    if spread:
                        value = spread(value, f)
                    value = value * (scale[k] * (1.0 / NEAR))
                    out[f, k, pl.ds(8 + 2 * r, n, stride=2), :] = value
                    out[f, k, pl.ds(9 + 2 * r, n, stride=2), :] = value

    def add_fix(once, two, fields, depth, into):
        for f in range(fields):
            for r, n in spans(0, height >> depth):
                for k in range(tiles):
                    at = pl.ds(8 + r, n)
                    into[f, k, at, :] = once[f, k, at, :] + two[f, k, at, :]

    assert chans <= 4 and LEVELS >= 3

    def spread_channel(value, f):
        ids = lane_ids(value.shape[0])
        odd = (ids & 1) == 1
        pair = jnp.where(odd, value, roll(value, -1)) if f & 1 else jnp.where(odd, roll(value, 1), value)
        high = (ids & 2) == 2
        return jnp.where(high, pair, roll(pair, -2)) if f & 2 else jnp.where(high, roll(pair, 2), pair)

    def level(depth):
        src, once, two = bufs[3 * (depth - 1) : 3 * depth]
        fields = chans if depth == 1 else 1
        if depth == LEVELS - 1:
            held = src
            for sweep in range(1, COARSE):
                into = (once, two)[sweep % 2]
                smooth(src, held, fields, depth, into)
                held = into
            return held
        smooth(src, src, fields, depth, once)
        smooth(src, once, fields, depth, two, True)
        below = bufs[3 * depth]
        shift = 1 << depth
        for r, n in spans(0, height >> (depth + 1)):
            ids = lane_ids(n) & 3
            for k in range(tiles):
                value = None
                for f in range(fields):
                    total = restricted(two.at[f], k, 8 + 2 * r, n, shift)
                    value = total if value is None else jnp.where(ids == f, total, value)
                below[0, k, 8 + r : 8 + r + n, :] = value
        fix = level(depth + 1)
        expand(fix, fields, depth, two, 0, height >> (depth + 1), spread_channel if depth == 1 else None)
        add_fix(once, two, fields, depth, once)
        smooth(src, once, fields, depth, two)
        smooth(src, two, fields, depth, once)
        return once

    fix = level(1)
    low, high = HALO - RIM, HALO + rows + RIM

    def fine_source(c):
        def tile(k, r, n):
            ids = lane_ids(n)
            seam = seam_source[c, 0, r : r + n, :]
            if k == own_tiles:
                return jnp.where(ids < HALF, roll(seam, HALF), seam)
            value = source_in[c, k, r : r + n, :]
            if k == 0:
                value = jnp.where(ids == 0, seam, value)
            if k == own_tiles - 1:
                value = jnp.where(ids == LANES - 1, roll(seam, HALF), value)
            return value

        return tile

    def finish(c, _):
        for r, n in spans(low // 2, high // 2):
            scale = scales(1, r, n)
            for k in range(tiles):
                value = fix[c, k, 8 + r : 8 + r + n, :] * (scale[k] * (1.0 / NEAR))
                fine[k, pl.ds(8 + 2 * r, n, stride=2), :] = value
                fine[k, pl.ds(9 + 2 * r, n, stride=2), :] = value
        for r, n in spans(low, high):
            ids = lane_ids(n)
            seam = seam_once[c, 0, r : r + n, :]
            turned = roll(seam, HALF)
            at = pl.ds(8 + r, n)
            for k in range(own_tiles):
                value = once_in[c, k, r : r + n, :]
                if k == 0:
                    value = jnp.where(ids < 2, seam, value)
                if k == own_tiles - 1:
                    value = jnp.where(ids >= LANES - 2, turned, value)
                fine[k, at, :] = fine[k, at, :] + value
            fine[own_tiles, at, :] = fine[own_tiles, at, :] + jnp.where(ids < HALF, turned, seam)
        add = fine_source(c)

        def first(piece, turned):
            r, n = piece
            _, found = swept(fine, add, scales(0, r, n), 1, 8 + r, n, True, turned)
            for k in range(tiles):
                fine_two[k, 8 + r : 8 + r + n, :] = found[k]

        def last(piece, turned):
            r, n = piece
            _, found = swept(fine_two, add, scales(0, r, n), 1, 8 + r, n, True, turned, own_tiles)
            for k in range(own_tiles):
                at = pl.ds(k * LANES, LANES)
                out_ref[c, r - HALO : r - HALO + n, at] = x_ref[c, r - HALO : r - HALO + n, at] + found[k]

        staggered(spans(low, high), lambda piece: turn(fine, 1, 8 + piece[0], piece[1]), first, 0)
        staggered(spans(HALO, HALO + rows), lambda piece: turn(fine_two, 1, 8 + piece[0], piece[1]), last, 0)
        return 0

    lax.fori_loop(0, chans, finish, 0)


def swaps(count, odd):
    pairs = [(i, i + 1) for i in range(odd, count - 1, 2)]
    return pairs + [(j, i) for i, j in pairs]


def shards(image_a, image_b, initial, coverage, seam_label):
    chans, rows, cols = image_a.shape
    tiles = cols // LANES
    height = rows + 2 * HALO
    vmem = pl.BlockSpec(memory_space=pltpu.VMEM)
    smem = pl.BlockSpec(memory_space=pltpu.SMEM)
    f32 = jnp.float32
    sds = functools.partial(jax.ShapeDtypeStruct, dtype=f32)
    params = pltpu.CompilerParams(vmem_limit_bytes=40 * 1024 * 1024)
    group, blk = lax.axis_size("group"), lax.axis_size("blk")
    central = sds((chans, tiles, height, LANES))
    column = sds((chans, height, LANES))
    coarse = sds((chans, tiles, height // 2, LANES))
    upright = sds((tiles, chans * STRIP + 8, LANES))
    beside = sds((sum(message_rows(chans, height)) + 8, LANES))

    last = rows // HALO - 1
    block = pl.BlockSpec((chans, HALO, cols), lambda i: (0, i * last, 0))
    whole = pl.BlockSpec(upright.shape, lambda i: (0, 0, 0))
    sent_even, sent_odd = pl.pallas_call(
        strips,
        grid=(2,),
        out_shape=(upright, upright),
        in_specs=[block, block, block, smem, smem],
        out_specs=(whole, whole),
        scratch_shapes=[pltpu.VMEM((tiles, HALO + 16, LANES), f32)] + [pltpu.VMEM((tiles, HALO, LANES), f32)] * 2
        + [pltpu.VMEM(upright.shape, f32)],
        compiler_params=params,
        name="strips",
    )(image_a, image_b, initial, coverage, seam_label)
    got_even = lax.ppermute(sent_even, "group", swaps(group, 0))
    got_odd = lax.ppermute(sent_odd, "group", swaps(group, 1))

    source, once, seam, coarser = pl.pallas_call(
        inside,
        out_shape=(central, central, column, coarse),
        in_specs=[vmem, vmem, vmem, smem, smem],
        out_specs=(vmem,) * 4,
        scratch_shapes=[pltpu.VMEM((tiles, rows + 16, LANES), f32)] * 2 + [pltpu.VMEM((tiles, height, LANES), f32)],
        compiler_params=params,
        cost_estimate=pl.CostEstimate(flops=200_000_000, bytes_accessed=4_000_000, transcendentals=0),
        name="inside",
    )(image_a, image_b, initial, coverage, seam_label)

    source, once, seam, coarser, sent_even, sent_odd = pl.pallas_call(
        join_rows,
        out_shape=(central, central, column, coarse, beside, beside),
        in_specs=[vmem] * 8 + [smem] * 2,
        out_specs=(vmem,) * 6,
        input_output_aliases={0: 0, 1: 1, 2: 2, 3: 3},
        scratch_shapes=[pltpu.VMEM(central.shape, f32), pltpu.VMEM((8, LANES), f32)]
        + [pltpu.VMEM(upright.shape, f32)] * 2
        + [pltpu.VMEM((tiles, 4 * chans, LANES), f32)]
        + [pltpu.VMEM(beside.shape, f32)] * 2,
        compiler_params=params,
        name="join_rows",
    )(source, once, seam, coarser, sent_even, sent_odd, got_even, got_odd, coverage, seam_label)
    got_even = lax.ppermute(sent_even, "blk", swaps(blk, 0))
    got_odd = lax.ppermute(sent_odd, "blk", swaps(blk, 1))

    scratch = [pltpu.VMEM(beside.shape, f32)] * 2 + [pltpu.VMEM((chans, 1, height, LANES), f32)] * 3
    scratch += [pltpu.VMEM((tiles + 1, height + 16, LANES), f32)] * 2
    for depth in range(1, LEVELS):
        fields = chans if depth == 1 else 1
        scratch += [pltpu.VMEM((fields, tiles + 1, (height >> depth) + 16, LANES), f32)] * 3
    return pl.pallas_call(
        cycle,
        out_shape=sds((chans, rows, cols)),
        in_specs=[vmem] * 8,
        out_specs=vmem,
        scratch_shapes=scratch,
        compiler_params=params,
        name="cycle",
    )(source, once, seam, coarser, sent_even, got_even, got_odd, initial)


def solution(mesh):
    placed = (
        P(None, "group", "blk"),
        P(None, "group", "blk"),
        P(None, "group", "blk"),
        P("group", "blk"),
        P("group", "blk"),
    )
    return jax.shard_map(
        shards, mesh=mesh, in_specs=placed, out_specs=P(None, "group", "blk"), check_vma=False
    )
```

```python
import functools

import jax
import jax.numpy as jnp
from jax import lax
from jax.experimental import pallas as pl
from jax.experimental.pallas import tpu as pltpu
from jax.sharding import PartitionSpec as P

LEVELS = 4
NU = 2
COARSE = 4
RELAX = 0.8
NEAR = 0.25 * RELAX

LANES = 128
HALF = LANES // 2
HALO = 64
STEP = 96


def source_reach():
    need = 0
    for _ in range(LEVELS - 1):
        need = -(-(need + NU) // 2)
    need += COARSE - 1
    for _ in range(LEVELS - 1):
        need = 2 * need + NU
    return need


REACH = source_reach()
STRIP = REACH + 2
assert STRIP % 8 == 0 and STRIP <= HALO
FIRST = HALO - STRIP
RIM = 8
SEAM = 6


def lane_ids(rows):
    return lax.broadcasted_iota(jnp.int32, (rows, LANES), 1)


def roll(tile, shift):
    return pltpu.roll(tile, shift % LANES, 1)


def spans(low, high, step=STEP):
    while low < high:
        yield low, min(step, high - low)
        low += step


def even_at(axis):
    return lax.rem(lax.axis_index(axis), 2) == 0


def own_source(mids, ups, downs, active):
    tiles = len(mids)
    rights = [roll(t, 1) for t in mids]
    lefts = [roll(t, -1) for t in mids]
    ids = lane_ids(mids[0].shape[0])
    found = []
    for k in range(tiles):
        before = jnp.where(ids == 0, rights[k - 1] if k else 0.0, rights[k])
        after = jnp.where(ids == LANES - 1, lefts[k + 1] if k + 1 < tiles else 0.0, lefts[k])
        beside = (ups[k] + downs[k]) + (before + after)
        found.append(active * (RELAX * mids[k] - NEAR * beside))
    return found


def staggered(items, begin, end, depth):
    waiting = []
    for item in items:
        waiting.append((item, begin(item)))
        if len(waiting) > depth:
            end(*waiting.pop(0))
    for each in waiting:
        end(*each)


def turn(src, shift, r, n):
    tiles = range(src.shape[0])
    return [roll(src[k, r : r + n, :], shift) for k in tiles], [roll(src[k, r : r + n, :], -shift) for k in tiles]


def swept(src, add, scale, shift, r, n, ring, turned, keep=None):
    tiles = src.shape[0]
    ids = lane_ids(n)
    mids = [src[k, r : r + n, :] for k in range(tiles)]
    rights, lefts = turned
    found = []
    for k in range(keep or tiles):
        before, after = rights[k], lefts[k]
        if tiles > 1 or not ring:
            before = jnp.where(ids < shift, rights[k - 1] if ring or k else 0.0, before)
            after = jnp.where(ids >= LANES - shift, lefts[(k + 1) % tiles] if ring or k + 1 < tiles else 0.0, after)
        beside = (src[k, r - 1 : r - 1 + n, :] + src[k, r + 1 : r + 1 + n, :]) + (before + after)
        more = add(k, r - 8, n) if callable(add) else add[k, r : r + n, :]
        found.append(scale[k] * (mids[k] + beside) + more)
    return mids, found


def restricted(rest, k, r, n, shift):
    total = rest[k, pl.ds(r, n, stride=2), :] + rest[k, pl.ds(r + 1, n, stride=2), :]
    even = (lane_ids(n) & shift) == 0
    return total + jnp.where(even, roll(total, -shift), roll(total, shift))


def strips(
    a_hbm, b_hbm, x_hbm, cover_ref, label_ref, even_ref, odd_ref,
    a_both, b_both, x_both, picked, other_a, other_b, built, sems,
):
    chans, block, cols = a_hbm.shape
    rows = HALO
    tiles = cols // LANES
    active = cover_ref[0, 0].astype(jnp.float32)
    marked = label_ref[0, 0].astype(jnp.float32)
    second = label_ref[0, 0] == 1
    eight = lane_ids(8)


    def fetches(step):
        low = pl.multiple_of(step * (block - HALO), 8)
        pairs = ((a_hbm, a_both), (b_hbm, b_both), (x_hbm, x_both))
        return [
            pltpu.make_async_copy(src.at[:, pl.ds(low, HALO), :], dst.at[step], sems.at[i, step])
            for i, (src, dst) in enumerate(pairs)
        ]

    for step in range(2):
        for fetch in fetches(step):
            fetch.start()

    def one_side(step, _):
        for fetch in fetches(step):
            fetch.wait()
        message(step, a_both.at[step], b_both.at[step], x_both.at[step])
        return 0

    def message(step, a_ref, b_ref, x_ref):
        top = step == 0
        low = jnp.where(top, 0, rows - STRIP)
        line = jnp.where(top, 0, rows - 1)
        spot = jnp.where(top, STRIP - 2, 0)
        for k in range(tiles):
            for edge in (7, 8 + rows):
                picked[k, edge : edge + 1, :] = jnp.zeros((1, LANES), jnp.float32)
        packed = jnp.zeros((8, LANES), jnp.float32)
        for c in range(chans):
            for k in range(tiles):
                at = pl.ds(k * LANES, LANES)
                for r, n in spans(0, rows):
                    x = x_ref[c, r : r + n, at]
                    from_a, from_b = a_ref[c, r : r + n, at] - x, b_ref[c, r : r + n, at] - x
                    other_a[k, r : r + n, :], other_b[k, r : r + n, :] = from_a, from_b
                    picked[k, 8 + r : 8 + r + n, :] = jnp.where(second, from_b, from_a)
            start = pl.multiple_of(low, 8)
            parts = [[picked[k, pl.ds(start + 8 + s, STRIP), :] for k in range(tiles)] for s in (0, -1, 1)]
            for k, found in enumerate(own_source(*parts, active)):
                built[k, c * STRIP : (c + 1) * STRIP, :] = found
            for k in range(tiles):
                built[k, pl.ds(c * STRIP + spot, 1), :] = other_a[k, pl.ds(line, 1), :]
                built[k, pl.ds(c * STRIP + spot + 1, 1), :] = other_b[k, pl.ds(line, 1), :]
            for t in range(STRIP // 8):
                lane = 4 * (chans * t + c)
                at = pl.ds(start + 8 * t, 8)
                packed = jnp.where(eight == lane, roll(other_a[0, at, :], lane), packed)
                packed = jnp.where(eight == lane + 1, roll(other_b[0, at, :], lane + 1), packed)
                packed = jnp.where(eight == lane + 2, roll(other_a[tiles - 1, at, :], lane + 3), packed)
                packed = jnp.where(eight == lane + 3, roll(other_b[tiles - 1, at, :], lane + 4), packed)
        built[0, chans * STRIP :, :] = packed
        for k in range(1, tiles):
            built[k, chans * STRIP :, :] = jnp.where(eight < HALF, active, marked)

        by_odd = top == even_at("group")

        @pl.when(by_odd)
        def _():
            odd_ref[...] = built[...]

        @pl.when(jnp.logical_not(by_odd))
        def _():
            even_ref[...] = built[...]

    lax.fori_loop(0, 2, one_side, 0)


def inside(a_ref, b_ref, x_ref, cover_ref, label_ref, source_ref, once_ref, seam_ref, coarse_ref, da, db, rest):
    chans, rows, cols = a_ref.shape
    tiles = cols // LANES
    active = cover_ref[0, 0].astype(jnp.float32)
    second = label_ref[0, 0] == 1
    for k in range(tiles):
        for buf in (da, db):
            buf[k, 0:8, :] = jnp.zeros((8, LANES), jnp.float32)
            buf[k, rows + 8 : rows + 16, :] = jnp.zeros((8, LANES), jnp.float32)
    scale = [active * NEAR] * tiles
    top, end = HALO, HALO + rows

    def pick(k, low, n):
        return jnp.where(second, db[k, low : low + n, :], da[k, low : low + n, :])

    def channel(c, _):
        for k in range(tiles):
            at = pl.ds(k * LANES, LANES)
            for r, n in spans(0, rows):
                x = x_ref[c, r : r + n, at]
                da[k, 8 + r : 8 + r + n, :] = a_ref[c, r : r + n, at] - x
                db[k, 8 + r : 8 + r + n, :] = b_ref[c, r : r + n, at] - x
        for r, n in spans(0, rows):
            parts = [[pick(k, 8 + s + r, n) for k in range(tiles)] for s in (0, -1, 1)]
            found = own_source(*parts, active)
            for k in range(tiles):
                source_ref[c, k, top + r : top + r + n, :] = found[k]
            ids = lane_ids(n)
            seam = jnp.where(ids < SEAM, found[0], roll(found[tiles - 1], HALF))
            at = pl.ds(8 + r, n)
            seam = jnp.where(ids == HALF, roll(da[tiles - 1, at, :], HALF + 1), seam)
            seam = jnp.where(ids == HALF + 1, roll(db[tiles - 1, at, :], HALF + 2), seam)
            seam = jnp.where(ids == LANES - 1, roll(da[0, at, :], -1), seam)
            seam_ref[c, top + r : top + r + n, :] = jnp.where(ids == LANES - 2, roll(db[0, at, :], -2), seam)
        source, once = source_ref.at[c], once_ref.at[c]

        def first(piece, turned):
            r, n = piece
            _, found = swept(source, source, scale, 1, r, n, False, turned)
            for k in range(tiles):
                once_ref[c, k, r : r + n, :] = found[k]

        def second_sweep(piece, turned):
            r, n = piece
            mids, found = swept(once, source, scale, 1, r, n, False, turned)
            for k in range(tiles):
                rest[k, r : r + n, :] = found[k] - mids[k]

        staggered(spans(top, end), lambda piece: turn(source, 1, *piece), first, 0)
        staggered(spans(top, end), lambda piece: turn(once, 1, *piece), second_sweep, 0)
        for r, n in spans(top // 2, end // 2):
            for k in range(tiles):
                coarse_ref[c, k, r : r + n, :] = restricted(rest, k, 2 * r, n, 1)
        return 0

    lax.fori_loop(0, chans, channel, 0)


def seam_units(chans, height):
    tiles_of = (height - 2 * FIRST) // 8
    for unit in range(chans * tiles_of):
        yield unit // tiles_of, FIRST + 8 * (unit % tiles_of), unit // 16, 8 * (unit % 16)


def message_rows(chans, height):
    quarter = height // 2
    cells = (chans // 2 * quarter + chans % 2 * quarter // 2) // 2
    units = -(-chans * ((height - 2 * FIRST) // 8) // 16) * 8
    return cells, units


def column_rows(chans, height):
    quarter = height // 2
    places = [(c, r, c + 1, r) for c in range(0, chans - 1, 2) for r in range(0, quarter, 8)]
    if chans % 2:
        places += [(chans - 1, r, chans - 1, r + quarter // 2) for r in range(0, quarter // 2, 8)]
    return places


def join_rows(
    source_in, once_in, seam_in, coarse_in, sent_even, sent_odd, got_even, got_odd, cover_ref, label_ref,
    source_ref, once_ref, seam_ref, coarse_ref, even_ref, odd_ref, rest, marks_ref, upper_got, lower_got, lines, left_out, right_out,
):
    chans, tiles, height, _ = source_ref.shape
    rows = height - 2 * HALO
    tail = chans * STRIP
    row_even, col_even = even_at("group"), even_at("blk")
    active = cover_ref[0, 0].astype(jnp.float32)
    marked = label_ref[0, 0].astype(jnp.float32)
    eight = lane_ids(8)

    def take(top, got):
        low = FIRST if top else HALO + rows
        their_spot = 0 if top else STRIP - 2
        my_spot = 0 if top else 2
        edge = HALO if top else HALO + rows - 1
        other = edge - 1 if top else edge + 1
        packed = got[0, tail:, :]
        marks = got[1, tail:, :]
        their_active = jnp.broadcast_to(marks[0:1, 0:1], (1, LANES))
        their_mark = jnp.broadcast_to(marks[0:1, HALF : HALF + 1], (1, LANES))
        band = 0 if top else 2
        marks_ref[band : band + 1, :] = their_active
        marks_ref[band + 3 : band + 4, :] = their_mark
        for c in range(chans):
            for k in range(tiles):
                source_ref[c, k, low : low + STRIP, :] = got[k, c * STRIP : (c + 1) * STRIP, :]
                their_a = got[k, c * STRIP + their_spot : c * STRIP + their_spot + 1, :]
                their_b = got[k, c * STRIP + their_spot + 1 : c * STRIP + their_spot + 2, :]
                my_a = lines[k, 4 * c + my_spot : 4 * c + my_spot + 1, :]
                my_b = lines[k, 4 * c + my_spot + 1 : 4 * c + my_spot + 2, :]
                for_mine = NEAR * active * jnp.where(marked == 1.0, their_b, their_a)
                for_theirs = NEAR * their_active * jnp.where(their_mark == 1.0, my_b, my_a)
                source_ref[c, k, edge : edge + 1, :] = source_ref[c, k, edge : edge + 1, :] - for_mine
                source_ref[c, k, other : other + 1, :] = source_ref[c, k, other : other + 1, :] - for_theirs
            for t in range(STRIP // 8):
                lane = 4 * (chans * t + c)
                last = roll(packed, HALF - lane - 2)
                once_a, once_b = roll(packed, LANES - 1 - lane), roll(packed, LANES - 2 - lane - 1)
                cells = jnp.where(eight == LANES - 1, once_a, jnp.where(eight == LANES - 2, once_b, last))
                r = low + 8 * t
                cells = jnp.where(eight < SEAM, source_ref[c, 0, r : r + 8, :], cells)
                end = roll(source_ref[c, tiles - 1, r : r + 8, :], HALF)
                seam_ref[c, r : r + 8, :] = jnp.where((eight >= HALF - SEAM) & (eight < HALF), end, cells)
            r = edge // 8 * 8
            cells = jnp.where(eight < SEAM, source_ref[c, 0, r : r + 8, :], seam_ref[c, r : r + 8, :])
            end = roll(source_ref[c, tiles - 1, r : r + 8, :], HALF)
            seam_ref[c, r : r + 8, :] = jnp.where((eight >= HALF - SEAM) & (eight < HALF), end, cells)

    def arrange(upper, lower, mine_up, mine_low):
        upper_got[...] = upper[...]
        lower_got[...] = lower[...]
        for c in range(chans):
            for k in range(tiles):
                lines[k, 4 * c : 4 * c + 2, :] = mine_up[k, (c + 1) * STRIP - 2 : (c + 1) * STRIP, :]
                lines[k, 4 * c + 2 : 4 * c + 4, :] = mine_low[k, c * STRIP : c * STRIP + 2, :]

    @pl.when(row_even)
    def _():
        arrange(got_odd, got_even, sent_odd, sent_even)

    @pl.when(jnp.logical_not(row_even))
    def _():
        arrange(got_even, got_odd, sent_even, sent_odd)

    take(True, upper_got)
    take(False, lower_got)
    marks_ref[1:2, :] = jnp.full((1, LANES), active)
    marks_ref[4:5, :] = jnp.full((1, LANES), marked)
    marks_ref[6:8, :] = jnp.zeros((2, LANES), jnp.float32)

    edges = ((FIRST, HALO, 0), (HALO, HALO + RIM, 1), (HALO + rows - RIM, HALO + rows, 1), (HALO + rows, height - FIRST, 2))
    spots = [(c, band, r, n) for c in range(chans) for low, high, band in edges for r, n in spans(low, high)]
    for stage in range(2):
        held = (source_ref, once_ref)[stage]

        def edge_sweep(spot, turned):
            c, band, r, n = spot
            scale = [jnp.broadcast_to(marks_ref[band : band + 1, :] * NEAR, (n, LANES))] * tiles
            mids, found = swept(held.at[c], source_ref.at[c], scale, 1, r, n, False, turned)
            for k in range(tiles):
                if stage == 0:
                    once_ref[c, k, r : r + n, :] = found[k]
                else:
                    rest[c, k, r : r + n, :] = found[k] - mids[k]

        staggered(spots, lambda spot: turn(held.at[spot[0]], 1, *spot[2:]), edge_sweep, 0)
    for c in range(chans):
        for low, high in ((FIRST, HALO + RIM), (HALO + rows - RIM, height - FIRST)):
            for k in range(tiles):
                coarse_ref[c, k, low // 2 : high // 2, :] = restricted(rest.at[c], k, low, (high - low) // 2, 1)
            zeros = jnp.zeros((FIRST // 2, LANES), jnp.float32)
        for k in range(tiles):
            coarse_ref[c, k, 0 : FIRST // 2, :] = zeros
            coarse_ref[c, k, (height - FIRST) // 2 : height // 2, :] = zeros

    cells, units = message_rows(chans, height)
    first_half = eight < HALF
    even_lane = (eight & 1) == 0

    def edge_cells(c, r):
        return jnp.where(first_half, coarse_ref[c, 0, r : r + 8, :], coarse_ref[c, tiles - 1, r : r + 8, :])

    def joined(place):
        c, r, d, s = place
        return jnp.where(even_lane, edge_cells(c, r), edge_cells(d, s))

    def pack(left, right):
        places = column_rows(chans, height)
        for t in range(cells // 8):
            upper, lower = joined(places[t]), joined(places[t + cells // 8])
            left[8 * t : 8 * t + 8, :] = jnp.where(first_half, upper, roll(lower, HALF))
            right[8 * t : 8 * t + 8, :] = jnp.where(first_half, roll(upper, HALF), lower)
        lefts = rights = jnp.zeros((8, LANES), jnp.float32)
        last = None
        for c, r, tile, lane in [*seam_units(chans, height), (None, None, -1, 0)]:
            if tile != last and last is not None:
                at = cells + 8 * last
                left[at : at + 8, :], right[at : at + 8, :] = lefts, rights
            last = tile
            if c is None:
                break
            value = seam_ref[c, r : r + 8, :]
            spot = (eight >= lane) & (eight < lane + 8)
            lefts = jnp.where(spot, roll(value, lane + 2), lefts)
            rights = jnp.where(spot, roll(value, lane - (HALF - SEAM)), rights)
        for out in (left, right):
            out[cells + units : cells + units + 8, :] = marks_ref[...]

    pack(left_out, right_out)

    @pl.when(col_even)
    def _():
        odd_ref[...] = left_out[...]
        even_ref[...] = right_out[...]

    @pl.when(jnp.logical_not(col_even))
    def _():
        even_ref[...] = left_out[...]
        odd_ref[...] = right_out[...]


def cycle(
    source_in, once_in, seam_in, coarse_in, sent_even, got_even, got_odd, x_ref, out_hbm,
    out_ref, sems, right_ref, left_ref, seam_source, seam_once, seam_rest, fine, fine_two, *bufs,
):
    chans, own_tiles, height, _ = source_in.shape
    rows = height - 2 * HALO
    tiles = own_tiles + 1
    cells, units = message_rows(chans, height)
    col_even = even_at("blk")
    eight = lane_ids(8)

    @pl.when(col_even)
    def _():
        right_ref[...] = got_even[...]
        left_ref[...] = got_odd[...]

    @pl.when(jnp.logical_not(col_even))
    def _():
        right_ref[...] = got_odd[...]
        left_ref[...] = got_even[...]

    at = cells + units

    def mark(ref, row):
        return jnp.broadcast_to(ref[at + row : at + row + 1, :], (8, LANES))

    own = [mark(sent_even, i) for i in range(6)]
    right = [mark(right_ref, i) for i in range(6)]
    left = [mark(left_ref, i) for i in range(6)]
    quarter3 = eight < HALF + HALF // 2
    first_half = eight < HALF

    def mixed(i):
        return jnp.where(first_half, own[i], jnp.where(quarter3, right[i], left[i]))

    seam_scale = [mixed(i) * NEAR for i in range(3)]
    seam_mark = [mixed(i + 3) == 1.0 for i in range(3)]
    own_scale = [own[i] * NEAR for i in range(3)]
    side_scale = [jnp.where(first_half, right[i], left[i]) * NEAR for i in range(3)]

    def wide(mask, n):
        return jnp.broadcast_to(mask[:1], (n, LANES))

    def over_rows(kinds, depth, r, n):
        full, halo = height >> depth, HALO >> depth
        ends = ((0, halo), (halo, full - halo), (full - halo, full))
        parts = [(max(a, r), min(b, r + n), kind) for (a, b), kind in zip(ends, kinds)]
        parts = [wide(kind, b - a) for a, b, kind in parts if b > a]
        return parts[0] if len(parts) == 1 else jnp.concatenate(parts, axis=0)

    def scales(depth, r, n):
        return [over_rows(own_scale, depth, r, n)] * own_tiles + [over_rows(side_scale, depth, r, n)]

    inner = (eight < SEAM) | ((eight >= HALF - SEAM) & (eight < HALF))
    outer = ((eight >= HALF) & (eight < HALF + SEAM)) | (eight >= LANES - SEAM)
    from_near = (eight == 0) | (eight == HALF - 1)
    from_own = (eight == HALF) | (eight == LANES - 1)
    up_one = (eight == HALF - 1) | (eight == LANES - 1)
    near_b = (eight == HALF - 2) | (eight == 1)
    right_unit = (eight >= HALF - 2) & (eight < HALF + SEAM)
    def unpack(unit):
        c, r, tile, lane = unit
        rights = roll(right_ref[cells + 8 * tile : cells + 8 * tile + 8, :], HALF - 2 - lane)
        lefts = roll(left_ref[cells + 8 * tile : cells + 8 * tile + 8, :], LANES - SEAM - lane)
        return rights, lefts

    def keep_near(unit, turned):
        c, r, _, _ = unit
        seam_rest[c, 0, r : r + 8, :] = jnp.where(right_unit, *turned)

    def second_cells(unit):
        c, r, _, _ = unit
        cells_b = jnp.where(near_b, seam_rest[c, 0, r : r + 8, :], seam_in[c, r : r + 8, :])
        return roll(cells_b, 1), roll(cells_b, -1)

    def put_seam(unit, turned):
        c, r, _, _ = unit
        band = 0 if r < HALO else 1 if r < HALO + rows else 2
        near, mine = seam_rest[c, 0, r : r + 8, :], seam_in[c, r : r + 8, :]
        value = jnp.where(inner, mine, jnp.where(outer, near, 0.0))
        border = jnp.where(seam_mark[band], jnp.where(up_one, *turned), jnp.where(from_near, near, mine))
        border = jnp.where(from_near | from_own, border, 0.0)
        seam_source[c, 0, r : r + 8, :] = value - seam_scale[band] * border

    units_of = list(seam_units(chans, height))
    staggered(units_of, unpack, keep_near, 24)
    staggered(units_of, second_cells, put_seam, 24)
    spots = [(c, r, n) for c in range(chans) for r, n in spans(FIRST, height - FIRST, 2 * STEP)]

    def seam_first(spot, turned):
        c, r, n = spot
        source = seam_source.at[c]
        _, found = swept(source, source, [over_rows(seam_scale, 0, r, n)], 1, r, n, True, turned)
        seam_once[c, 0, r : r + n, :] = found[0]

    def seam_second(spot, turned):
        c, r, n = spot
        scale = [over_rows(seam_scale, 0, r, n)]
        mids, found = swept(seam_once.at[c], seam_source.at[c], scale, 1, r, n, True, turned)
        seam_rest[c, 0, r : r + n, :] = found[0] - mids[0]

    staggered(spots, lambda spot: turn(seam_source.at[spot[0]], 1, *spot[1:]), seam_first, 0)
    staggered(spots, lambda spot: turn(seam_once.at[spot[0]], 1, *spot[1:]), seam_second, 0)

    one_src, one_once, one_two = bufs[0:3]
    half_rows = height // 2
    eights = lane_ids(8)
    even_lane = (eights & 1) == 0
    places = column_rows(chans, height)
    for t, (c, r, d, s) in enumerate(places):
        low, upper = (8 * t, True) if t < cells // 8 else (8 * t - cells, False)
        from_right, from_left = right_ref[low : low + 8, :], left_ref[low : low + 8, :]
        if upper:
            value = jnp.where(first_half, from_right, roll(from_left, HALF))
        else:
            value = jnp.where(first_half, roll(from_right, HALF), from_left)
        one_src[c, own_tiles, 8 + r : 16 + r, :] = jnp.where(even_lane, value, roll(value, 1))
        one_src[d, own_tiles, 8 + s : 16 + s, :] = jnp.where(even_lane, roll(value, -1), value)
    for c in range(chans):
        for r, n in spans(0, half_rows):
            for k in range(own_tiles):
                one_src[c, k, 8 + r : 8 + r + n, :] = coarse_in[c, k, r : r + n, :]
        for r, n in spans(FIRST // 2, half_rows - FIRST // 2):
            ids = lane_ids(n)
            seam = restricted(seam_rest.at[c], 0, 2 * r, n, 1)
            turned = roll(seam, HALF)
            at = pl.ds(8 + r, n)
            one_src[c, 0, at, :] = jnp.where(ids < 4, seam, one_src[c, 0, at, :])
            one_src[c, own_tiles - 1, at, :] = jnp.where(ids >= LANES - 4, turned, one_src[c, own_tiles - 1, at, :])
            side = jnp.where(ids < 4, turned, one_src[c, own_tiles, at, :])
            one_src[c, own_tiles, at, :] = jnp.where(ids >= LANES - 4, seam, side)

    def smooth(src, once, fields, depth, into, minus=False):
        def one_sweep(spot, turned):
            f, r, n = spot
            mids, found = swept(once.at[f], src.at[f], scales(depth, r, n), 1 << depth, 8 + r, n, True, turned)
            for k in range(tiles):
                into[f, k, 8 + r : 8 + r + n, :] = found[k] - mids[k] if minus else found[k]

        spots = [(f, r, n) for f in range(fields) for r, n in spans(0, height >> depth)]
        staggered(spots, lambda spot: turn(once.at[spot[0]], 1 << depth, 8 + spot[1], spot[2]), one_sweep, 0)

    def expand(fix, fields, depth, out, low, high, spread):
        for f in range(fields):
            for r, n in spans(low, high):
                scale = scales(depth + 1, r, n)
                for k in range(tiles):
                    value = fix[0 if spread else f, k, 8 + r : 8 + r + n, :]
                    if spread:
                        value = spread(value, f)
                    value = value * (scale[k] * (1.0 / NEAR))
                    out[f, k, pl.ds(8 + 2 * r, n, stride=2), :] = value
                    out[f, k, pl.ds(9 + 2 * r, n, stride=2), :] = value

    def add_fix(once, two, fields, depth, into):
        for f in range(fields):
            for r, n in spans(0, height >> depth):
                for k in range(tiles):
                    at = pl.ds(8 + r, n)
                    into[f, k, at, :] = once[f, k, at, :] + two[f, k, at, :]

    assert chans <= 4 and LEVELS >= 3

    def spread_channel(value, f):
        ids = lane_ids(value.shape[0])
        odd = (ids & 1) == 1
        pair = jnp.where(odd, value, roll(value, -1)) if f & 1 else jnp.where(odd, roll(value, 1), value)
        high = (ids & 2) == 2
        return jnp.where(high, pair, roll(pair, -2)) if f & 2 else jnp.where(high, roll(pair, 2), pair)

    def level(depth):
        src, once, two = bufs[3 * (depth - 1) : 3 * depth]
        fields = chans if depth == 1 else 1
        if depth == LEVELS - 1:
            held = src
            for sweep in range(1, COARSE):
                into = (once, two)[sweep % 2]
                smooth(src, held, fields, depth, into)
                held = into
            return held
        smooth(src, src, fields, depth, once)
        smooth(src, once, fields, depth, two, True)
        below = bufs[3 * depth]
        shift = 1 << depth
        for r, n in spans(0, height >> (depth + 1)):
            ids = lane_ids(n) & 3
            for k in range(tiles):
                value = None
                for f in range(fields):
                    total = restricted(two.at[f], k, 8 + 2 * r, n, shift)
                    value = total if value is None else jnp.where(ids == f, total, value)
                below[0, k, 8 + r : 8 + r + n, :] = value
        fix = level(depth + 1)
        expand(fix, fields, depth, two, 0, height >> (depth + 1), spread_channel if depth == 1 else None)
        add_fix(once, two, fields, depth, once)
        smooth(src, once, fields, depth, two)
        smooth(src, two, fields, depth, once)
        return once

    fix = level(1)
    low, high = HALO - RIM, HALO + rows + RIM

    def fine_source(c):
        def tile(k, r, n):
            ids = lane_ids(n)
            seam = seam_source[c, 0, r : r + n, :]
            if k == own_tiles:
                return jnp.where(ids < HALF, roll(seam, HALF), seam)
            value = source_in[c, k, r : r + n, :]
            if k == 0:
                value = jnp.where(ids == 0, seam, value)
            if k == own_tiles - 1:
                value = jnp.where(ids == LANES - 1, roll(seam, HALF), value)
            return value

        return tile

    def finish(c, _):
        for r, n in spans(low // 2, high // 2):
            scale = scales(1, r, n)
            for k in range(tiles):
                value = fix[c, k, 8 + r : 8 + r + n, :] * (scale[k] * (1.0 / NEAR))
                fine[k, pl.ds(8 + 2 * r, n, stride=2), :] = value
                fine[k, pl.ds(9 + 2 * r, n, stride=2), :] = value
        for r, n in spans(low, high):
            ids = lane_ids(n)
            seam = seam_once[c, 0, r : r + n, :]
            turned = roll(seam, HALF)
            at = pl.ds(8 + r, n)
            for k in range(own_tiles):
                value = once_in[c, k, r : r + n, :]
                if k == 0:
                    value = jnp.where(ids < 2, seam, value)
                if k == own_tiles - 1:
                    value = jnp.where(ids >= LANES - 2, turned, value)
                fine[k, at, :] = fine[k, at, :] + value
            fine[own_tiles, at, :] = fine[own_tiles, at, :] + jnp.where(ids < HALF, turned, seam)
        add = fine_source(c)

        def first(piece, turned):
            r, n = piece
            _, found = swept(fine, add, scales(0, r, n), 1, 8 + r, n, True, turned)
            for k in range(tiles):
                fine_two[k, 8 + r : 8 + r + n, :] = found[k]

        def last(piece, turned):
            r, n = piece
            _, found = swept(fine_two, add, scales(0, r, n), 1, 8 + r, n, True, turned, own_tiles)
            for k in range(own_tiles):
                at = pl.ds(k * LANES, LANES)
                out_ref[c, r - HALO : r - HALO + n, at] = x_ref[c, r - HALO : r - HALO + n, at] + found[k]

        staggered(spans(low, high), lambda piece: turn(fine, 1, 8 + piece[0], piece[1]), first, 0)
        staggered(spans(HALO, HALO + rows), lambda piece: turn(fine_two, 1, 8 + piece[0], piece[1]), last, 0)
        leave(c).start()
        return 0

    def leave(c):
        return pltpu.make_async_copy(out_ref.at[c], out_hbm.at[c], sems.at[c])

    lax.fori_loop(0, chans, finish, 0)
    for c in range(chans):
        leave(c).wait()


def swaps(count, odd):
    pairs = [(i, i + 1) for i in range(odd, count - 1, 2)]
    return pairs + [(j, i) for i, j in pairs]


def shards(image_a, image_b, initial, coverage, seam_label):
    chans, rows, cols = image_a.shape
    tiles = cols // LANES
    height = rows + 2 * HALO
    vmem = pl.BlockSpec(memory_space=pltpu.VMEM)
    smem = pl.BlockSpec(memory_space=pltpu.SMEM)
    hbm = pl.BlockSpec(memory_space=pltpu.HBM)
    f32 = jnp.float32
    sds = functools.partial(jax.ShapeDtypeStruct, dtype=f32)
    params = pltpu.CompilerParams(vmem_limit_bytes=40 * 1024 * 1024)
    group, blk = lax.axis_size("group"), lax.axis_size("blk")
    central = sds((chans, tiles, height, LANES))
    column = sds((chans, height, LANES))
    coarse = sds((chans, tiles, height // 2, LANES))
    upright = sds((tiles, chans * STRIP + 8, LANES))
    beside = sds((sum(message_rows(chans, height)) + 8, LANES))

    sent_even, sent_odd = pl.pallas_call(
        strips,
        out_shape=(upright, upright),
        in_specs=[hbm, hbm, hbm, smem, smem],
        out_specs=(vmem, vmem),
        scratch_shapes=[pltpu.VMEM((2, chans, HALO, cols), f32)] * 3
        + [pltpu.VMEM((tiles, HALO + 16, LANES), f32)]
        + [pltpu.VMEM((tiles, HALO, LANES), f32)] * 2
        + [pltpu.VMEM(upright.shape, f32), pltpu.SemaphoreType.DMA((3, 2))],
        compiler_params=pltpu.CompilerParams(vmem_limit_bytes=56_000_000),
        name="strips",
    )(image_a, image_b, initial, coverage, seam_label)
    got_even = lax.ppermute(sent_even, "group", swaps(group, 0))
    got_odd = lax.ppermute(sent_odd, "group", swaps(group, 1))

    source, once, seam, coarser = pl.pallas_call(
        inside,
        out_shape=(central, central, column, coarse),
        in_specs=[vmem, vmem, vmem, smem, smem],
        out_specs=(vmem,) * 4,
        scratch_shapes=[pltpu.VMEM((tiles, rows + 16, LANES), f32)] * 2 + [pltpu.VMEM((tiles, height, LANES), f32)],
        compiler_params=params,
        cost_estimate=pl.CostEstimate(flops=200_000_000, bytes_accessed=4_000_000, transcendentals=0),
        name="inside",
    )(image_a, image_b, initial, coverage, seam_label)

    source, once, seam, coarser, sent_even, sent_odd = pl.pallas_call(
        join_rows,
        out_shape=(central, central, column, coarse, beside, beside),
        in_specs=[vmem] * 8 + [smem] * 2,
        out_specs=(vmem,) * 6,
        input_output_aliases={0: 0, 1: 1, 2: 2, 3: 3},
        scratch_shapes=[pltpu.VMEM(central.shape, f32), pltpu.VMEM((8, LANES), f32)]
        + [pltpu.VMEM(upright.shape, f32)] * 2
        + [pltpu.VMEM((tiles, 4 * chans, LANES), f32)]
        + [pltpu.VMEM(beside.shape, f32)] * 2,
        compiler_params=params,
        name="join_rows",
    )(source, once, seam, coarser, sent_even, sent_odd, got_even, got_odd, coverage, seam_label)
    got_even = lax.ppermute(sent_even, "blk", swaps(blk, 0))
    got_odd = lax.ppermute(sent_odd, "blk", swaps(blk, 1))

    scratch = [pltpu.VMEM(image_a.shape, f32), pltpu.SemaphoreType.DMA((chans,))]
    scratch += [pltpu.VMEM(beside.shape, f32)] * 2 + [pltpu.VMEM((chans, 1, height, LANES), f32)] * 3
    scratch += [pltpu.VMEM((tiles + 1, height + 16, LANES), f32)] * 2
    for depth in range(1, LEVELS):
        fields = chans if depth == 1 else 1
        scratch += [pltpu.VMEM((fields, tiles + 1, (height >> depth) + 16, LANES), f32)] * 3
    return pl.pallas_call(
        cycle,
        out_shape=sds((chans, rows, cols)),
        in_specs=[vmem] * 8,
        out_specs=hbm,
        scratch_shapes=scratch,
        compiler_params=params,
        name="cycle",
    )(source, once, seam, coarser, sent_even, got_even, got_odd, initial)


def solution(mesh):
    placed = (
        P(None, "group", "blk"),
        P(None, "group", "blk"),
        P(None, "group", "blk"),
        P("group", "blk"),
        P("group", "blk"),
    )
    return jax.shard_map(
        shards, mesh=mesh, in_specs=placed, out_specs=P(None, "group", "blk"), check_vma=False
    )
```

```python
import functools

import jax
import jax.numpy as jnp
from jax import lax
from jax.experimental import pallas as pl
from jax.experimental.pallas import tpu as pltpu
from jax.sharding import PartitionSpec as P

LEVELS = 4
NU = 2
COARSE = 4
RELAX = 0.8
NEAR = 0.25 * RELAX

LANES = 128
HALF = LANES // 2
HALO = 64
STEP = 96


def source_reach():
    need = 0
    for _ in range(LEVELS - 1):
        need = -(-(need + NU) // 2)
    need += COARSE - 1
    for _ in range(LEVELS - 1):
        need = 2 * need + NU
    return need


REACH = source_reach()
STRIP = REACH + 2
assert STRIP % 8 == 0 and STRIP <= HALO
FIRST = HALO - STRIP
RIM = 8
SEAM = 6
QUARTER = LANES // 4
LEFT, RIGHT = 8, 24


def lane_ids(rows):
    return lax.broadcasted_iota(jnp.int32, (rows, LANES), 1)


def roll(tile, shift):
    return pltpu.roll(tile, shift % LANES, 1)


def spans(low, high, step=STEP):
    while low < high:
        yield low, min(step, high - low)
        low += step


def even_at(axis):
    return lax.rem(lax.axis_index(axis), 2) == 0


def own_source(mids, ups, downs, active):
    tiles = len(mids)
    rights = [roll(t, 1) for t in mids]
    lefts = [roll(t, -1) for t in mids]
    ids = lane_ids(mids[0].shape[0])
    found = []
    for k in range(tiles):
        before = jnp.where(ids == 0, rights[k - 1] if k else 0.0, rights[k])
        after = jnp.where(ids == LANES - 1, lefts[k + 1] if k + 1 < tiles else 0.0, lefts[k])
        beside = (ups[k] + downs[k]) + (before + after)
        found.append(active * (RELAX * mids[k] - NEAR * beside))
    return found


def staggered(items, begin, end, depth):
    waiting = []
    for item in items:
        waiting.append((item, begin(item)))
        if len(waiting) > depth:
            end(*waiting.pop(0))
    for each in waiting:
        end(*each)


def turn(src, shift, r, n):
    tiles = range(src.shape[0])
    return [roll(src[k, r : r + n, :], shift) for k in tiles], [roll(src[k, r : r + n, :], -shift) for k in tiles]


def swept(src, add, scale, shift, r, n, ring, turned, keep=None):
    tiles = src.shape[0]
    ids = lane_ids(n)
    mids = [src[k, r : r + n, :] for k in range(tiles)]
    rights, lefts = turned
    found = []
    for k in range(keep or tiles):
        before, after = rights[k], lefts[k]
        if tiles > 1 or not ring:
            before = jnp.where(ids < shift, rights[k - 1] if ring or k else 0.0, before)
            after = jnp.where(ids >= LANES - shift, lefts[(k + 1) % tiles] if ring or k + 1 < tiles else 0.0, after)
        beside = (src[k, r - 1 : r - 1 + n, :] + src[k, r + 1 : r + 1 + n, :]) + (before + after)
        more = add(k, r - 8, n) if callable(add) else add[k, r : r + n, :]
        found.append(scale[k] * (mids[k] + beside) + more)
    return mids, found


def restricted(rest, k, r, n, shift):
    total = rest[k, pl.ds(r, n, stride=2), :] + rest[k, pl.ds(r + 1, n, stride=2), :]
    even = (lane_ids(n) & shift) == 0
    return total + jnp.where(even, roll(total, -shift), roll(total, shift))


def strips(
    a_hbm, b_hbm, x_hbm, cover_ref, label_ref, even_ref, odd_ref,
    a_both, b_both, x_both, picked, other_a, other_b, built, sems,
):
    chans, block, cols = a_hbm.shape
    rows = HALO
    tiles = cols // LANES
    active = cover_ref[0, 0].astype(jnp.float32)
    marked = label_ref[0, 0].astype(jnp.float32)
    second = label_ref[0, 0] == 1
    eight = lane_ids(8)


    def fetches(step):
        low = pl.multiple_of(step * (block - HALO), 8)
        pairs = ((a_hbm, a_both), (b_hbm, b_both), (x_hbm, x_both))
        return [
            pltpu.make_async_copy(src.at[:, pl.ds(low, HALO), :], dst.at[step], sems.at[i, step])
            for i, (src, dst) in enumerate(pairs)
        ]

    for step in range(2):
        for fetch in fetches(step):
            fetch.start()

    def one_side(step, _):
        for fetch in fetches(step):
            fetch.wait()
        message(step, a_both.at[step], b_both.at[step], x_both.at[step])
        return 0

    def message(step, a_ref, b_ref, x_ref):
        top = step == 0
        low = jnp.where(top, 0, rows - STRIP)
        line = jnp.where(top, 0, rows - 1)
        spot = jnp.where(top, STRIP - 2, 0)
        for k in range(tiles):
            for edge in (7, 8 + rows):
                picked[k, edge : edge + 1, :] = jnp.zeros((1, LANES), jnp.float32)
        packed = jnp.zeros((8, LANES), jnp.float32)
        for c in range(chans):
            for k in range(tiles):
                at = pl.ds(k * LANES, LANES)
                for r, n in spans(0, rows):
                    x = x_ref[c, r : r + n, at]
                    from_a, from_b = a_ref[c, r : r + n, at] - x, b_ref[c, r : r + n, at] - x
                    other_a[k, r : r + n, :], other_b[k, r : r + n, :] = from_a, from_b
                    picked[k, 8 + r : 8 + r + n, :] = jnp.where(second, from_b, from_a)
            start = pl.multiple_of(low, 8)
            parts = [[picked[k, pl.ds(start + 8 + s, STRIP), :] for k in range(tiles)] for s in (0, -1, 1)]
            for k, found in enumerate(own_source(*parts, active)):
                built[k, c * STRIP : (c + 1) * STRIP, :] = found
            for k in range(tiles):
                built[k, pl.ds(c * STRIP + spot, 1), :] = other_a[k, pl.ds(line, 1), :]
                built[k, pl.ds(c * STRIP + spot + 1, 1), :] = other_b[k, pl.ds(line, 1), :]
            for t in range(STRIP // 8):
                lane = QUARTER * c + 4 * t
                at = pl.ds(start + 8 * t, 8)
                packed = jnp.where(eight == lane, roll(other_b[0, at, :], lane), packed)
                packed = jnp.where(eight == lane + 1, roll(other_a[0, at, :], lane + 1), packed)
                packed = jnp.where(eight == lane + 2, roll(other_a[tiles - 1, at, :], lane + 3), packed)
                packed = jnp.where(eight == lane + 3, roll(other_b[tiles - 1, at, :], lane + 4), packed)
        built[0, chans * STRIP :, :] = packed
        for k in range(1, tiles):
            built[k, chans * STRIP :, :] = jnp.where(eight < HALF, active, marked)

        by_odd = top == even_at("group")

        @pl.when(by_odd)
        def _():
            odd_ref[...] = built[...]

        @pl.when(jnp.logical_not(by_odd))
        def _():
            even_ref[...] = built[...]

    lax.fori_loop(0, 2, one_side, 0)


def inside(a_ref, b_ref, x_ref, cover_ref, label_ref, source_ref, once_ref, seam_ref, coarse_ref, da, db, rest):
    chans, rows, cols = a_ref.shape
    tiles = cols // LANES
    active = cover_ref[0, 0].astype(jnp.float32)
    second = label_ref[0, 0] == 1
    for k in range(tiles):
        for buf in (da, db):
            buf[k, 0:8, :] = jnp.zeros((8, LANES), jnp.float32)
            buf[k, rows + 8 : rows + 16, :] = jnp.zeros((8, LANES), jnp.float32)
    scale = [active * NEAR] * tiles
    top, end = HALO, HALO + rows

    def pick(k, low, n):
        return jnp.where(second, db[k, low : low + n, :], da[k, low : low + n, :])

    seam_ref[...] = jnp.zeros(seam_ref.shape, jnp.float32)

    def channel(c, _):
        for k in range(tiles):
            at = pl.ds(k * LANES, LANES)
            for r, n in spans(0, rows):
                x = x_ref[c, r : r + n, at]
                da[k, 8 + r : 8 + r + n, :] = a_ref[c, r : r + n, at] - x
                db[k, 8 + r : 8 + r + n, :] = b_ref[c, r : r + n, at] - x
        for r, n in spans(0, rows):
            parts = [[pick(k, 8 + s + r, n) for k in range(tiles)] for s in (0, -1, 1)]
            found = own_source(*parts, active)
            for k in range(tiles):
                source_ref[c, k, top + r : top + r + n, :] = found[k]
            ids = lane_ids(n)
            base = QUARTER * c
            at = pl.ds(8 + r, n)
            seam = pltpu.roll(found[0], base + LEFT, 1)
            for source, cell, lane in (
                (found[tiles - 1], LANES - SEAM, RIGHT - SEAM),
                (da[0, at, :], 0, LEFT - 1),
                (db[0, at, :], 0, LEFT - 2),
                (da[tiles - 1, at, :], LANES - 1, RIGHT),
                (db[tiles - 1, at, :], LANES - 1, RIGHT + 1),
            ):
                spot = (ids >= base + lane) & (ids < base + lane + (SEAM if cell == LANES - SEAM else 1))
                seam = jnp.where(spot, pltpu.roll(source, base + lane + (LANES - cell) % LANES, 1), seam)
            at = pl.ds(top + r, n)
            mine = (ids >= base + LEFT - 2) & (ids < base + RIGHT + 2)
            mine = mine & ((ids < base + LEFT + SEAM) | (ids >= base + RIGHT - SEAM))
            seam_ref[at, :] = jnp.where(mine, seam, seam_ref[at, :])
        source, once = source_ref.at[c], once_ref.at[c]

        def first(piece, turned):
            r, n = piece
            _, found = swept(source, source, scale, 1, r, n, False, turned)
            for k in range(tiles):
                once_ref[c, k, r : r + n, :] = found[k]

        def second_sweep(piece, turned):
            r, n = piece
            mids, found = swept(once, source, scale, 1, r, n, False, turned)
            for k in range(tiles):
                rest[k, r : r + n, :] = found[k] - mids[k]

        staggered(spans(top, end), lambda piece: turn(source, 1, *piece), first, 0)
        staggered(spans(top, end), lambda piece: turn(once, 1, *piece), second_sweep, 0)
        for r, n in spans(top // 2, end // 2):
            for k in range(tiles):
                coarse_ref[c, k, r : r + n, :] = restricted(rest, k, 2 * r, n, 1)
        return 0

    lax.fori_loop(0, chans, channel, 0)


def seam_units(height):
    for t in range((height - 2 * FIRST) // 8):
        yield FIRST + 8 * t, t // 4, t % 4


def message_rows(chans, height):
    quarter = height // 2
    cells = (chans // 2 * quarter + chans % 2 * quarter // 2) // 2
    return cells, -(-(height - 2 * FIRST) // 32) * 8


def column_rows(chans, height):
    quarter = height // 2
    places = [(c, r, c + 1, r) for c in range(0, chans - 1, 2) for r in range(0, quarter, 8)]
    if chans % 2:
        places += [(chans - 1, r, chans - 1, r + quarter // 2) for r in range(0, quarter // 2, 8)]
    return places


def join_rows(
    source_in, once_in, seam_in, coarse_in, sent_even, sent_odd, got_even, got_odd, cover_ref, label_ref,
    source_ref, once_ref, seam_ref, coarse_ref, even_ref, odd_ref, rest, marks_ref, upper_got, lower_got, lines, left_out, right_out,
):
    chans, tiles, height, _ = source_ref.shape
    rows = height - 2 * HALO
    tail = chans * STRIP
    row_even, col_even = even_at("group"), even_at("blk")
    active = cover_ref[0, 0].astype(jnp.float32)
    marked = label_ref[0, 0].astype(jnp.float32)
    eight = lane_ids(8)

    place = eight & (QUARTER - 1)

    def take(top, got):
        low = FIRST if top else HALO + rows
        their_spot = 0 if top else STRIP - 2
        my_spot = 0 if top else 2
        edge = HALO if top else HALO + rows - 1
        other = edge - 1 if top else edge + 1
        packed = got[0, tail:, :]
        marks = got[1, tail:, :]
        their_active = jnp.broadcast_to(marks[0:1, 0:1], (1, LANES))
        their_mark = jnp.broadcast_to(marks[0:1, HALF : HALF + 1], (1, LANES))
        band = 0 if top else 2
        marks_ref[band : band + 1, :] = their_active
        marks_ref[band + 3 : band + 4, :] = their_mark
        for c in range(chans):
            for k in range(tiles):
                source_ref[c, k, low : low + STRIP, :] = got[k, c * STRIP : (c + 1) * STRIP, :]
                their_a = got[k, c * STRIP + their_spot : c * STRIP + their_spot + 1, :]
                their_b = got[k, c * STRIP + their_spot + 1 : c * STRIP + their_spot + 2, :]
                my_a = lines[k, 4 * c + my_spot : 4 * c + my_spot + 1, :]
                my_b = lines[k, 4 * c + my_spot + 1 : 4 * c + my_spot + 2, :]
                for_mine = NEAR * active * jnp.where(marked == 1.0, their_b, their_a)
                for_theirs = NEAR * their_active * jnp.where(their_mark == 1.0, my_b, my_a)
                source_ref[c, k, edge : edge + 1, :] = source_ref[c, k, edge : edge + 1, :] - for_mine
                source_ref[c, k, other : other + 1, :] = source_ref[c, k, other : other + 1, :] - for_theirs

        def seam_of(r, cells):
            for c in range(chans):
                base = QUARTER * c
                spot = (eight >= base + LEFT) & (eight < base + LEFT + SEAM)
                cells = jnp.where(spot, roll(source_ref[c, 0, r : r + 8, :], base + LEFT), cells)
                spot = (eight >= base + RIGHT - SEAM) & (eight < base + RIGHT)
                cells = jnp.where(spot, roll(source_ref[c, tiles - 1, r : r + 8, :], base + RIGHT), cells)
            seam_ref[r : r + 8, :] = cells

        for t in range(STRIP // 8):
            firsts, lasts = roll(packed, LEFT - 2 - 4 * t), roll(packed, RIGHT - 2 - 4 * t)
            cells = jnp.where((place == LEFT - 2) | (place == LEFT - 1), firsts, 0.0)
            cells = jnp.where((place == RIGHT) | (place == RIGHT + 1), lasts, cells)
            seam_of(low + 8 * t, jnp.where(eight < QUARTER * chans, cells, 0.0))
        r = edge // 8 * 8
        seam_of(r, seam_ref[r : r + 8, :])

    def arrange(upper, lower, mine_up, mine_low):
        upper_got[...] = upper[...]
        lower_got[...] = lower[...]
        for c in range(chans):
            for k in range(tiles):
                lines[k, 4 * c : 4 * c + 2, :] = mine_up[k, (c + 1) * STRIP - 2 : (c + 1) * STRIP, :]
                lines[k, 4 * c + 2 : 4 * c + 4, :] = mine_low[k, c * STRIP : c * STRIP + 2, :]

    @pl.when(row_even)
    def _():
        arrange(got_odd, got_even, sent_odd, sent_even)

    @pl.when(jnp.logical_not(row_even))
    def _():
        arrange(got_even, got_odd, sent_even, sent_odd)

    take(True, upper_got)
    take(False, lower_got)
    marks_ref[1:2, :] = jnp.full((1, LANES), active)
    marks_ref[4:5, :] = jnp.full((1, LANES), marked)
    marks_ref[6:8, :] = jnp.zeros((2, LANES), jnp.float32)

    edges = ((FIRST, HALO, 0), (HALO, HALO + RIM, 1), (HALO + rows - RIM, HALO + rows, 1), (HALO + rows, height - FIRST, 2))
    spots = [(c, band, r, n) for c in range(chans) for low, high, band in edges for r, n in spans(low, high)]
    for stage in range(2):
        held = (source_ref, once_ref)[stage]

        def edge_sweep(spot, turned):
            c, band, r, n = spot
            scale = [jnp.broadcast_to(marks_ref[band : band + 1, :] * NEAR, (n, LANES))] * tiles
            mids, found = swept(held.at[c], source_ref.at[c], scale, 1, r, n, False, turned)
            for k in range(tiles):
                if stage == 0:
                    once_ref[c, k, r : r + n, :] = found[k]
                else:
                    rest[c, k, r : r + n, :] = found[k] - mids[k]

        staggered(spots, lambda spot: turn(held.at[spot[0]], 1, *spot[2:]), edge_sweep, 0)
    for c in range(chans):
        for low, high in ((FIRST, HALO + RIM), (HALO + rows - RIM, height - FIRST)):
            for k in range(tiles):
                coarse_ref[c, k, low // 2 : high // 2, :] = restricted(rest.at[c], k, low, (high - low) // 2, 1)
            zeros = jnp.zeros((FIRST // 2, LANES), jnp.float32)
        for k in range(tiles):
            coarse_ref[c, k, 0 : FIRST // 2, :] = zeros
            coarse_ref[c, k, (height - FIRST) // 2 : height // 2, :] = zeros

    cells, units = message_rows(chans, height)
    first_half = eight < HALF
    even_lane = (eight & 1) == 0

    def edge_cells(c, r):
        return jnp.where(first_half, coarse_ref[c, 0, r : r + 8, :], coarse_ref[c, tiles - 1, r : r + 8, :])

    def joined(place):
        c, r, d, s = place
        return jnp.where(even_lane, edge_cells(c, r), edge_cells(d, s))

    def pack(left, right):
        places = column_rows(chans, height)
        for t in range(cells // 8):
            upper, lower = joined(places[t]), joined(places[t + cells // 8])
            left[8 * t : 8 * t + 8, :] = jnp.where(first_half, upper, roll(lower, HALF))
            right[8 * t : 8 * t + 8, :] = jnp.where(first_half, roll(upper, HALF), lower)
        lefts = rights = jnp.zeros((8, LANES), jnp.float32)
        for r, tile, slot in seam_units(height):
            value = seam_ref[r : r + 8, :]
            spot = (place >> 3) == slot
            lefts = jnp.where(spot, roll(value, 8 * slot - (LEFT - 2)), lefts)
            rights = jnp.where(spot, roll(value, 8 * slot - (RIGHT - SEAM)), rights)
            at = cells + 8 * tile
            left[at : at + 8, :], right[at : at + 8, :] = lefts, rights
        for out in (left, right):
            out[cells + units : cells + units + 8, :] = marks_ref[...]

    pack(left_out, right_out)

    @pl.when(col_even)
    def _():
        odd_ref[...] = left_out[...]
        even_ref[...] = right_out[...]

    @pl.when(jnp.logical_not(col_even))
    def _():
        even_ref[...] = left_out[...]
        odd_ref[...] = right_out[...]


def cycle(
    source_in, once_in, seam_in, coarse_in, sent_even, got_even, got_odd, x_ref, out_hbm,
    out_ref, sems, right_ref, left_ref, seam_source, seam_once, seam_rest, fine, fine_two, fix, *bufs,
):
    chans, own_tiles, height, _ = source_in.shape
    rows = height - 2 * HALO
    tiles = own_tiles + 1
    cells, units = message_rows(chans, height)
    col_even = even_at("blk")
    eight = lane_ids(8)

    @pl.when(col_even)
    def _():
        right_ref[...] = got_even[...]
        left_ref[...] = got_odd[...]

    @pl.when(jnp.logical_not(col_even))
    def _():
        right_ref[...] = got_odd[...]
        left_ref[...] = got_even[...]

    at = cells + units

    def mark(ref, row):
        return jnp.broadcast_to(ref[at + row : at + row + 1, :], (8, LANES))

    own = [mark(sent_even, i) for i in range(6)]
    right = [mark(right_ref, i) for i in range(6)]
    left = [mark(left_ref, i) for i in range(6)]
    first_half = eight < HALF
    place = eight & (QUARTER - 1)

    def mixed(i):
        return jnp.where(place < LEFT, left[i], jnp.where(place < RIGHT, own[i], right[i]))

    seam_scale = [jnp.where(eight < QUARTER * chans, mixed(i), 0.0) * NEAR for i in range(3)]
    seam_mark = [mixed(i + 3) == 1.0 for i in range(3)]
    own_scale = [own[i] * NEAR for i in range(3)]
    side_scale = [jnp.where(first_half, right[i], left[i]) * NEAR for i in range(3)]

    def wide(mask, n):
        return jnp.broadcast_to(mask[:1], (n, LANES))

    def over_rows(kinds, depth, r, n):
        full, halo = height >> depth, HALO >> depth
        ends = ((0, halo), (halo, full - halo), (full - halo, full))
        parts = [(max(a, r), min(b, r + n), kind) for (a, b), kind in zip(ends, kinds)]
        parts = [wide(kind, b - a) for a, b, kind in parts if b > a]
        return parts[0] if len(parts) == 1 else jnp.concatenate(parts, axis=0)

    def scales(depth, r, n):
        return [over_rows(own_scale, depth, r, n)] * own_tiles + [over_rows(side_scale, depth, r, n)]

    inner = ((place >= LEFT) & (place < LEFT + SEAM)) | ((place >= RIGHT - SEAM) & (place < RIGHT))
    outer = ((place >= LEFT - SEAM) & (place < LEFT)) | ((place >= RIGHT) & (place < RIGHT + SEAM))
    from_near = (place == LEFT) | (place == RIGHT - 1)
    from_own = (place == LEFT - 1) | (place == RIGHT)
    up_one = (place == LEFT - 1) | (place == RIGHT - 1)
    near_b = (place == LEFT + 1) | (place == RIGHT - 2)
    right_unit = place >= RIGHT - 2

    def unpack(unit):
        r, tile, slot = unit
        rights = roll(right_ref[cells + 8 * tile : cells + 8 * tile + 8, :], RIGHT - 2 - 8 * slot)
        lefts = roll(left_ref[cells + 8 * tile : cells + 8 * tile + 8, :], LEFT - SEAM - 8 * slot)
        return rights, lefts

    def keep_near(unit, turned):
        r = unit[0]
        seam_rest[0, r : r + 8, :] = jnp.where(right_unit, *turned)

    def second_cells(unit):
        r = unit[0]
        cells_b = jnp.where(near_b, seam_rest[0, r : r + 8, :], seam_in[r : r + 8, :])
        return roll(cells_b, 1), roll(cells_b, -1)

    def put_seam(unit, turned):
        r = unit[0]
        band = 0 if r < HALO else 1 if r < HALO + rows else 2
        near, mine = seam_rest[0, r : r + 8, :], seam_in[r : r + 8, :]
        value = jnp.where(inner, mine, jnp.where(outer, near, 0.0))
        border = jnp.where(seam_mark[band], jnp.where(up_one, *turned), jnp.where(from_near, near, mine))
        border = jnp.where(from_near | from_own, border, 0.0)
        seam_source[0, r : r + 8, :] = value - seam_scale[band] * border

    staggered(seam_units(height), unpack, keep_near, 24)
    staggered(seam_units(height), second_cells, put_seam, 24)
    for r, n in spans(FIRST, height - FIRST, height):
        _, found = swept(
            seam_source, seam_source, [over_rows(seam_scale, 0, r, n)], 1, r, n, True, turn(seam_source, 1, r, n)
        )
        seam_once[0, r : r + n, :] = found[0]
        mids, found = swept(
            seam_once, seam_source, [over_rows(seam_scale, 0, r, n)], 1, r, n, True, turn(seam_once, 1, r, n)
        )
        seam_rest[0, r : r + n, :] = found[0] - mids[0]

    one_src, one_once, one_two = bufs[0:3]
    half_rows = height // 2
    eights = lane_ids(8)
    even_lane = (eights & 1) == 0
    places = column_rows(chans, height)
    for t, (c, r, d, s) in enumerate(places):
        low, upper = (8 * t, True) if t < cells // 8 else (8 * t - cells, False)
        from_right, from_left = right_ref[low : low + 8, :], left_ref[low : low + 8, :]
        if upper:
            value = jnp.where(first_half, from_right, roll(from_left, HALF))
        else:
            value = jnp.where(first_half, roll(from_right, HALF), from_left)
        if c == d:
            one_src[c // 2, own_tiles, 8 + r : 16 + r, :] = jnp.where(even_lane, value, roll(value, 1))
            one_src[c // 2, own_tiles, 8 + s : 16 + s, :] = jnp.where(even_lane, roll(value, -1), value)
        else:
            one_src[c // 2, own_tiles, 8 + r : 16 + r, :] = value

    pairs = [(c, min(c + 1, chans - 1)) for c in range(0, chans, 2)]

    def paired(of, pair, n):
        first, second = pair
        return of(first) if first == second else jnp.where((lane_ids(n) & 1) == 0, of(first), of(second))

    for f, pair in enumerate(pairs):
        for r, n in spans(0, half_rows):
            for k in range(own_tiles):
                one_src[f, k, 8 + r : 8 + r + n, :] = paired(lambda c: coarse_in[c, k, r : r + n, :], pair, n)
    for r, n in spans(FIRST // 2, half_rows - FIRST // 2):
        ids = lane_ids(n)
        seam = restricted(seam_rest, 0, 2 * r, n, 1)
        at = pl.ds(8 + r, n)
        for f, pair in enumerate(pairs):
            by_left = paired(lambda c: roll(seam, -QUARTER * c - LEFT), pair, n)
            by_right = paired(lambda c: roll(seam, -QUARTER * c - RIGHT), pair, n)
            one_src[f, 0, at, :] = jnp.where(ids < 4, by_left, one_src[f, 0, at, :])
            inner_end = one_src[f, own_tiles - 1, at, :]
            one_src[f, own_tiles - 1, at, :] = jnp.where(ids >= LANES - 4, by_right, inner_end)
            side = jnp.where(ids < 4, by_right, one_src[f, own_tiles, at, :])
            one_src[f, own_tiles, at, :] = jnp.where(ids >= LANES - 4, by_left, side)

    def smooth(src, once, fields, depth, into, minus=False):
        def one_sweep(spot, turned):
            f, r, n = spot
            mids, found = swept(once.at[f], src.at[f], scales(depth, r, n), 1 << depth, 8 + r, n, True, turned)
            for k in range(tiles):
                into[f, k, 8 + r : 8 + r + n, :] = found[k] - mids[k] if minus else found[k]

        spots = [(f, r, n) for f in range(fields) for r, n in spans(0, height >> depth)]
        staggered(spots, lambda spot: turn(once.at[spot[0]], 1 << depth, 8 + spot[1], spot[2]), one_sweep, 0)

    def expand(fix, fields, depth, out, low, high, spread):
        for f in range(fields):
            for r, n in spans(low, high):
                scale = scales(depth + 1, r, n)
                for k in range(tiles):
                    value = fix[0 if spread else f, k, 8 + r : 8 + r + n, :]
                    if spread:
                        value = spread(value, f)
                    value = value * (scale[k] * (1.0 / NEAR))
                    out[f, k, pl.ds(8 + 2 * r, n, stride=2), :] = value
                    out[f, k, pl.ds(9 + 2 * r, n, stride=2), :] = value

    def add_fix(once, two, fields, depth, into):
        for f in range(fields):
            for r, n in spans(0, height >> depth):
                for k in range(tiles):
                    at = pl.ds(8 + r, n)
                    into[f, k, at, :] = once[f, k, at, :] + two[f, k, at, :]

    assert chans <= 4 and LEVELS >= 3

    def spread_pair(value, f):
        high = (lane_ids(value.shape[0]) & 2) == 2
        return jnp.where(high, value, roll(value, -2)) if f else jnp.where(high, roll(value, 2), value)

    def level(depth):
        src, once, two = bufs[3 * (depth - 1) : 3 * depth]
        fields = len(pairs) if depth == 1 else 1
        if depth == LEVELS - 1:
            held = src
            for sweep in range(1, COARSE):
                into = (once, two)[sweep % 2]
                smooth(src, held, fields, depth, into)
                held = into
            return held
        smooth(src, src, fields, depth, once)
        smooth(src, once, fields, depth, two, True)
        below = bufs[3 * depth]
        shift = 1 << depth
        for r, n in spans(0, height >> (depth + 1)):
            half = (lane_ids(n) & 2) >> 1
            for k in range(tiles):
                value = None
                for f in range(fields):
                    total = restricted(two.at[f], k, 8 + 2 * r, n, shift)
                    value = total if value is None else jnp.where(half == f, total, value)
                below[0, k, 8 + r : 8 + r + n, :] = value
        fix = level(depth + 1)
        expand(fix, fields, depth, two, 0, height >> (depth + 1), spread_pair if depth == 1 else None)
        add_fix(once, two, fields, depth, once)
        smooth(src, once, fields, depth, two)
        smooth(src, two, fields, depth, once)
        return once

    paired_fix = level(1)
    low, high = HALO - RIM, HALO + rows + RIM
    for f, (even, odd) in enumerate(pairs):
        for r, n in spans(low // 2, high // 2):
            at = pl.ds(8 + r, n)
            odd_lane = (lane_ids(n) & 1) == 1
            for k in range(tiles):
                value = paired_fix[f, k, at, :]
                if even == odd:
                    fix[even, k, at, :] = value
                else:
                    fix[even, k, at, :] = jnp.where(odd_lane, roll(value, 1), value)
                    fix[odd, k, at, :] = jnp.where(odd_lane, value, roll(value, -1))

    def at_borders(seam, c):
        base = QUARTER * c
        return pltpu.roll(seam, LANES - LEFT - base, 1), pltpu.roll(seam, LANES - RIGHT - base, 1)

    def fine_source(c):
        def tile(k, r, n):
            ids = lane_ids(n)
            by_left, by_right = at_borders(seam_source[0, r : r + n, :], c)
            if k == own_tiles:
                return jnp.where(ids < HALF, by_right, by_left)
            value = source_in[c, k, r : r + n, :]
            if k == 0:
                value = jnp.where(ids == 0, by_left, value)
            if k == own_tiles - 1:
                value = jnp.where(ids == LANES - 1, by_right, value)
            return value

        return tile

    def finish(c, _):
        for r, n in spans(low // 2, high // 2):
            scale = scales(1, r, n)
            for k in range(tiles):
                value = fix[c, k, 8 + r : 8 + r + n, :] * (scale[k] * (1.0 / NEAR))
                fine[k, pl.ds(8 + 2 * r, n, stride=2), :] = value
                fine[k, pl.ds(9 + 2 * r, n, stride=2), :] = value
        for r, n in spans(low, high):
            ids = lane_ids(n)
            by_left, by_right = at_borders(seam_once[0, r : r + n, :], c)
            at = pl.ds(8 + r, n)
            for k in range(own_tiles):
                value = once_in[c, k, r : r + n, :]
                if k == 0:
                    value = jnp.where(ids < 2, by_left, value)
                if k == own_tiles - 1:
                    value = jnp.where(ids >= LANES - 2, by_right, value)
                fine[k, at, :] = fine[k, at, :] + value
            fine[own_tiles, at, :] = fine[own_tiles, at, :] + jnp.where(ids < HALF, by_right, by_left)
        add = fine_source(c)

        def first(piece, turned):
            r, n = piece
            _, found = swept(fine, add, scales(0, r, n), 1, 8 + r, n, True, turned)
            for k in range(tiles):
                fine_two[k, 8 + r : 8 + r + n, :] = found[k]

        def last(piece, turned):
            r, n = piece
            _, found = swept(fine_two, add, scales(0, r, n), 1, 8 + r, n, True, turned, own_tiles)
            for k in range(own_tiles):
                at = pl.ds(k * LANES, LANES)
                out_ref[c, r - HALO : r - HALO + n, at] = x_ref[c, r - HALO : r - HALO + n, at] + found[k]

        staggered(spans(low, high), lambda piece: turn(fine, 1, 8 + piece[0], piece[1]), first, 0)
        staggered(spans(HALO, HALO + rows), lambda piece: turn(fine_two, 1, 8 + piece[0], piece[1]), last, 0)
        leave(c).start()
        return 0

    def leave(c):
        return pltpu.make_async_copy(out_ref.at[c], out_hbm.at[c], sems.at[c])

    lax.fori_loop(0, chans, finish, 0)
    for c in range(chans):
        leave(c).wait()


def swaps(count, odd):
    pairs = [(i, i + 1) for i in range(odd, count - 1, 2)]
    return pairs + [(j, i) for i, j in pairs]


def shards(image_a, image_b, initial, coverage, seam_label):
    chans, rows, cols = image_a.shape
    tiles = cols // LANES
    height = rows + 2 * HALO
    vmem = pl.BlockSpec(memory_space=pltpu.VMEM)
    smem = pl.BlockSpec(memory_space=pltpu.SMEM)
    hbm = pl.BlockSpec(memory_space=pltpu.HBM)
    f32 = jnp.float32
    sds = functools.partial(jax.ShapeDtypeStruct, dtype=f32)
    params = pltpu.CompilerParams(vmem_limit_bytes=40 * 1024 * 1024)
    group, blk = lax.axis_size("group"), lax.axis_size("blk")
    central = sds((chans, tiles, height, LANES))
    assert chans <= 4
    column = sds((height, LANES))
    coarse = sds((chans, tiles, height // 2, LANES))
    upright = sds((tiles, chans * STRIP + 8, LANES))
    beside = sds((sum(message_rows(chans, height)) + 8, LANES))

    sent_even, sent_odd = pl.pallas_call(
        strips,
        out_shape=(upright, upright),
        in_specs=[hbm, hbm, hbm, smem, smem],
        out_specs=(vmem, vmem),
        scratch_shapes=[pltpu.VMEM((2, chans, HALO, cols), f32)] * 3
        + [pltpu.VMEM((tiles, HALO + 16, LANES), f32)]
        + [pltpu.VMEM((tiles, HALO, LANES), f32)] * 2
        + [pltpu.VMEM(upright.shape, f32), pltpu.SemaphoreType.DMA((3, 2))],
        compiler_params=pltpu.CompilerParams(vmem_limit_bytes=56_000_000),
        name="strips",
    )(image_a, image_b, initial, coverage, seam_label)
    got_even = lax.ppermute(sent_even, "group", swaps(group, 0))
    got_odd = lax.ppermute(sent_odd, "group", swaps(group, 1))

    source, once, seam, coarser = pl.pallas_call(
        inside,
        out_shape=(central, central, column, coarse),
        in_specs=[vmem, vmem, vmem, smem, smem],
        out_specs=(vmem,) * 4,
        scratch_shapes=[pltpu.VMEM((tiles, rows + 16, LANES), f32)] * 2 + [pltpu.VMEM((tiles, height, LANES), f32)],
        compiler_params=params,
        cost_estimate=pl.CostEstimate(flops=200_000_000, bytes_accessed=4_000_000, transcendentals=0),
        name="inside",
    )(image_a, image_b, initial, coverage, seam_label)

    source, once, seam, coarser, sent_even, sent_odd = pl.pallas_call(
        join_rows,
        out_shape=(central, central, column, coarse, beside, beside),
        in_specs=[vmem] * 8 + [smem] * 2,
        out_specs=(vmem,) * 6,
        input_output_aliases={0: 0, 1: 1, 2: 2, 3: 3},
        scratch_shapes=[pltpu.VMEM(central.shape, f32), pltpu.VMEM((8, LANES), f32)]
        + [pltpu.VMEM(upright.shape, f32)] * 2
        + [pltpu.VMEM((tiles, 4 * chans, LANES), f32)]
        + [pltpu.VMEM(beside.shape, f32)] * 2,
        compiler_params=params,
        name="join_rows",
    )(source, once, seam, coarser, sent_even, sent_odd, got_even, got_odd, coverage, seam_label)
    got_even = lax.ppermute(sent_even, "blk", swaps(blk, 0))
    got_odd = lax.ppermute(sent_odd, "blk", swaps(blk, 1))

    scratch = [pltpu.VMEM(image_a.shape, f32), pltpu.SemaphoreType.DMA((chans,))]
    scratch += [pltpu.VMEM(beside.shape, f32)] * 2 + [pltpu.VMEM((1, height, LANES), f32)] * 3
    scratch += [pltpu.VMEM((tiles + 1, height + 16, LANES), f32)] * 2
    scratch += [pltpu.VMEM((chans, tiles + 1, height // 2 + 16, LANES), f32)]
    for depth in range(1, LEVELS):
        fields = (chans + 1) // 2 if depth == 1 else 1
        scratch += [pltpu.VMEM((fields, tiles + 1, (height >> depth) + 16, LANES), f32)] * 3
    return pl.pallas_call(
        cycle,
        out_shape=sds((chans, rows, cols)),
        in_specs=[vmem] * 8,
        out_specs=hbm,
        scratch_shapes=scratch,
        compiler_params=params,
        name="cycle",
    )(source, once, seam, coarser, sent_even, got_even, got_odd, initial)


def solution(mesh):
    placed = (
        P(None, "group", "blk"),
        P(None, "group", "blk"),
        P(None, "group", "blk"),
        P("group", "blk"),
        P("group", "blk"),
    )
    return jax.shard_map(
        shards, mesh=mesh, in_specs=placed, out_specs=P(None, "group", "blk"), check_vma=False
    )
```

```python
import functools

import jax
import jax.numpy as jnp
from jax import lax
from jax.experimental import pallas as pl
from jax.experimental.pallas import tpu as pltpu
from jax.sharding import PartitionSpec as P

LEVELS = 4
NU = 2
COARSE = 4
RELAX = 0.8
NEAR = 0.25 * RELAX

LANES = 128
HALF = LANES // 2
HALO = 64
STEP = 96


def source_reach():
    need = 0
    for _ in range(LEVELS - 1):
        need = -(-(need + NU) // 2)
    need += COARSE - 1
    for _ in range(LEVELS - 1):
        need = 2 * need + NU
    return need


REACH = source_reach()
STRIP = REACH + 2
assert STRIP % 8 == 0 and STRIP <= HALO
FIRST = HALO - STRIP
RIM = 8
SEAM = 6
QUARTER = LANES // 4
LEFT, RIGHT = 8, 24


def lane_ids(rows):
    return lax.broadcasted_iota(jnp.int32, (rows, LANES), 1)


def roll(tile, shift):
    return pltpu.roll(tile, shift % LANES, 1)


def spans(low, high, step=STEP):
    while low < high:
        yield low, min(step, high - low)
        low += step


def even_at(axis):
    return lax.rem(lax.axis_index(axis), 2) == 0


def own_source(mids, ups, downs, active):
    tiles = len(mids)
    rights = [roll(t, 1) for t in mids]
    lefts = [roll(t, -1) for t in mids]
    ids = lane_ids(mids[0].shape[0])
    found = []
    for k in range(tiles):
        before = jnp.where(ids == 0, rights[k - 1] if k else 0.0, rights[k])
        after = jnp.where(ids == LANES - 1, lefts[k + 1] if k + 1 < tiles else 0.0, lefts[k])
        beside = (ups[k] + downs[k]) + (before + after)
        found.append(active * (RELAX * mids[k] - NEAR * beside))
    return found


def staggered(items, begin, end, depth):
    waiting = []
    for item in items:
        waiting.append((item, begin(item)))
        if len(waiting) > depth:
            end(*waiting.pop(0))
    for each in waiting:
        end(*each)


def turn(src, shift, r, n):
    tiles = range(src.shape[0])
    return [roll(src[k, r : r + n, :], shift) for k in tiles], [roll(src[k, r : r + n, :], -shift) for k in tiles]


def swept(src, add, scale, shift, r, n, ring, turned, keep=None):
    tiles = src.shape[0]
    ids = lane_ids(n)
    mids = [src[k, r : r + n, :] for k in range(tiles)]
    rights, lefts = turned
    found = []
    for k in range(keep or tiles):
        before, after = rights[k], lefts[k]
        if tiles > 1 or not ring:
            before = jnp.where(ids < shift, rights[k - 1] if ring or k else 0.0, before)
            after = jnp.where(ids >= LANES - shift, lefts[(k + 1) % tiles] if ring or k + 1 < tiles else 0.0, after)
        beside = (src[k, r - 1 : r - 1 + n, :] + src[k, r + 1 : r + 1 + n, :]) + (before + after)
        more = add(k, r - 8, n) if callable(add) else add[k, r : r + n, :]
        found.append(scale[k] * (mids[k] + beside) + more)
    return mids, found


def restricted(rest, k, r, n, shift):
    total = rest[k, pl.ds(r, n, stride=2), :] + rest[k, pl.ds(r + 1, n, stride=2), :]
    even = (lane_ids(n) & shift) == 0
    return total + jnp.where(even, roll(total, -shift), roll(total, shift))


def strip_rows(chans, tiles):
    assert tiles == 2 and 2 * chans + 2 <= 8
    at_coarse = 8 * tiles * chans
    at_seam = at_coarse + chans * (HALO // 2)
    return at_coarse, at_seam, at_seam + 8 * -(-STRIP // 16)


def strips(
    a_hbm, b_hbm, x_hbm, cover_ref, label_ref, even_ref, odd_ref,
    a_both, b_both, x_both, picked, other_a, other_b, source, once, rest, built, sems,
):
    chans, block, cols = a_hbm.shape
    rows = HALO
    tiles = cols // LANES
    active = cover_ref[0, 0].astype(jnp.float32)
    marked = label_ref[0, 0].astype(jnp.float32)
    second = label_ref[0, 0] == 1
    eight = lane_ids(8)


    def fetches(step):
        low = pl.multiple_of(step * (block - HALO), 8)
        pairs = ((a_hbm, a_both), (b_hbm, b_both), (x_hbm, x_both))
        return [
            pltpu.make_async_copy(src.at[:, pl.ds(low, HALO), :], dst.at[step], sems.at[i, step])
            for i, (src, dst) in enumerate(pairs)
        ]

    for step in range(2):
        for fetch in fetches(step):
            fetch.start()

    def one_side(step, _):
        for fetch in fetches(step):
            fetch.wait()
        message(step, a_both.at[step], b_both.at[step], x_both.at[step])
        return 0

    def message(step, a_ref, b_ref, x_ref):
        top = step == 0
        start = pl.multiple_of(jnp.where(top, 0, rows - STRIP), 8)
        near = pl.multiple_of(jnp.where(top, 8, rows), 8)
        line = jnp.where(top, 0, rows - 1)
        at_coarse, at_seam, at_marks = strip_rows(chans, tiles)
        scale = [active * NEAR] * tiles
        place = eight & (QUARTER - 1)
        seams = [jnp.zeros((8, LANES), jnp.float32) for _ in range(STRIP // 8)]
        channels = range(chans)
        for c in channels:
            for k in range(tiles):
                for edge in (7, 8 + rows):
                    picked[c, k, edge : edge + 1, :] = jnp.zeros((1, LANES), jnp.float32)
                at = pl.ds(k * LANES, LANES)
                x = x_ref[c, :, at]
                from_a, from_b = a_ref[c, :, at] - x, b_ref[c, :, at] - x
                other_a[c, k], other_b[c, k] = from_a, from_b
                picked[c, k, 8 : 8 + rows, :] = jnp.where(second, from_b, from_a)
        for c in channels:
            parts = [[picked[c, k, 8 + s : 8 + s + rows, :] for k in range(tiles)] for s in (0, -1, 1)]
            for k, found in enumerate(own_source(*parts, active)):
                source[c, k, 8 : 8 + rows, :] = found
        for c in channels:
            src = source.at[c]
            _, found = swept(src, src, scale, 1, 8, rows, False, turn(src, 1, 8, rows))
            for k in range(tiles):
                once[c, k, 8 : 8 + rows, :] = found[k]
        for c in channels:
            mids, found = swept(once.at[c], source.at[c], scale, 1, 8, rows, False, turn(once.at[c], 1, 8, rows))
            for k in range(tiles):
                rest[c, k, 8 : 8 + rows, :] = found[k] - mids[k]
        for c in channels:
            first, last = (restricted(rest.at[c], k, 8, rows // 2, 1) for k in range(tiles))
            low = at_coarse + c * (rows // 2)
            built[low : low + rows // 2, :] = jnp.where((lane_ids(rows // 2) & 1) == 0, first, last)
            for k in range(tiles):
                low = 8 * (tiles * c + k)
                built[low : low + 8, :] = source[c, k, pl.ds(near, 8), :]
                low = at_marks + 8 * k + 2 * c
                built[low : low + 1, :] = other_a[c, k, pl.ds(line, 1), :]
                built[low + 1 : low + 2, :] = other_b[c, k, pl.ds(line, 1), :]
            base = QUARTER * c
            for t in range(STRIP // 8):
                at, own_at = pl.ds(start + 8 * t, 8), pl.ds(8 + start + 8 * t, 8)
                seam = seams[t]
                for cells, cell, lane, width in (
                    (source[c, 0, own_at, :], 0, LEFT, SEAM),
                    (source[c, tiles - 1, own_at, :], LANES - SEAM, RIGHT - SEAM, SEAM),
                    (other_a[c, 0, at, :], 0, LEFT - 1, 1),
                    (other_b[c, 0, at, :], 0, LEFT - 2, 1),
                    (other_a[c, tiles - 1, at, :], LANES - 1, RIGHT, 1),
                    (other_b[c, tiles - 1, at, :], LANES - 1, RIGHT + 1, 1),
                ):
                    spot = (eight >= base + lane) & (eight < base + lane + width)
                    seam = jnp.where(spot, roll(cells, base + lane - cell), seam)
                seams[t] = seam
        for t in range(STRIP // 8):
            slot = 2 * (t & 1)
            if slot == 0:
                packed = jnp.zeros((8, LANES), jnp.float32)
            packed = jnp.where((place >> 3) == slot, roll(seams[t], 8 * slot - (LEFT - 2)), packed)
            packed = jnp.where((place >> 3) == slot + 1, roll(seams[t], 8 * slot + 8 - (RIGHT - SEAM)), packed)
            built[at_seam + 8 * (t // 2) : at_seam + 8 * (t // 2) + 8, :] = packed
        for k in range(tiles):
            low = at_marks + 8 * k + 2 * chans
            built[low : low + 1, :] = jnp.full((1, LANES), active)
            built[low + 1 : low + 2, :] = jnp.full((1, LANES), marked)

        by_odd = top == even_at("group")

        @pl.when(by_odd)
        def _():
            odd_ref[...] = built[...]

        @pl.when(jnp.logical_not(by_odd))
        def _():
            even_ref[...] = built[...]

    lax.fori_loop(0, 2, one_side, 0)


def inside(a_ref, b_ref, x_ref, cover_ref, label_ref, source_ref, once_ref, seam_ref, coarse_ref, da, db, rest):
    chans, rows, cols = a_ref.shape
    tiles = cols // LANES
    active = cover_ref[0, 0].astype(jnp.float32)
    second = label_ref[0, 0] == 1
    for k in range(tiles):
        for buf in (da, db):
            buf[k, 0:8, :] = jnp.zeros((8, LANES), jnp.float32)
            buf[k, rows + 8 : rows + 16, :] = jnp.zeros((8, LANES), jnp.float32)
    scale = [active * NEAR] * tiles
    top, end = HALO, HALO + rows

    def pick(k, low, n):
        return jnp.where(second, db[k, low : low + n, :], da[k, low : low + n, :])

    seam_ref[...] = jnp.zeros(seam_ref.shape, jnp.float32)

    def channel(c, _):
        for k in range(tiles):
            at = pl.ds(k * LANES, LANES)
            for r, n in spans(0, rows):
                x = x_ref[c, r : r + n, at]
                da[k, 8 + r : 8 + r + n, :] = a_ref[c, r : r + n, at] - x
                db[k, 8 + r : 8 + r + n, :] = b_ref[c, r : r + n, at] - x
        for r, n in spans(0, rows):
            parts = [[pick(k, 8 + s + r, n) for k in range(tiles)] for s in (0, -1, 1)]
            found = own_source(*parts, active)
            for k in range(tiles):
                source_ref[c, k, top + r : top + r + n, :] = found[k]
            ids = lane_ids(n)
            base = QUARTER * c
            at = pl.ds(8 + r, n)
            seam = pltpu.roll(found[0], base + LEFT, 1)
            for source, cell, lane in (
                (found[tiles - 1], LANES - SEAM, RIGHT - SEAM),
                (da[0, at, :], 0, LEFT - 1),
                (db[0, at, :], 0, LEFT - 2),
                (da[tiles - 1, at, :], LANES - 1, RIGHT),
                (db[tiles - 1, at, :], LANES - 1, RIGHT + 1),
            ):
                spot = (ids >= base + lane) & (ids < base + lane + (SEAM if cell == LANES - SEAM else 1))
                seam = jnp.where(spot, pltpu.roll(source, base + lane + (LANES - cell) % LANES, 1), seam)
            at = pl.ds(top + r, n)
            mine = (ids >= base + LEFT - 2) & (ids < base + RIGHT + 2)
            mine = mine & ((ids < base + LEFT + SEAM) | (ids >= base + RIGHT - SEAM))
            seam_ref[at, :] = jnp.where(mine, seam, seam_ref[at, :])
        source, once = source_ref.at[c], once_ref.at[c]

        def first(piece, turned):
            r, n = piece
            _, found = swept(source, source, scale, 1, r, n, False, turned)
            for k in range(tiles):
                once_ref[c, k, r : r + n, :] = found[k]

        def second_sweep(piece, turned):
            r, n = piece
            mids, found = swept(once, source, scale, 1, r, n, False, turned)
            for k in range(tiles):
                rest[k, r : r + n, :] = found[k] - mids[k]

        staggered(spans(top, end), lambda piece: turn(source, 1, *piece), first, 0)
        staggered(spans(top, end), lambda piece: turn(once, 1, *piece), second_sweep, 0)
        for r, n in spans(top // 2, end // 2):
            for k in range(tiles):
                coarse_ref[c, k, r : r + n, :] = restricted(rest, k, 2 * r, n, 1)
        return 0

    lax.fori_loop(0, chans, channel, 0)


def seam_units(height):
    for t in range((height - 2 * FIRST) // 8):
        yield FIRST + 8 * t, t // 4, t % 4


def message_rows(chans, height):
    quarter = height // 2
    cells = (chans // 2 * quarter + chans % 2 * quarter // 2) // 2
    return cells, -(-(height - 2 * FIRST) // 32) * 8


def column_rows(chans, height):
    quarter = height // 2
    places = [(c, r, c + 1, r) for c in range(0, chans - 1, 2) for r in range(0, quarter, 8)]
    if chans % 2:
        places += [(chans - 1, r, chans - 1, r + quarter // 2) for r in range(0, quarter // 2, 8)]
    return places


def join_rows(
    source_in, once_in, seam_in, coarse_in, sent_even, sent_odd, got_even, got_odd, cover_ref, label_ref,
    source_ref, once_ref, seam_ref, coarse_ref, even_ref, odd_ref, rest, marks_ref, upper_got, lower_got, lines, left_out, right_out,
):
    chans, tiles, height, _ = source_ref.shape
    rows = height - 2 * HALO
    row_even, col_even = even_at("group"), even_at("blk")
    active = cover_ref[0, 0].astype(jnp.float32)
    marked = label_ref[0, 0].astype(jnp.float32)
    eight = lane_ids(8)

    place = eight & (QUARTER - 1)

    at_coarse, at_seam, at_marks = strip_rows(chans, tiles)

    def take(top, got):
        near = HALO - 8 if top else HALO + rows
        mine = lines[0 if top else 1]
        edge = HALO if top else HALO + rows - 1
        other = edge - 1 if top else edge + 1
        their_active = got[at_marks + 2 * chans : at_marks + 2 * chans + 1, :]
        their_mark = got[at_marks + 2 * chans + 1 : at_marks + 2 * chans + 2, :]
        band = 0 if top else 2
        marks_ref[band : band + 1, :] = their_active
        marks_ref[band + 3 : band + 4, :] = their_mark
        half_halo = HALO // 2
        coarse_at = 0 if top else (height - HALO) // 2
        even_cell = (lane_ids(half_halo) & 1) == 0
        for c in range(chans):
            cells = got[at_coarse + c * half_halo : at_coarse + (c + 1) * half_halo, :]
            at = pl.ds(coarse_at, half_halo)
            coarse_ref[c, 0, at, :] = jnp.where(even_cell, cells, roll(cells, 1))
            coarse_ref[c, 1, at, :] = jnp.where(even_cell, roll(cells, -1), cells)
            for k in range(tiles):
                source_ref[c, k, near : near + 8, :] = got[8 * (tiles * c + k) : 8 * (tiles * c + k) + 8, :]
                low = at_marks + 8 * k + 2 * c
                their_a, their_b = got[low : low + 1, :], got[low + 1 : low + 2, :]
                my_a, my_b = mine[k, 2 * c : 2 * c + 1, :], mine[k, 2 * c + 1 : 2 * c + 2, :]
                for_mine = NEAR * active * jnp.where(marked == 1.0, their_b, their_a)
                for_theirs = NEAR * their_active * jnp.where(their_mark == 1.0, my_b, my_a)
                source_ref[c, k, edge : edge + 1, :] = source_ref[c, k, edge : edge + 1, :] - for_mine
                source_ref[c, k, other : other + 1, :] = source_ref[c, k, other : other + 1, :] - for_theirs

        def seam_of(r, cells):
            for c in range(chans):
                base = QUARTER * c
                spot = (eight >= base + LEFT) & (eight < base + LEFT + SEAM)
                cells = jnp.where(spot, roll(source_ref[c, 0, r : r + 8, :], base + LEFT), cells)
                spot = (eight >= base + RIGHT - SEAM) & (eight < base + RIGHT)
                cells = jnp.where(spot, roll(source_ref[c, tiles - 1, r : r + 8, :], base + RIGHT), cells)
            seam_ref[r : r + 8, :] = cells

        in_left = (place >= LEFT - 2) & (place < LEFT + SEAM)
        in_right = (place >= RIGHT - SEAM) & (place < RIGHT + 2)
        for t in range(STRIP // 8):
            packed = got[at_seam + 8 * (t // 2) : at_seam + 8 * (t // 2) + 8, :]
            slot = 2 * (t & 1)
            firsts = jnp.where(in_left, roll(packed, LEFT - 2 - 8 * slot), 0.0)
            cells = jnp.where(in_right, roll(packed, RIGHT - SEAM - 8 * slot - 8), firsts)
            cells = jnp.where(eight < QUARTER * chans, cells, 0.0)
            r = (FIRST if top else HALO + rows) + 8 * t
            if r == near:
                seam_of(r, cells)
            else:
                seam_ref[r : r + 8, :] = cells
        r = edge // 8 * 8
        seam_of(r, seam_ref[r : r + 8, :])

    def arrange(upper, lower, mine_up, mine_low):
        upper_got[...] = upper[...]
        lower_got[...] = lower[...]
        for k in range(tiles):
            at = pl.ds(at_marks + 8 * k, 8)
            lines[0, k], lines[1, k] = mine_up[at, :], mine_low[at, :]

    @pl.when(row_even)
    def _():
        arrange(got_odd, got_even, sent_odd, sent_even)

    @pl.when(jnp.logical_not(row_even))
    def _():
        arrange(got_even, got_odd, sent_even, sent_odd)

    take(True, upper_got)
    take(False, lower_got)
    marks_ref[1:2, :] = jnp.full((1, LANES), active)
    marks_ref[4:5, :] = jnp.full((1, LANES), marked)
    marks_ref[6:8, :] = jnp.zeros((2, LANES), jnp.float32)

    bottom = HALO + rows
    edges = ((HALO - 8, HALO, 0), (HALO, HALO + RIM, 1), (bottom - RIM, bottom, 1), (bottom, bottom + 8, 2))
    spots = [(c, band, r, n) for c in range(chans) for low, high, band in edges for r, n in spans(low, high)]
    for stage in range(2):
        held = (source_ref, once_ref)[stage]

        def edge_sweep(spot, turned):
            c, band, r, n = spot
            scale = [jnp.broadcast_to(marks_ref[band : band + 1, :] * NEAR, (n, LANES))] * tiles
            mids, found = swept(held.at[c], source_ref.at[c], scale, 1, r, n, False, turned)
            for k in range(tiles):
                if stage == 0:
                    once_ref[c, k, r : r + n, :] = found[k]
                else:
                    rest[c, k, r : r + n, :] = found[k] - mids[k]

        staggered(spots, lambda spot: turn(held.at[spot[0]], 1, *spot[2:]), edge_sweep, 0)
    for c in range(chans):
        for low, high in ((HALO - 4, HALO + RIM), (bottom - RIM, bottom + 4)):
            for k in range(tiles):
                coarse_ref[c, k, low // 2 : high // 2, :] = restricted(rest.at[c], k, low, (high - low) // 2, 1)

    cells, units = message_rows(chans, height)
    first_half = eight < HALF
    even_lane = (eight & 1) == 0

    def edge_cells(c, r):
        return jnp.where(first_half, coarse_ref[c, 0, r : r + 8, :], coarse_ref[c, tiles - 1, r : r + 8, :])

    def joined(place):
        c, r, d, s = place
        return jnp.where(even_lane, edge_cells(c, r), edge_cells(d, s))

    def pack(left, right):
        places = column_rows(chans, height)
        for t in range(cells // 8):
            upper, lower = joined(places[t]), joined(places[t + cells // 8])
            left[8 * t : 8 * t + 8, :] = jnp.where(first_half, upper, roll(lower, HALF))
            right[8 * t : 8 * t + 8, :] = jnp.where(first_half, roll(upper, HALF), lower)
        lefts = rights = jnp.zeros((8, LANES), jnp.float32)
        for r, tile, slot in seam_units(height):
            value = seam_ref[r : r + 8, :]
            spot = (place >> 3) == slot
            lefts = jnp.where(spot, roll(value, 8 * slot - (LEFT - 2)), lefts)
            rights = jnp.where(spot, roll(value, 8 * slot - (RIGHT - SEAM)), rights)
            at = cells + 8 * tile
            left[at : at + 8, :], right[at : at + 8, :] = lefts, rights
        for out in (left, right):
            out[cells + units : cells + units + 8, :] = marks_ref[...]

    pack(left_out, right_out)

    @pl.when(col_even)
    def _():
        odd_ref[...] = left_out[...]
        even_ref[...] = right_out[...]

    @pl.when(jnp.logical_not(col_even))
    def _():
        even_ref[...] = left_out[...]
        odd_ref[...] = right_out[...]


def cycle(
    source_in, once_in, seam_in, coarse_in, sent_even, got_even, got_odd, x_ref, out_hbm,
    out_ref, sems, right_ref, left_ref, seam_source, seam_once, seam_rest, fine, fine_two, fix, *bufs,
):
    chans, own_tiles, height, _ = source_in.shape
    rows = height - 2 * HALO
    tiles = own_tiles + 1
    cells, units = message_rows(chans, height)
    col_even = even_at("blk")
    eight = lane_ids(8)

    @pl.when(col_even)
    def _():
        right_ref[...] = got_even[...]
        left_ref[...] = got_odd[...]

    @pl.when(jnp.logical_not(col_even))
    def _():
        right_ref[...] = got_odd[...]
        left_ref[...] = got_even[...]

    at = cells + units

    def mark(ref, row):
        return jnp.broadcast_to(ref[at + row : at + row + 1, :], (8, LANES))

    own = [mark(sent_even, i) for i in range(6)]
    right = [mark(right_ref, i) for i in range(6)]
    left = [mark(left_ref, i) for i in range(6)]
    first_half = eight < HALF
    place = eight & (QUARTER - 1)

    def mixed(i):
        return jnp.where(place < LEFT, left[i], jnp.where(place < RIGHT, own[i], right[i]))

    seam_scale = [jnp.where(eight < QUARTER * chans, mixed(i), 0.0) * NEAR for i in range(3)]
    seam_mark = [mixed(i + 3) == 1.0 for i in range(3)]
    own_scale = [own[i] * NEAR for i in range(3)]
    side_scale = [jnp.where(first_half, right[i], left[i]) * NEAR for i in range(3)]

    def wide(mask, n):
        return jnp.broadcast_to(mask[:1], (n, LANES))

    def over_rows(kinds, depth, r, n):
        full, halo = height >> depth, HALO >> depth
        ends = ((0, halo), (halo, full - halo), (full - halo, full))
        parts = [(max(a, r), min(b, r + n), kind) for (a, b), kind in zip(ends, kinds)]
        parts = [wide(kind, b - a) for a, b, kind in parts if b > a]
        return parts[0] if len(parts) == 1 else jnp.concatenate(parts, axis=0)

    def scales(depth, r, n):
        return [over_rows(own_scale, depth, r, n)] * own_tiles + [over_rows(side_scale, depth, r, n)]

    inner = ((place >= LEFT) & (place < LEFT + SEAM)) | ((place >= RIGHT - SEAM) & (place < RIGHT))
    outer = ((place >= LEFT - SEAM) & (place < LEFT)) | ((place >= RIGHT) & (place < RIGHT + SEAM))
    from_near = (place == LEFT) | (place == RIGHT - 1)
    from_own = (place == LEFT - 1) | (place == RIGHT)
    up_one = (place == LEFT - 1) | (place == RIGHT - 1)
    near_b = (place == LEFT + 1) | (place == RIGHT - 2)
    right_unit = place >= RIGHT - 2

    def unpack(unit):
        r, tile, slot = unit
        rights = roll(right_ref[cells + 8 * tile : cells + 8 * tile + 8, :], RIGHT - 2 - 8 * slot)
        lefts = roll(left_ref[cells + 8 * tile : cells + 8 * tile + 8, :], LEFT - SEAM - 8 * slot)
        return rights, lefts

    def keep_near(unit, turned):
        r = unit[0]
        seam_rest[0, r : r + 8, :] = jnp.where(right_unit, *turned)

    def second_cells(unit):
        r = unit[0]
        cells_b = jnp.where(near_b, seam_rest[0, r : r + 8, :], seam_in[r : r + 8, :])
        return roll(cells_b, 1), roll(cells_b, -1)

    def put_seam(unit, turned):
        r = unit[0]
        band = 0 if r < HALO else 1 if r < HALO + rows else 2
        near, mine = seam_rest[0, r : r + 8, :], seam_in[r : r + 8, :]
        value = jnp.where(inner, mine, jnp.where(outer, near, 0.0))
        border = jnp.where(seam_mark[band], jnp.where(up_one, *turned), jnp.where(from_near, near, mine))
        border = jnp.where(from_near | from_own, border, 0.0)
        seam_source[0, r : r + 8, :] = value - seam_scale[band] * border

    staggered(seam_units(height), unpack, keep_near, 24)
    staggered(seam_units(height), second_cells, put_seam, 24)
    for r, n in spans(FIRST, height - FIRST, height):
        _, found = swept(
            seam_source, seam_source, [over_rows(seam_scale, 0, r, n)], 1, r, n, True, turn(seam_source, 1, r, n)
        )
        seam_once[0, r : r + n, :] = found[0]
        mids, found = swept(
            seam_once, seam_source, [over_rows(seam_scale, 0, r, n)], 1, r, n, True, turn(seam_once, 1, r, n)
        )
        seam_rest[0, r : r + n, :] = found[0] - mids[0]

    one_src, one_once, one_two = bufs[0:3]
    half_rows = height // 2
    eights = lane_ids(8)
    even_lane = (eights & 1) == 0
    places = column_rows(chans, height)
    for t, (c, r, d, s) in enumerate(places):
        low, upper = (8 * t, True) if t < cells // 8 else (8 * t - cells, False)
        from_right, from_left = right_ref[low : low + 8, :], left_ref[low : low + 8, :]
        if upper:
            value = jnp.where(first_half, from_right, roll(from_left, HALF))
        else:
            value = jnp.where(first_half, roll(from_right, HALF), from_left)
        if c == d:
            one_src[c // 2, own_tiles, 8 + r : 16 + r, :] = jnp.where(even_lane, value, roll(value, 1))
            one_src[c // 2, own_tiles, 8 + s : 16 + s, :] = jnp.where(even_lane, roll(value, -1), value)
        else:
            one_src[c // 2, own_tiles, 8 + r : 16 + r, :] = value

    pairs = [(c, min(c + 1, chans - 1)) for c in range(0, chans, 2)]

    def paired(of, pair, n):
        first, second = pair
        return of(first) if first == second else jnp.where((lane_ids(n) & 1) == 0, of(first), of(second))

    for f, pair in enumerate(pairs):
        for r, n in spans(0, half_rows):
            for k in range(own_tiles):
                one_src[f, k, 8 + r : 8 + r + n, :] = paired(lambda c: coarse_in[c, k, r : r + n, :], pair, n)
    for r, n in spans(FIRST // 2, half_rows - FIRST // 2):
        ids = lane_ids(n)
        seam = restricted(seam_rest, 0, 2 * r, n, 1)
        at = pl.ds(8 + r, n)
        for f, pair in enumerate(pairs):
            by_left = paired(lambda c: roll(seam, -QUARTER * c - LEFT), pair, n)
            by_right = paired(lambda c: roll(seam, -QUARTER * c - RIGHT), pair, n)
            one_src[f, 0, at, :] = jnp.where(ids < 4, by_left, one_src[f, 0, at, :])
            inner_end = one_src[f, own_tiles - 1, at, :]
            one_src[f, own_tiles - 1, at, :] = jnp.where(ids >= LANES - 4, by_right, inner_end)
            side = jnp.where(ids < 4, by_right, one_src[f, own_tiles, at, :])
            one_src[f, own_tiles, at, :] = jnp.where(ids >= LANES - 4, by_left, side)

    def smooth(src, once, fields, depth, into, minus=False):
        def one_sweep(spot, turned):
            f, r, n = spot
            mids, found = swept(once.at[f], src.at[f], scales(depth, r, n), 1 << depth, 8 + r, n, True, turned)
            for k in range(tiles):
                into[f, k, 8 + r : 8 + r + n, :] = found[k] - mids[k] if minus else found[k]

        spots = [(f, r, n) for f in range(fields) for r, n in spans(0, height >> depth)]
        staggered(spots, lambda spot: turn(once.at[spot[0]], 1 << depth, 8 + spot[1], spot[2]), one_sweep, 0)

    def expand(fix, fields, depth, out, low, high, spread):
        for f in range(fields):
            for r, n in spans(low, high):
                scale = scales(depth + 1, r, n)
                for k in range(tiles):
                    value = fix[0 if spread else f, k, 8 + r : 8 + r + n, :]
                    if spread:
                        value = spread(value, f)
                    value = value * (scale[k] * (1.0 / NEAR))
                    out[f, k, pl.ds(8 + 2 * r, n, stride=2), :] = value
                    out[f, k, pl.ds(9 + 2 * r, n, stride=2), :] = value

    def add_fix(once, two, fields, depth, into):
        for f in range(fields):
            for r, n in spans(0, height >> depth):
                for k in range(tiles):
                    at = pl.ds(8 + r, n)
                    into[f, k, at, :] = once[f, k, at, :] + two[f, k, at, :]

    assert chans <= 4 and LEVELS >= 3

    def spread_pair(value, f):
        high = (lane_ids(value.shape[0]) & 2) == 2
        return jnp.where(high, value, roll(value, -2)) if f else jnp.where(high, roll(value, 2), value)

    def level(depth):
        src, once, two = bufs[3 * (depth - 1) : 3 * depth]
        fields = len(pairs) if depth == 1 else 1
        if depth == LEVELS - 1:
            held = src
            for sweep in range(1, COARSE):
                into = (once, two)[sweep % 2]
                smooth(src, held, fields, depth, into)
                held = into
            return held
        smooth(src, src, fields, depth, once)
        smooth(src, once, fields, depth, two, True)
        below = bufs[3 * depth]
        shift = 1 << depth
        for r, n in spans(0, height >> (depth + 1)):
            half = (lane_ids(n) & 2) >> 1
            for k in range(tiles):
                value = None
                for f in range(fields):
                    total = restricted(two.at[f], k, 8 + 2 * r, n, shift)
                    value = total if value is None else jnp.where(half == f, total, value)
                below[0, k, 8 + r : 8 + r + n, :] = value
        fix = level(depth + 1)
        expand(fix, fields, depth, two, 0, height >> (depth + 1), spread_pair if depth == 1 else None)
        add_fix(once, two, fields, depth, once)
        smooth(src, once, fields, depth, two)
        smooth(src, two, fields, depth, once)
        return once

    paired_fix = level(1)
    low, high = HALO - RIM, HALO + rows + RIM
    for f, (even, odd) in enumerate(pairs):
        for r, n in spans(low // 2, high // 2):
            at = pl.ds(8 + r, n)
            odd_lane = (lane_ids(n) & 1) == 1
            for k in range(tiles):
                value = paired_fix[f, k, at, :]
                if even == odd:
                    fix[even, k, at, :] = value
                else:
                    fix[even, k, at, :] = jnp.where(odd_lane, roll(value, 1), value)
                    fix[odd, k, at, :] = jnp.where(odd_lane, value, roll(value, -1))

    def at_borders(seam, c):
        base = QUARTER * c
        return pltpu.roll(seam, LANES - LEFT - base, 1), pltpu.roll(seam, LANES - RIGHT - base, 1)

    def fine_source(c):
        def tile(k, r, n):
            ids = lane_ids(n)
            by_left, by_right = at_borders(seam_source[0, r : r + n, :], c)
            if k == own_tiles:
                return jnp.where(ids < HALF, by_right, by_left)
            value = source_in[c, k, r : r + n, :]
            if k == 0:
                value = jnp.where(ids == 0, by_left, value)
            if k == own_tiles - 1:
                value = jnp.where(ids == LANES - 1, by_right, value)
            return value

        return tile

    def finish(c, _):
        for r, n in spans(low // 2, high // 2):
            scale = scales(1, r, n)
            for k in range(tiles):
                value = fix[c, k, 8 + r : 8 + r + n, :] * (scale[k] * (1.0 / NEAR))
                fine[k, pl.ds(8 + 2 * r, n, stride=2), :] = value
                fine[k, pl.ds(9 + 2 * r, n, stride=2), :] = value
        for r, n in spans(low, high):
            ids = lane_ids(n)
            by_left, by_right = at_borders(seam_once[0, r : r + n, :], c)
            at = pl.ds(8 + r, n)
            for k in range(own_tiles):
                value = once_in[c, k, r : r + n, :]
                if k == 0:
                    value = jnp.where(ids < 2, by_left, value)
                if k == own_tiles - 1:
                    value = jnp.where(ids >= LANES - 2, by_right, value)
                fine[k, at, :] = fine[k, at, :] + value
            fine[own_tiles, at, :] = fine[own_tiles, at, :] + jnp.where(ids < HALF, by_right, by_left)
        add = fine_source(c)

        def first(piece, turned):
            r, n = piece
            _, found = swept(fine, add, scales(0, r, n), 1, 8 + r, n, True, turned)
            for k in range(tiles):
                fine_two[k, 8 + r : 8 + r + n, :] = found[k]

        def last(piece, turned):
            r, n = piece
            _, found = swept(fine_two, add, scales(0, r, n), 1, 8 + r, n, True, turned, own_tiles)
            for k in range(own_tiles):
                at = pl.ds(k * LANES, LANES)
                out_ref[c, r - HALO : r - HALO + n, at] = x_ref[c, r - HALO : r - HALO + n, at] + found[k]

        staggered(spans(low, high), lambda piece: turn(fine, 1, 8 + piece[0], piece[1]), first, 0)
        staggered(spans(HALO, HALO + rows), lambda piece: turn(fine_two, 1, 8 + piece[0], piece[1]), last, 0)
        leave(c).start()
        return 0

    def leave(c):
        return pltpu.make_async_copy(out_ref.at[c], out_hbm.at[c], sems.at[c])

    lax.fori_loop(0, chans, finish, 0)
    for c in range(chans):
        leave(c).wait()


def swaps(count, odd):
    pairs = [(i, i + 1) for i in range(odd, count - 1, 2)]
    return pairs + [(j, i) for i, j in pairs]


def shards(image_a, image_b, initial, coverage, seam_label):
    chans, rows, cols = image_a.shape
    tiles = cols // LANES
    height = rows + 2 * HALO
    vmem = pl.BlockSpec(memory_space=pltpu.VMEM)
    smem = pl.BlockSpec(memory_space=pltpu.SMEM)
    hbm = pl.BlockSpec(memory_space=pltpu.HBM)
    f32 = jnp.float32
    sds = functools.partial(jax.ShapeDtypeStruct, dtype=f32)
    params = pltpu.CompilerParams(vmem_limit_bytes=40 * 1024 * 1024)
    group, blk = lax.axis_size("group"), lax.axis_size("blk")
    central = sds((chans, tiles, height, LANES))
    assert chans <= 4
    column = sds((height, LANES))
    coarse = sds((chans, tiles, height // 2, LANES))
    upright = sds((strip_rows(chans, tiles)[2] + 8 * tiles, LANES))
    beside = sds((sum(message_rows(chans, height)) + 8, LANES))

    sent_even, sent_odd = pl.pallas_call(
        strips,
        out_shape=(upright, upright),
        in_specs=[hbm, hbm, hbm, smem, smem],
        out_specs=(vmem, vmem),
        scratch_shapes=[pltpu.VMEM((2, chans, HALO, cols), f32)] * 3
        + [pltpu.VMEM((chans, tiles, HALO + 16, LANES), f32)]
        + [pltpu.VMEM((chans, tiles, HALO, LANES), f32)] * 2
        + [pltpu.VMEM((chans, tiles, HALO + 16, LANES), f32)] * 3
        + [pltpu.VMEM(upright.shape, f32), pltpu.SemaphoreType.DMA((3, 2))],
        compiler_params=pltpu.CompilerParams(vmem_limit_bytes=56_000_000),
        name="strips",
    )(image_a, image_b, initial, coverage, seam_label)
    got_even = lax.ppermute(sent_even, "group", swaps(group, 0))
    got_odd = lax.ppermute(sent_odd, "group", swaps(group, 1))

    source, once, seam, coarser = pl.pallas_call(
        inside,
        out_shape=(central, central, column, coarse),
        in_specs=[vmem, vmem, vmem, smem, smem],
        out_specs=(vmem,) * 4,
        scratch_shapes=[pltpu.VMEM((tiles, rows + 16, LANES), f32)] * 2 + [pltpu.VMEM((tiles, height, LANES), f32)],
        compiler_params=params,
        cost_estimate=pl.CostEstimate(flops=200_000_000, bytes_accessed=4_000_000, transcendentals=0),
        name="inside",
    )(image_a, image_b, initial, coverage, seam_label)

    source, once, seam, coarser, sent_even, sent_odd = pl.pallas_call(
        join_rows,
        out_shape=(central, central, column, coarse, beside, beside),
        in_specs=[vmem] * 8 + [smem] * 2,
        out_specs=(vmem,) * 6,
        input_output_aliases={0: 0, 1: 1, 2: 2, 3: 3},
        scratch_shapes=[pltpu.VMEM(central.shape, f32), pltpu.VMEM((8, LANES), f32)]
        + [pltpu.VMEM(upright.shape, f32)] * 2
        + [pltpu.VMEM((2, tiles, 8, LANES), f32)]
        + [pltpu.VMEM(beside.shape, f32)] * 2,
        compiler_params=params,
        name="join_rows",
    )(source, once, seam, coarser, sent_even, sent_odd, got_even, got_odd, coverage, seam_label)
    got_even = lax.ppermute(sent_even, "blk", swaps(blk, 0))
    got_odd = lax.ppermute(sent_odd, "blk", swaps(blk, 1))

    scratch = [pltpu.VMEM(image_a.shape, f32), pltpu.SemaphoreType.DMA((chans,))]
    scratch += [pltpu.VMEM(beside.shape, f32)] * 2 + [pltpu.VMEM((1, height, LANES), f32)] * 3
    scratch += [pltpu.VMEM((tiles + 1, height + 16, LANES), f32)] * 2
    scratch += [pltpu.VMEM((chans, tiles + 1, height // 2 + 16, LANES), f32)]
    for depth in range(1, LEVELS):
        fields = (chans + 1) // 2 if depth == 1 else 1
        scratch += [pltpu.VMEM((fields, tiles + 1, (height >> depth) + 16, LANES), f32)] * 3
    return pl.pallas_call(
        cycle,
        out_shape=sds((chans, rows, cols)),
        in_specs=[vmem] * 8,
        out_specs=hbm,
        scratch_shapes=scratch,
        compiler_params=params,
        name="cycle",
    )(source, once, seam, coarser, sent_even, got_even, got_odd, initial)


def solution(mesh):
    placed = (
        P(None, "group", "blk"),
        P(None, "group", "blk"),
        P(None, "group", "blk"),
        P("group", "blk"),
        P("group", "blk"),
    )
    return jax.shard_map(
        shards, mesh=mesh, in_specs=placed, out_specs=P(None, "group", "blk"), check_vma=False
    )
```

```python
import functools

import jax
import jax.numpy as jnp
from jax import lax
from jax.experimental import pallas as pl
from jax.experimental.pallas import tpu as pltpu
from jax.sharding import PartitionSpec as P

LEVELS = 4
NU = 2
COARSE = 4
RELAX = 0.8
NEAR = 0.25 * RELAX

LANES = 128
HALF = LANES // 2
HALO = 64
STEP = 96


def source_reach():
    need = 0
    for _ in range(LEVELS - 1):
        need = -(-(need + NU) // 2)
    need += COARSE - 1
    for _ in range(LEVELS - 1):
        need = 2 * need + NU
    return need


REACH = source_reach()
STRIP = REACH + 2
assert STRIP % 8 == 0 and STRIP <= HALO
FIRST = HALO - STRIP
RIM = 8
SEAM = 6
QUARTER = LANES // 4
LEFT, RIGHT = 8, 24


def lane_ids(rows):
    return lax.broadcasted_iota(jnp.int32, (rows, LANES), 1)


def roll(tile, shift):
    return pltpu.roll(tile, shift % LANES, 1)


def spans(low, high, step=STEP):
    while low < high:
        yield low, min(step, high - low)
        low += step


def even_at(axis):
    return lax.rem(lax.axis_index(axis), 2) == 0


def own_source(mids, ups, downs, active):
    tiles = len(mids)
    rights = [roll(t, 1) for t in mids]
    lefts = [roll(t, -1) for t in mids]
    ids = lane_ids(mids[0].shape[0])
    found = []
    for k in range(tiles):
        before = jnp.where(ids == 0, rights[k - 1] if k else 0.0, rights[k])
        after = jnp.where(ids == LANES - 1, lefts[k + 1] if k + 1 < tiles else 0.0, lefts[k])
        beside = (ups[k] + downs[k]) + (before + after)
        found.append(active * (RELAX * mids[k] - NEAR * beside))
    return found


def staggered(items, begin, end, depth):
    waiting = []
    for item in items:
        waiting.append((item, begin(item)))
        if len(waiting) > depth:
            end(*waiting.pop(0))
    for each in waiting:
        end(*each)


def turn(src, shift, r, n):
    tiles = range(src.shape[0])
    return [roll(src[k, r : r + n, :], shift) for k in tiles], [roll(src[k, r : r + n, :], -shift) for k in tiles]


def swept(src, add, scale, shift, r, n, ring, turned, keep=None):
    tiles = src.shape[0]
    ids = lane_ids(n)
    mids = [src[k, r : r + n, :] for k in range(tiles)]
    rights, lefts = turned
    found = []
    for k in range(keep or tiles):
        before, after = rights[k], lefts[k]
        if tiles > 1 or not ring:
            before = jnp.where(ids < shift, rights[k - 1] if ring or k else 0.0, before)
            after = jnp.where(ids >= LANES - shift, lefts[(k + 1) % tiles] if ring or k + 1 < tiles else 0.0, after)
        beside = (src[k, r - 1 : r - 1 + n, :] + src[k, r + 1 : r + 1 + n, :]) + (before + after)
        more = add(k, r - 8, n) if callable(add) else add[k, r : r + n, :]
        found.append(scale[k] * (mids[k] + beside) + more)
    return mids, found


def restricted(rest, k, r, n, shift):
    total = rest[k, pl.ds(r, n, stride=2), :] + rest[k, pl.ds(r + 1, n, stride=2), :]
    even = (lane_ids(n) & shift) == 0
    return total + jnp.where(even, roll(total, -shift), roll(total, shift))


def strip_rows(chans, tiles):
    assert tiles == 2 and 2 * chans + 2 <= 8
    at_coarse = 8 * tiles * chans
    at_seam = at_coarse + chans * (HALO // 2)
    return at_coarse, at_seam, at_seam + 8 * -(-STRIP // 16)


def strips(
    a_hbm, b_hbm, x_hbm, cover_ref, label_ref, even_ref, odd_ref,
    a_both, b_both, x_both, picked, other_a, other_b, source, once, rest, built, sems,
):
    chans, block, cols = a_hbm.shape
    rows = HALO
    tiles = cols // LANES
    active = cover_ref[0, 0].astype(jnp.float32)
    marked = label_ref[0, 0].astype(jnp.float32)
    second = label_ref[0, 0] == 1
    eight = lane_ids(8)


    def fetches(step):
        low = pl.multiple_of(step * (block - HALO), 8)
        pairs = ((a_hbm, a_both), (b_hbm, b_both), (x_hbm, x_both))
        return [
            pltpu.make_async_copy(src.at[:, pl.ds(low, HALO), :], dst.at[step], sems.at[i, step])
            for i, (src, dst) in enumerate(pairs)
        ]

    for step in range(2):
        for fetch in fetches(step):
            fetch.start()

    def one_side(step, _):
        for fetch in fetches(step):
            fetch.wait()
        message(step, a_both.at[step], b_both.at[step], x_both.at[step])
        return 0

    def message(step, a_ref, b_ref, x_ref):
        top = step == 0
        start = pl.multiple_of(jnp.where(top, 0, rows - STRIP), 8)
        near = pl.multiple_of(jnp.where(top, 8, rows), 8)
        line = jnp.where(top, 0, rows - 1)
        at_coarse, at_seam, at_marks = strip_rows(chans, tiles)
        scale = [active * NEAR] * tiles
        place = eight & (QUARTER - 1)
        seams = [jnp.zeros((8, LANES), jnp.float32) for _ in range(STRIP // 8)]
        channels = range(chans)
        for c in channels:
            for k in range(tiles):
                for edge in (7, 8 + rows):
                    picked[c, k, edge : edge + 1, :] = jnp.zeros((1, LANES), jnp.float32)
                at = pl.ds(k * LANES, LANES)
                x = x_ref[c, :, at]
                from_a, from_b = a_ref[c, :, at] - x, b_ref[c, :, at] - x
                other_a[c, k], other_b[c, k] = from_a, from_b
                picked[c, k, 8 : 8 + rows, :] = jnp.where(second, from_b, from_a)
        for c in channels:
            parts = [[picked[c, k, 8 + s : 8 + s + rows, :] for k in range(tiles)] for s in (0, -1, 1)]
            for k, found in enumerate(own_source(*parts, active)):
                source[c, k, 8 : 8 + rows, :] = found
        for c in channels:
            src = source.at[c]
            _, found = swept(src, src, scale, 1, 8, rows, False, turn(src, 1, 8, rows))
            for k in range(tiles):
                once[c, k, 8 : 8 + rows, :] = found[k]
        for c in channels:
            mids, found = swept(once.at[c], source.at[c], scale, 1, 8, rows, False, turn(once.at[c], 1, 8, rows))
            for k in range(tiles):
                rest[c, k, 8 : 8 + rows, :] = found[k] - mids[k]
        for c in channels:
            first, last = (restricted(rest.at[c], k, 8, rows // 2, 1) for k in range(tiles))
            low = at_coarse + c * (rows // 2)
            built[low : low + rows // 2, :] = jnp.where((lane_ids(rows // 2) & 1) == 0, first, last)
            for k in range(tiles):
                low = 8 * (tiles * c + k)
                built[low : low + 8, :] = source[c, k, pl.ds(near, 8), :]
                low = at_marks + 8 * k + 2 * c
                built[low : low + 1, :] = other_a[c, k, pl.ds(line, 1), :]
                built[low + 1 : low + 2, :] = other_b[c, k, pl.ds(line, 1), :]
            base = QUARTER * c
            for t in range(STRIP // 8):
                at, own_at = pl.ds(start + 8 * t, 8), pl.ds(8 + start + 8 * t, 8)
                seam = seams[t]
                for cells, cell, lane, width in (
                    (source[c, 0, own_at, :], 0, LEFT, SEAM),
                    (source[c, tiles - 1, own_at, :], LANES - SEAM, RIGHT - SEAM, SEAM),
                    (other_a[c, 0, at, :], 0, LEFT - 1, 1),
                    (other_b[c, 0, at, :], 0, LEFT - 2, 1),
                    (other_a[c, tiles - 1, at, :], LANES - 1, RIGHT, 1),
                    (other_b[c, tiles - 1, at, :], LANES - 1, RIGHT + 1, 1),
                ):
                    spot = (eight >= base + lane) & (eight < base + lane + width)
                    seam = jnp.where(spot, roll(cells, base + lane - cell), seam)
                seams[t] = seam
        for t in range(STRIP // 8):
            slot = 2 * (t & 1)
            if slot == 0:
                packed = jnp.zeros((8, LANES), jnp.float32)
            packed = jnp.where((place >> 3) == slot, roll(seams[t], 8 * slot - (LEFT - 2)), packed)
            packed = jnp.where((place >> 3) == slot + 1, roll(seams[t], 8 * slot + 8 - (RIGHT - SEAM)), packed)
            built[at_seam + 8 * (t // 2) : at_seam + 8 * (t // 2) + 8, :] = packed
        for k in range(tiles):
            low = at_marks + 8 * k + 2 * chans
            built[low : low + 1, :] = jnp.full((1, LANES), active)
            built[low + 1 : low + 2, :] = jnp.full((1, LANES), marked)

        by_odd = top == even_at("group")

        @pl.when(by_odd)
        def _():
            odd_ref[...] = built[...]

        @pl.when(jnp.logical_not(by_odd))
        def _():
            even_ref[...] = built[...]

    lax.fori_loop(0, 2, one_side, 0)


def inside(a_ref, b_ref, x_ref, cover_ref, label_ref, source_ref, once_ref, seam_ref, coarse_ref, da, db, rest):
    chans, rows, cols = a_ref.shape
    tiles = cols // LANES
    active = cover_ref[0, 0].astype(jnp.float32)
    second = label_ref[0, 0] == 1
    for k in range(tiles):
        for buf in (da, db):
            buf[k, 0:8, :] = jnp.zeros((8, LANES), jnp.float32)
            buf[k, rows + 8 : rows + 16, :] = jnp.zeros((8, LANES), jnp.float32)
    scale = [active * NEAR] * tiles
    top, end = HALO, HALO + rows

    def pick(k, low, n):
        return jnp.where(second, db[k, low : low + n, :], da[k, low : low + n, :])

    seam_ref[...] = jnp.zeros(seam_ref.shape, jnp.float32)

    def channel(c, _):
        for k in range(tiles):
            at = pl.ds(k * LANES, LANES)
            for r, n in spans(0, rows):
                x = x_ref[c, r : r + n, at]
                da[k, 8 + r : 8 + r + n, :] = a_ref[c, r : r + n, at] - x
                db[k, 8 + r : 8 + r + n, :] = b_ref[c, r : r + n, at] - x
        for r, n in spans(0, rows):
            parts = [[pick(k, 8 + s + r, n) for k in range(tiles)] for s in (0, -1, 1)]
            found = own_source(*parts, active)
            for k in range(tiles):
                source_ref[c, k, top + r : top + r + n, :] = found[k]
            ids = lane_ids(n)
            base = QUARTER * c
            at = pl.ds(8 + r, n)
            seam = pltpu.roll(found[0], base + LEFT, 1)
            for source, cell, lane in (
                (found[tiles - 1], LANES - SEAM, RIGHT - SEAM),
                (da[0, at, :], 0, LEFT - 1),
                (db[0, at, :], 0, LEFT - 2),
                (da[tiles - 1, at, :], LANES - 1, RIGHT),
                (db[tiles - 1, at, :], LANES - 1, RIGHT + 1),
            ):
                spot = (ids >= base + lane) & (ids < base + lane + (SEAM if cell == LANES - SEAM else 1))
                seam = jnp.where(spot, pltpu.roll(source, base + lane + (LANES - cell) % LANES, 1), seam)
            at = pl.ds(top + r, n)
            mine = (ids >= base + LEFT - 2) & (ids < base + RIGHT + 2)
            mine = mine & ((ids < base + LEFT + SEAM) | (ids >= base + RIGHT - SEAM))
            seam_ref[at, :] = jnp.where(mine, seam, seam_ref[at, :])
        source, once = source_ref.at[c], once_ref.at[c]

        def first(piece, turned):
            r, n = piece
            _, found = swept(source, source, scale, 1, r, n, False, turned)
            for k in range(tiles):
                once_ref[c, k, r : r + n, :] = found[k]

        def second_sweep(piece, turned):
            r, n = piece
            mids, found = swept(once, source, scale, 1, r, n, False, turned)
            for k in range(tiles):
                rest[k, r : r + n, :] = found[k] - mids[k]

        staggered(spans(top, end), lambda piece: turn(source, 1, *piece), first, 0)
        staggered(spans(top, end), lambda piece: turn(once, 1, *piece), second_sweep, 0)
        for r, n in spans(top // 2, end // 2):
            for k in range(tiles):
                coarse_ref[c, k, r : r + n, :] = restricted(rest, k, 2 * r, n, 1)
        return 0

    lax.fori_loop(0, chans, channel, 0)


def seam_units(height):
    for t in range((height - 2 * FIRST) // 8):
        yield FIRST + 8 * t, t // 4, t % 4


def message_rows(chans, height):
    quarter = height // 2
    cells = (chans // 2 * quarter + chans % 2 * quarter // 2) // 2
    return cells, -(-(height - 2 * FIRST) // 32) * 8


def column_rows(chans, height):
    quarter = height // 2
    places = [(c, r, c + 1, r) for c in range(0, chans - 1, 2) for r in range(0, quarter, 8)]
    if chans % 2:
        places += [(chans - 1, r, chans - 1, r + quarter // 2) for r in range(0, quarter // 2, 8)]
    return places


def join_rows(
    source_in, once_in, seam_in, coarse_in, sent_even, sent_odd, got_even, got_odd, cover_ref, label_ref,
    source_ref, once_ref, seam_ref, coarse_ref, even_ref, odd_ref, rest, marks_ref, upper_got, lower_got, lines, left_out, right_out,
):
    chans, tiles, height, _ = source_ref.shape
    rows = height - 2 * HALO
    row_even, col_even = even_at("group"), even_at("blk")
    active = cover_ref[0, 0].astype(jnp.float32)
    marked = label_ref[0, 0].astype(jnp.float32)
    eight = lane_ids(8)

    place = eight & (QUARTER - 1)

    at_coarse, at_seam, at_marks = strip_rows(chans, tiles)

    def take(top, got):
        near = HALO - 8 if top else HALO + rows
        mine = lines[0 if top else 1]
        edge = HALO if top else HALO + rows - 1
        other = edge - 1 if top else edge + 1
        their_active = got[at_marks + 2 * chans : at_marks + 2 * chans + 1, :]
        their_mark = got[at_marks + 2 * chans + 1 : at_marks + 2 * chans + 2, :]
        band = 0 if top else 2
        marks_ref[band : band + 1, :] = their_active
        marks_ref[band + 3 : band + 4, :] = their_mark
        half_halo = HALO // 2
        coarse_at = 0 if top else (height - HALO) // 2
        even_cell = (lane_ids(half_halo) & 1) == 0
        for c in range(chans):
            cells = got[at_coarse + c * half_halo : at_coarse + (c + 1) * half_halo, :]
            at = pl.ds(coarse_at, half_halo)
            coarse_ref[c, 0, at, :] = jnp.where(even_cell, cells, roll(cells, 1))
            coarse_ref[c, 1, at, :] = jnp.where(even_cell, roll(cells, -1), cells)
            for k in range(tiles):
                source_ref[c, k, near : near + 8, :] = got[8 * (tiles * c + k) : 8 * (tiles * c + k) + 8, :]
                low = at_marks + 8 * k + 2 * c
                their_a, their_b = got[low : low + 1, :], got[low + 1 : low + 2, :]
                my_a, my_b = mine[k, 2 * c : 2 * c + 1, :], mine[k, 2 * c + 1 : 2 * c + 2, :]
                for_mine = NEAR * active * jnp.where(marked == 1.0, their_b, their_a)
                for_theirs = NEAR * their_active * jnp.where(their_mark == 1.0, my_b, my_a)
                source_ref[c, k, edge : edge + 1, :] = source_ref[c, k, edge : edge + 1, :] - for_mine
                source_ref[c, k, other : other + 1, :] = source_ref[c, k, other : other + 1, :] - for_theirs

        def seam_of(r, cells):
            for c in range(chans):
                base = QUARTER * c
                spot = (eight >= base + LEFT) & (eight < base + LEFT + SEAM)
                cells = jnp.where(spot, roll(source_ref[c, 0, r : r + 8, :], base + LEFT), cells)
                spot = (eight >= base + RIGHT - SEAM) & (eight < base + RIGHT)
                cells = jnp.where(spot, roll(source_ref[c, tiles - 1, r : r + 8, :], base + RIGHT), cells)
            seam_ref[r : r + 8, :] = cells

        in_left = (place >= LEFT - 2) & (place < LEFT + SEAM)
        in_right = (place >= RIGHT - SEAM) & (place < RIGHT + 2)
        for t in range(STRIP // 8):
            packed = got[at_seam + 8 * (t // 2) : at_seam + 8 * (t // 2) + 8, :]
            slot = 2 * (t & 1)
            firsts = jnp.where(in_left, roll(packed, LEFT - 2 - 8 * slot), 0.0)
            cells = jnp.where(in_right, roll(packed, RIGHT - SEAM - 8 * slot - 8), firsts)
            cells = jnp.where(eight < QUARTER * chans, cells, 0.0)
            r = (FIRST if top else HALO + rows) + 8 * t
            if r == near:
                seam_of(r, cells)
            else:
                seam_ref[r : r + 8, :] = cells
        r = edge // 8 * 8
        seam_of(r, seam_ref[r : r + 8, :])

    def arrange(upper, lower, mine_up, mine_low):
        upper_got[...] = upper[...]
        lower_got[...] = lower[...]
        for k in range(tiles):
            at = pl.ds(at_marks + 8 * k, 8)
            lines[0, k], lines[1, k] = mine_up[at, :], mine_low[at, :]

    @pl.when(row_even)
    def _():
        arrange(got_odd, got_even, sent_odd, sent_even)

    @pl.when(jnp.logical_not(row_even))
    def _():
        arrange(got_even, got_odd, sent_even, sent_odd)

    take(True, upper_got)
    take(False, lower_got)
    marks_ref[1:2, :] = jnp.full((1, LANES), active)
    marks_ref[4:5, :] = jnp.full((1, LANES), marked)
    marks_ref[6:8, :] = jnp.zeros((2, LANES), jnp.float32)

    bottom = HALO + rows
    edges = ((HALO - 8, HALO, 0), (HALO, HALO + RIM, 1), (bottom - RIM, bottom, 1), (bottom, bottom + 8, 2))
    spots = [(c, band, r, n) for c in range(chans) for low, high, band in edges for r, n in spans(low, high)]
    for stage in range(2):
        held = (source_ref, once_ref)[stage]

        def edge_sweep(spot, turned):
            c, band, r, n = spot
            scale = [jnp.broadcast_to(marks_ref[band : band + 1, :] * NEAR, (n, LANES))] * tiles
            mids, found = swept(held.at[c], source_ref.at[c], scale, 1, r, n, False, turned)
            for k in range(tiles):
                if stage == 0:
                    once_ref[c, k, r : r + n, :] = found[k]
                else:
                    rest[c, k, r : r + n, :] = found[k] - mids[k]

        staggered(spots, lambda spot: turn(held.at[spot[0]], 1, *spot[2:]), edge_sweep, 0)
    for c in range(chans):
        for low, high in ((HALO - 4, HALO + RIM), (bottom - RIM, bottom + 4)):
            for k in range(tiles):
                coarse_ref[c, k, low // 2 : high // 2, :] = restricted(rest.at[c], k, low, (high - low) // 2, 1)

    cells, units = message_rows(chans, height)
    first_half = eight < HALF
    even_lane = (eight & 1) == 0

    def edge_cells(c, r):
        return jnp.where(first_half, coarse_ref[c, 0, r : r + 8, :], coarse_ref[c, tiles - 1, r : r + 8, :])

    def joined(place):
        c, r, d, s = place
        return jnp.where(even_lane, edge_cells(c, r), edge_cells(d, s))

    def pack(left, right):
        places = column_rows(chans, height)
        for t in range(cells // 8):
            upper, lower = joined(places[t]), joined(places[t + cells // 8])
            left[8 * t : 8 * t + 8, :] = jnp.where(first_half, upper, roll(lower, HALF))
            right[8 * t : 8 * t + 8, :] = jnp.where(first_half, roll(upper, HALF), lower)
        lefts = rights = jnp.zeros((8, LANES), jnp.float32)
        for r, tile, slot in seam_units(height):
            value = seam_ref[r : r + 8, :]
            spot = (place >> 3) == slot
            lefts = jnp.where(spot, roll(value, 8 * slot - (LEFT - 2)), lefts)
            rights = jnp.where(spot, roll(value, 8 * slot - (RIGHT - SEAM)), rights)
            at = cells + 8 * tile
            left[at : at + 8, :], right[at : at + 8, :] = lefts, rights
        for out in (left, right):
            out[cells + units : cells + units + 8, :] = marks_ref[...]

    pack(left_out, right_out)

    @pl.when(col_even)
    def _():
        odd_ref[...] = left_out[...]
        even_ref[...] = right_out[...]

    @pl.when(jnp.logical_not(col_even))
    def _():
        even_ref[...] = left_out[...]
        odd_ref[...] = right_out[...]


def cycle(
    source_in, once_in, seam_in, coarse_in, sent_even, got_even, got_odd, x_ref, out_hbm,
    out_ref, sems, right_ref, left_ref, seam_source, seam_once, seam_rest, fine, fine_two, fix, *bufs,
):
    chans, own_tiles, height, _ = source_in.shape
    rows = height - 2 * HALO
    tiles = own_tiles + 1
    cells, units = message_rows(chans, height)
    col_even = even_at("blk")
    eight = lane_ids(8)

    @pl.when(col_even)
    def _():
        right_ref[...] = got_even[...]
        left_ref[...] = got_odd[...]

    @pl.when(jnp.logical_not(col_even))
    def _():
        right_ref[...] = got_odd[...]
        left_ref[...] = got_even[...]

    at = cells + units

    def mark(ref, row):
        return jnp.broadcast_to(ref[at + row : at + row + 1, :], (8, LANES))

    own = [mark(sent_even, i) for i in range(6)]
    right = [mark(right_ref, i) for i in range(6)]
    left = [mark(left_ref, i) for i in range(6)]
    first_half = eight < HALF
    place = eight & (QUARTER - 1)

    def mixed(i):
        return jnp.where(place < LEFT, left[i], jnp.where(place < RIGHT, own[i], right[i]))

    seam_scale = [jnp.where(eight < QUARTER * chans, mixed(i), 0.0) * NEAR for i in range(3)]
    seam_mark = [mixed(i + 3) == 1.0 for i in range(3)]
    own_scale = [own[i] * NEAR for i in range(3)]
    side_scale = [jnp.where(first_half, right[i], left[i]) * NEAR for i in range(3)]

    def wide(mask, n):
        return jnp.broadcast_to(mask[:1], (n, LANES))

    def over_rows(kinds, depth, r, n):
        full, halo = height >> depth, HALO >> depth
        ends = ((0, halo), (halo, full - halo), (full - halo, full))
        parts = [(max(a, r), min(b, r + n), kind) for (a, b), kind in zip(ends, kinds)]
        parts = [wide(kind, b - a) for a, b, kind in parts if b > a]
        return parts[0] if len(parts) == 1 else jnp.concatenate(parts, axis=0)

    def scales(depth, r, n):
        return [over_rows(own_scale, depth, r, n)] * own_tiles + [over_rows(side_scale, depth, r, n)]

    inner = ((place >= LEFT) & (place < LEFT + SEAM)) | ((place >= RIGHT - SEAM) & (place < RIGHT))
    outer = ((place >= LEFT - SEAM) & (place < LEFT)) | ((place >= RIGHT) & (place < RIGHT + SEAM))
    from_near = (place == LEFT) | (place == RIGHT - 1)
    from_own = (place == LEFT - 1) | (place == RIGHT)
    up_one = (place == LEFT - 1) | (place == RIGHT - 1)
    near_b = (place == LEFT + 1) | (place == RIGHT - 2)
    right_unit = place >= RIGHT - 2

    def unpack(unit):
        r, tile, slot = unit
        rights = roll(right_ref[cells + 8 * tile : cells + 8 * tile + 8, :], RIGHT - 2 - 8 * slot)
        lefts = roll(left_ref[cells + 8 * tile : cells + 8 * tile + 8, :], LEFT - SEAM - 8 * slot)
        return rights, lefts

    def keep_near(unit, turned):
        r = unit[0]
        seam_rest[0, r : r + 8, :] = jnp.where(right_unit, *turned)

    def second_cells(unit):
        r = unit[0]
        cells_b = jnp.where(near_b, seam_rest[0, r : r + 8, :], seam_in[r : r + 8, :])
        return roll(cells_b, 1), roll(cells_b, -1)

    def put_seam(unit, turned):
        r = unit[0]
        band = 0 if r < HALO else 1 if r < HALO + rows else 2
        near, mine = seam_rest[0, r : r + 8, :], seam_in[r : r + 8, :]
        value = jnp.where(inner, mine, jnp.where(outer, near, 0.0))
        border = jnp.where(seam_mark[band], jnp.where(up_one, *turned), jnp.where(from_near, near, mine))
        border = jnp.where(from_near | from_own, border, 0.0)
        seam_source[0, r : r + 8, :] = value - seam_scale[band] * border

    staggered(seam_units(height), unpack, keep_near, 24)
    staggered(seam_units(height), second_cells, put_seam, 24)
    for r, n in spans(FIRST, height - FIRST, height):
        _, found = swept(
            seam_source, seam_source, [over_rows(seam_scale, 0, r, n)], 1, r, n, True, turn(seam_source, 1, r, n)
        )
        seam_once[0, r : r + n, :] = found[0]
        mids, found = swept(
            seam_once, seam_source, [over_rows(seam_scale, 0, r, n)], 1, r, n, True, turn(seam_once, 1, r, n)
        )
        seam_rest[0, r : r + n, :] = found[0] - mids[0]

    one_src, one_once, one_two = bufs[0:3]
    half_rows = height // 2
    eights = lane_ids(8)
    even_lane = (eights & 1) == 0
    places = column_rows(chans, height)
    for t, (c, r, d, s) in enumerate(places):
        low, upper = (8 * t, True) if t < cells // 8 else (8 * t - cells, False)
        from_right, from_left = right_ref[low : low + 8, :], left_ref[low : low + 8, :]
        if upper:
            value = jnp.where(first_half, from_right, roll(from_left, HALF))
        else:
            value = jnp.where(first_half, roll(from_right, HALF), from_left)
        if c == d:
            one_src[c // 2, own_tiles, 8 + r : 16 + r, :] = jnp.where(even_lane, value, roll(value, 1))
            one_src[c // 2, own_tiles, 8 + s : 16 + s, :] = jnp.where(even_lane, roll(value, -1), value)
        else:
            one_src[c // 2, own_tiles, 8 + r : 16 + r, :] = value

    pairs = [(c, min(c + 1, chans - 1)) for c in range(0, chans, 2)]

    def paired(of, pair, n):
        first, second = pair
        return of(first) if first == second else jnp.where((lane_ids(n) & 1) == 0, of(first), of(second))

    for f, pair in enumerate(pairs):
        for r, n in spans(0, half_rows):
            for k in range(own_tiles):
                one_src[f, k, 8 + r : 8 + r + n, :] = paired(lambda c: coarse_in[c, k, r : r + n, :], pair, n)
    for r, n in spans(FIRST // 2, half_rows - FIRST // 2):
        ids = lane_ids(n)
        seam = restricted(seam_rest, 0, 2 * r, n, 1)
        at = pl.ds(8 + r, n)
        for f, pair in enumerate(pairs):
            by_left = paired(lambda c: roll(seam, -QUARTER * c - LEFT), pair, n)
            by_right = paired(lambda c: roll(seam, -QUARTER * c - RIGHT), pair, n)
            one_src[f, 0, at, :] = jnp.where(ids < 4, by_left, one_src[f, 0, at, :])
            inner_end = one_src[f, own_tiles - 1, at, :]
            one_src[f, own_tiles - 1, at, :] = jnp.where(ids >= LANES - 4, by_right, inner_end)
            side = jnp.where(ids < 4, by_right, one_src[f, own_tiles, at, :])
            one_src[f, own_tiles, at, :] = jnp.where(ids >= LANES - 4, by_left, side)

    def smooth(src, once, fields, depth, into, minus=False):
        def one_sweep(spot, turned):
            f, r, n = spot
            mids, found = swept(once.at[f], src.at[f], scales(depth, r, n), 1 << depth, 8 + r, n, True, turned)
            for k in range(tiles):
                into[f, k, 8 + r : 8 + r + n, :] = found[k] - mids[k] if minus else found[k]

        spots = [(f, r, n) for f in range(fields) for r, n in spans(0, height >> depth)]
        staggered(spots, lambda spot: turn(once.at[spot[0]], 1 << depth, 8 + spot[1], spot[2]), one_sweep, 0)

    def expand(fix, fields, depth, out, low, high, spread):
        for f in range(fields):
            for r, n in spans(low, high):
                scale = scales(depth + 1, r, n)
                for k in range(tiles):
                    value = fix[0 if spread else f, k, 8 + r : 8 + r + n, :]
                    if spread:
                        value = spread(value, f)
                    value = value * (scale[k] * (1.0 / NEAR))
                    out[f, k, pl.ds(8 + 2 * r, n, stride=2), :] = value
                    out[f, k, pl.ds(9 + 2 * r, n, stride=2), :] = value

    def add_fix(once, two, fields, depth, into):
        for f in range(fields):
            for r, n in spans(0, height >> depth):
                for k in range(tiles):
                    at = pl.ds(8 + r, n)
                    into[f, k, at, :] = once[f, k, at, :] + two[f, k, at, :]

    assert chans <= 4 and LEVELS >= 3

    def spread_pair(value, f):
        high = (lane_ids(value.shape[0]) & 2) == 2
        return jnp.where(high, value, roll(value, -2)) if f else jnp.where(high, roll(value, 2), value)

    def level(depth):
        src, once, two = bufs[3 * (depth - 1) : 3 * depth]
        fields = len(pairs) if depth == 1 else 1
        if depth == LEVELS - 1:
            held = src
            for sweep in range(1, COARSE):
                into = (once, two)[sweep % 2]
                smooth(src, held, fields, depth, into)
                held = into
            return held
        smooth(src, src, fields, depth, once)
        smooth(src, once, fields, depth, two, True)
        below = bufs[3 * depth]
        shift = 1 << depth
        for r, n in spans(0, height >> (depth + 1)):
            half = (lane_ids(n) & 2) >> 1
            for k in range(tiles):
                value = None
                for f in range(fields):
                    total = restricted(two.at[f], k, 8 + 2 * r, n, shift)
                    value = total if value is None else jnp.where(half == f, total, value)
                below[0, k, 8 + r : 8 + r + n, :] = value
        fix = level(depth + 1)
        expand(fix, fields, depth, two, 0, height >> (depth + 1), spread_pair if depth == 1 else None)
        add_fix(once, two, fields, depth, once)
        smooth(src, once, fields, depth, two)
        smooth(src, two, fields, depth, once)
        return once

    paired_fix = level(1)
    low, high = HALO - RIM, HALO + rows + RIM
    for f, (even, odd) in enumerate(pairs):
        for r, n in spans(low // 2, high // 2):
            at = pl.ds(8 + r, n)
            odd_lane = (lane_ids(n) & 1) == 1
            for k in range(tiles):
                value = paired_fix[f, k, at, :]
                if even == odd:
                    fix[even, k, at, :] = value
                else:
                    fix[even, k, at, :] = jnp.where(odd_lane, roll(value, 1), value)
                    fix[odd, k, at, :] = jnp.where(odd_lane, value, roll(value, -1))

    def at_borders(seam, c):
        base = QUARTER * c
        return pltpu.roll(seam, LANES - LEFT - base, 1), pltpu.roll(seam, LANES - RIGHT - base, 1)

    def fine_source(c):
        def tile(k, r, n):
            ids = lane_ids(n)
            by_left, by_right = at_borders(seam_source[0, r : r + n, :], c)
            if k == own_tiles:
                return jnp.where(ids < HALF, by_right, by_left)
            value = source_in[c, k, r : r + n, :]
            if k == 0:
                value = jnp.where(ids == 0, by_left, value)
            if k == own_tiles - 1:
                value = jnp.where(ids == LANES - 1, by_right, value)
            return value

        return tile

    for c in range(chans):
        for r, n in spans(low // 2, high // 2):
            scale = scales(1, r, n)
            for k in range(tiles):
                value = fix[c, k, 8 + r : 8 + r + n, :] * (scale[k] * (1.0 / NEAR))
                fine[c, k, pl.ds(8 + 2 * r, n, stride=2), :] = value
                fine[c, k, pl.ds(9 + 2 * r, n, stride=2), :] = value
    for c in range(chans):
        for r, n in spans(low, high):
            ids = lane_ids(n)
            by_left, by_right = at_borders(seam_once[0, r : r + n, :], c)
            at = pl.ds(8 + r, n)
            for k in range(own_tiles):
                value = once_in[c, k, r : r + n, :]
                if k == 0:
                    value = jnp.where(ids < 2, by_left, value)
                if k == own_tiles - 1:
                    value = jnp.where(ids >= LANES - 2, by_right, value)
                fine[c, k, at, :] = fine[c, k, at, :] + value
            fine[c, own_tiles, at, :] = fine[c, own_tiles, at, :] + jnp.where(ids < HALF, by_right, by_left)
    for c in range(chans):
        add, src = fine_source(c), fine.at[c]
        for r, n in spans(low, high):
            _, found = swept(src, add, scales(0, r, n), 1, 8 + r, n, True, turn(src, 1, 8 + r, n))
            for k in range(tiles):
                fine_two[c, k, 8 + r : 8 + r + n, :] = found[k]

    def leave(c):
        return pltpu.make_async_copy(out_ref.at[c], out_hbm.at[c], sems.at[c])

    for c in range(chans):
        add, src = fine_source(c), fine_two.at[c]
        for r, n in spans(HALO, HALO + rows):
            _, found = swept(src, add, scales(0, r, n), 1, 8 + r, n, True, turn(src, 1, 8 + r, n), own_tiles)
            for k in range(own_tiles):
                at = pl.ds(k * LANES, LANES)
                out_ref[c, r - HALO : r - HALO + n, at] = x_ref[c, r - HALO : r - HALO + n, at] + found[k]
        leave(c).start()
    for c in range(chans):
        leave(c).wait()


def swaps(count, odd):
    pairs = [(i, i + 1) for i in range(odd, count - 1, 2)]
    return pairs + [(j, i) for i, j in pairs]


def shards(image_a, image_b, initial, coverage, seam_label):
    chans, rows, cols = image_a.shape
    tiles = cols // LANES
    height = rows + 2 * HALO
    vmem = pl.BlockSpec(memory_space=pltpu.VMEM)
    smem = pl.BlockSpec(memory_space=pltpu.SMEM)
    hbm = pl.BlockSpec(memory_space=pltpu.HBM)
    f32 = jnp.float32
    sds = functools.partial(jax.ShapeDtypeStruct, dtype=f32)
    params = pltpu.CompilerParams(vmem_limit_bytes=40 * 1024 * 1024)
    group, blk = lax.axis_size("group"), lax.axis_size("blk")
    central = sds((chans, tiles, height, LANES))
    assert chans <= 4
    column = sds((height, LANES))
    coarse = sds((chans, tiles, height // 2, LANES))
    upright = sds((strip_rows(chans, tiles)[2] + 8 * tiles, LANES))
    beside = sds((sum(message_rows(chans, height)) + 8, LANES))

    sent_even, sent_odd = pl.pallas_call(
        strips,
        out_shape=(upright, upright),
        in_specs=[hbm, hbm, hbm, smem, smem],
        out_specs=(vmem, vmem),
        scratch_shapes=[pltpu.VMEM((2, chans, HALO, cols), f32)] * 3
        + [pltpu.VMEM((chans, tiles, HALO + 16, LANES), f32)]
        + [pltpu.VMEM((chans, tiles, HALO, LANES), f32)] * 2
        + [pltpu.VMEM((chans, tiles, HALO + 16, LANES), f32)] * 3
        + [pltpu.VMEM(upright.shape, f32), pltpu.SemaphoreType.DMA((3, 2))],
        compiler_params=pltpu.CompilerParams(vmem_limit_bytes=56_000_000),
        name="strips",
    )(image_a, image_b, initial, coverage, seam_label)
    got_even = lax.ppermute(sent_even, "group", swaps(group, 0))
    got_odd = lax.ppermute(sent_odd, "group", swaps(group, 1))

    source, once, seam, coarser = pl.pallas_call(
        inside,
        out_shape=(central, central, column, coarse),
        in_specs=[vmem, vmem, vmem, smem, smem],
        out_specs=(vmem,) * 4,
        scratch_shapes=[pltpu.VMEM((tiles, rows + 16, LANES), f32)] * 2 + [pltpu.VMEM((tiles, height, LANES), f32)],
        compiler_params=params,
        cost_estimate=pl.CostEstimate(flops=200_000_000, bytes_accessed=4_000_000, transcendentals=0),
        name="inside",
    )(image_a, image_b, initial, coverage, seam_label)

    source, once, seam, coarser, sent_even, sent_odd = pl.pallas_call(
        join_rows,
        out_shape=(central, central, column, coarse, beside, beside),
        in_specs=[vmem] * 8 + [smem] * 2,
        out_specs=(vmem,) * 6,
        input_output_aliases={0: 0, 1: 1, 2: 2, 3: 3},
        scratch_shapes=[pltpu.VMEM(central.shape, f32), pltpu.VMEM((8, LANES), f32)]
        + [pltpu.VMEM(upright.shape, f32)] * 2
        + [pltpu.VMEM((2, tiles, 8, LANES), f32)]
        + [pltpu.VMEM(beside.shape, f32)] * 2,
        compiler_params=params,
        name="join_rows",
    )(source, once, seam, coarser, sent_even, sent_odd, got_even, got_odd, coverage, seam_label)
    got_even = lax.ppermute(sent_even, "blk", swaps(blk, 0))
    got_odd = lax.ppermute(sent_odd, "blk", swaps(blk, 1))

    scratch = [pltpu.VMEM(image_a.shape, f32), pltpu.SemaphoreType.DMA((chans,))]
    scratch += [pltpu.VMEM(beside.shape, f32)] * 2 + [pltpu.VMEM((1, height, LANES), f32)] * 3
    scratch += [pltpu.VMEM((chans, tiles + 1, height + 16, LANES), f32)] * 2
    scratch += [pltpu.VMEM((chans, tiles + 1, height // 2 + 16, LANES), f32)]
    for depth in range(1, LEVELS):
        fields = (chans + 1) // 2 if depth == 1 else 1
        scratch += [pltpu.VMEM((fields, tiles + 1, (height >> depth) + 16, LANES), f32)] * 3
    return pl.pallas_call(
        cycle,
        out_shape=sds((chans, rows, cols)),
        in_specs=[vmem] * 8,
        out_specs=hbm,
        scratch_shapes=scratch,
        compiler_params=params,
        name="cycle",
    )(source, once, seam, coarser, sent_even, got_even, got_odd, initial)


def solution(mesh):
    placed = (
        P(None, "group", "blk"),
        P(None, "group", "blk"),
        P(None, "group", "blk"),
        P("group", "blk"),
        P("group", "blk"),
    )
    return jax.shard_map(
        shards, mesh=mesh, in_specs=placed, out_specs=P(None, "group", "blk"), check_vma=False
    )
```

```python
import functools

import jax
import jax.numpy as jnp
from jax import lax
from jax.experimental import pallas as pl
from jax.experimental.pallas import tpu as pltpu
from jax.sharding import PartitionSpec as P

LEVELS = 4
NU = 2
COARSE = 4
RELAX = 0.8
NEAR = 0.25 * RELAX

LANES = 128
HALF = LANES // 2
HALO = 64
STEP = 96


def source_reach():
    need = 0
    for _ in range(LEVELS - 1):
        need = -(-(need + NU) // 2)
    need += COARSE - 1
    for _ in range(LEVELS - 1):
        need = 2 * need + NU
    return need


REACH = source_reach()
STRIP = REACH + 2
assert STRIP % 8 == 0 and STRIP <= HALO
FIRST = HALO - STRIP
RIM = 8
SEAM = 6
QUARTER = LANES // 4
LEFT, RIGHT = 8, 24


def lane_ids(rows):
    return lax.broadcasted_iota(jnp.int32, (rows, LANES), 1)


def roll(tile, shift):
    return pltpu.roll(tile, shift % LANES, 1)


def spans(low, high, step=STEP):
    while low < high:
        yield low, min(step, high - low)
        low += step


def even_at(axis):
    return lax.rem(lax.axis_index(axis), 2) == 0


def own_source(mids, ups, downs, active):
    tiles = len(mids)
    rights = [roll(t, 1) for t in mids]
    lefts = [roll(t, -1) for t in mids]
    ids = lane_ids(mids[0].shape[0])
    found = []
    for k in range(tiles):
        before = jnp.where(ids == 0, rights[k - 1] if k else 0.0, rights[k])
        after = jnp.where(ids == LANES - 1, lefts[k + 1] if k + 1 < tiles else 0.0, lefts[k])
        beside = (ups[k] + downs[k]) + (before + after)
        found.append(active * (RELAX * mids[k] - NEAR * beside))
    return found


def staggered(items, begin, end, depth):
    waiting = []
    for item in items:
        waiting.append((item, begin(item)))
        if len(waiting) > depth:
            end(*waiting.pop(0))
    for each in waiting:
        end(*each)


def turn(src, shift, r, n):
    tiles = range(src.shape[0])
    return [roll(src[k, r : r + n, :], shift) for k in tiles], [roll(src[k, r : r + n, :], -shift) for k in tiles]


def swept(src, add, scale, shift, r, n, ring, turned, keep=None):
    tiles = src.shape[0]
    ids = lane_ids(n)
    mids = [src[k, r : r + n, :] for k in range(tiles)]
    rights, lefts = turned
    found = []
    for k in range(keep or tiles):
        before, after = rights[k], lefts[k]
        if tiles > 1 or not ring:
            before = jnp.where(ids < shift, rights[k - 1] if ring or k else 0.0, before)
            after = jnp.where(ids >= LANES - shift, lefts[(k + 1) % tiles] if ring or k + 1 < tiles else 0.0, after)
        beside = (src[k, r - 1 : r - 1 + n, :] + src[k, r + 1 : r + 1 + n, :]) + (before + after)
        more = add(k, r - 8, n) if callable(add) else add[k, r : r + n, :]
        found.append(scale[k] * (mids[k] + beside) + more)
    return mids, found


def restricted(rest, k, r, n, shift):
    total = rest[k, pl.ds(r, n, stride=2), :] + rest[k, pl.ds(r + 1, n, stride=2), :]
    even = (lane_ids(n) & shift) == 0
    return total + jnp.where(even, roll(total, -shift), roll(total, shift))


def strip_rows(chans, tiles):
    assert tiles == 2 and 2 * chans + 2 <= 8
    at_coarse = 8 * tiles * chans
    at_seam = at_coarse + chans * (HALO // 2)
    return at_coarse, at_seam, at_seam + 8 * -(-STRIP // 16)


def strips(
    a_hbm, b_hbm, x_hbm, cover_ref, label_ref, even_ref, odd_ref,
    a_both, b_both, x_both, picked, other_a, other_b, source, once, rest, built, sems,
):
    chans, block, cols = a_hbm.shape
    rows = HALO
    tiles = cols // LANES
    active = cover_ref[0, 0].astype(jnp.float32)
    marked = label_ref[0, 0].astype(jnp.float32)
    second = label_ref[0, 0] == 1
    eight = lane_ids(8)


    def fetches(step):
        low = pl.multiple_of(step * (block - HALO), 8)
        pairs = ((a_hbm, a_both), (b_hbm, b_both), (x_hbm, x_both))
        return [
            pltpu.make_async_copy(src.at[:, pl.ds(low, HALO), :], dst.at[step], sems.at[i, step])
            for i, (src, dst) in enumerate(pairs)
        ]

    for step in range(2):
        for fetch in fetches(step):
            fetch.start()

    def one_side(step, _):
        for fetch in fetches(step):
            fetch.wait()
        message(step, a_both.at[step], b_both.at[step], x_both.at[step])
        return 0

    def message(step, a_ref, b_ref, x_ref):
        top = step == 0
        start = pl.multiple_of(jnp.where(top, 0, rows - STRIP), 8)
        near = pl.multiple_of(jnp.where(top, 8, rows), 8)
        line = jnp.where(top, 0, rows - 1)
        at_coarse, at_seam, at_marks = strip_rows(chans, tiles)
        scale = [active * NEAR] * tiles
        place = eight & (QUARTER - 1)
        seams = [jnp.zeros((8, LANES), jnp.float32) for _ in range(STRIP // 8)]
        channels = range(chans)
        for c in channels:
            for k in range(tiles):
                for edge in (7, 8 + rows):
                    picked[c, k, edge : edge + 1, :] = jnp.zeros((1, LANES), jnp.float32)
                at = pl.ds(k * LANES, LANES)
                x = x_ref[c, :, at]
                from_a, from_b = a_ref[c, :, at] - x, b_ref[c, :, at] - x
                other_a[c, k], other_b[c, k] = from_a, from_b
                picked[c, k, 8 : 8 + rows, :] = jnp.where(second, from_b, from_a)
        for c in channels:
            parts = [[picked[c, k, 8 + s : 8 + s + rows, :] for k in range(tiles)] for s in (0, -1, 1)]
            for k, found in enumerate(own_source(*parts, active)):
                source[c, k, 8 : 8 + rows, :] = found
        for c in channels:
            src = source.at[c]
            _, found = swept(src, src, scale, 1, 8, rows, False, turn(src, 1, 8, rows))
            for k in range(tiles):
                once[c, k, 8 : 8 + rows, :] = found[k]
        for c in channels:
            mids, found = swept(once.at[c], source.at[c], scale, 1, 8, rows, False, turn(once.at[c], 1, 8, rows))
            for k in range(tiles):
                rest[c, k, 8 : 8 + rows, :] = found[k] - mids[k]
        for c in channels:
            first, last = (restricted(rest.at[c], k, 8, rows // 2, 1) for k in range(tiles))
            low = at_coarse + c * (rows // 2)
            built[low : low + rows // 2, :] = jnp.where((lane_ids(rows // 2) & 1) == 0, first, last)
            for k in range(tiles):
                low = 8 * (tiles * c + k)
                built[low : low + 8, :] = source[c, k, pl.ds(near, 8), :]
                low = at_marks + 8 * k + 2 * c
                built[low : low + 1, :] = other_a[c, k, pl.ds(line, 1), :]
                built[low + 1 : low + 2, :] = other_b[c, k, pl.ds(line, 1), :]
            base = QUARTER * c
            for t in range(STRIP // 8):
                at, own_at = pl.ds(start + 8 * t, 8), pl.ds(8 + start + 8 * t, 8)
                seam = seams[t]
                for cells, cell, lane, width in (
                    (source[c, 0, own_at, :], 0, LEFT, SEAM),
                    (source[c, tiles - 1, own_at, :], LANES - SEAM, RIGHT - SEAM, SEAM),
                    (other_a[c, 0, at, :], 0, LEFT - 1, 1),
                    (other_b[c, 0, at, :], 0, LEFT - 2, 1),
                    (other_a[c, tiles - 1, at, :], LANES - 1, RIGHT, 1),
                    (other_b[c, tiles - 1, at, :], LANES - 1, RIGHT + 1, 1),
                ):
                    spot = (eight >= base + lane) & (eight < base + lane + width)
                    seam = jnp.where(spot, roll(cells, base + lane - cell), seam)
                seams[t] = seam
        for t in range(STRIP // 8):
            slot = 2 * (t & 1)
            if slot == 0:
                packed = jnp.zeros((8, LANES), jnp.float32)
            packed = jnp.where((place >> 3) == slot, roll(seams[t], 8 * slot - (LEFT - 2)), packed)
            packed = jnp.where((place >> 3) == slot + 1, roll(seams[t], 8 * slot + 8 - (RIGHT - SEAM)), packed)
            built[at_seam + 8 * (t // 2) : at_seam + 8 * (t // 2) + 8, :] = packed
        for k in range(tiles):
            low = at_marks + 8 * k + 2 * chans
            built[low : low + 1, :] = jnp.full((1, LANES), active)
            built[low + 1 : low + 2, :] = jnp.full((1, LANES), marked)

        by_odd = top == even_at("group")

        @pl.when(by_odd)
        def _():
            odd_ref[...] = built[...]

        @pl.when(jnp.logical_not(by_odd))
        def _():
            even_ref[...] = built[...]

    lax.fori_loop(0, 2, one_side, 0)


def inside(a_ref, b_ref, x_ref, cover_ref, label_ref, source_ref, once_ref, seam_ref, coarse_ref, da, db, rest):
    chans, rows, cols = a_ref.shape
    tiles = cols // LANES
    active = cover_ref[0, 0].astype(jnp.float32)
    second = label_ref[0, 0] == 1
    for k in range(tiles):
        for buf in (da, db):
            buf[k, 0:8, :] = jnp.zeros((8, LANES), jnp.float32)
            buf[k, rows + 8 : rows + 16, :] = jnp.zeros((8, LANES), jnp.float32)
    scale = [active * NEAR] * tiles
    top, end = HALO, HALO + rows

    def pick(k, low, n):
        return jnp.where(second, db[k, low : low + n, :], da[k, low : low + n, :])

    seam_ref[...] = jnp.zeros(seam_ref.shape, jnp.float32)

    def channel(c, _):
        for k in range(tiles):
            at = pl.ds(k * LANES, LANES)
            for r, n in spans(0, rows):
                x = x_ref[c, r : r + n, at]
                da[k, 8 + r : 8 + r + n, :] = a_ref[c, r : r + n, at] - x
                db[k, 8 + r : 8 + r + n, :] = b_ref[c, r : r + n, at] - x
        for r, n in spans(0, rows):
            parts = [[pick(k, 8 + s + r, n) for k in range(tiles)] for s in (0, -1, 1)]
            found = own_source(*parts, active)
            for k in range(tiles):
                source_ref[c, k, top + r : top + r + n, :] = found[k]
            ids = lane_ids(n)
            base = QUARTER * c
            at = pl.ds(8 + r, n)
            seam = pltpu.roll(found[0], base + LEFT, 1)
            for source, cell, lane in (
                (found[tiles - 1], LANES - SEAM, RIGHT - SEAM),
                (da[0, at, :], 0, LEFT - 1),
                (db[0, at, :], 0, LEFT - 2),
                (da[tiles - 1, at, :], LANES - 1, RIGHT),
                (db[tiles - 1, at, :], LANES - 1, RIGHT + 1),
            ):
                spot = (ids >= base + lane) & (ids < base + lane + (SEAM if cell == LANES - SEAM else 1))
                seam = jnp.where(spot, pltpu.roll(source, base + lane + (LANES - cell) % LANES, 1), seam)
            at = pl.ds(top + r, n)
            mine = (ids >= base + LEFT - 2) & (ids < base + RIGHT + 2)
            mine = mine & ((ids < base + LEFT + SEAM) | (ids >= base + RIGHT - SEAM))
            seam_ref[at, :] = jnp.where(mine, seam, seam_ref[at, :])
        source, once = source_ref.at[c], once_ref.at[c]

        def first(piece, turned):
            r, n = piece
            _, found = swept(source, source, scale, 1, r, n, False, turned)
            for k in range(tiles):
                once_ref[c, k, r : r + n, :] = found[k]

        def second_sweep(piece, turned):
            r, n = piece
            mids, found = swept(once, source, scale, 1, r, n, False, turned)
            for k in range(tiles):
                rest[k, r : r + n, :] = found[k] - mids[k]

        staggered(spans(top, end), lambda piece: turn(source, 1, *piece), first, 0)
        staggered(spans(top, end), lambda piece: turn(once, 1, *piece), second_sweep, 0)
        for r, n in spans(top // 2, end // 2):
            for k in range(tiles):
                coarse_ref[c, k, r : r + n, :] = restricted(rest, k, 2 * r, n, 1)
        return 0

    lax.fori_loop(0, chans, channel, 0)


def seam_units(height):
    for t in range((height - 2 * FIRST) // 8):
        yield FIRST + 8 * t, t // 4, t % 4


def message_rows(chans, height):
    quarter = height // 2
    cells = (chans // 2 * quarter + chans % 2 * quarter // 2) // 2
    return cells, -(-(height - 2 * FIRST) // 32) * 8


def column_rows(chans, height):
    quarter = height // 2
    places = [(c, r, c + 1, r) for c in range(0, chans - 1, 2) for r in range(0, quarter, 8)]
    if chans % 2:
        places += [(chans - 1, r, chans - 1, r + quarter // 2) for r in range(0, quarter // 2, 8)]
    return places


def join_rows(
    source_in, once_in, seam_in, coarse_in, sent_even, sent_odd, got_even, got_odd, cover_ref, label_ref,
    source_ref, once_ref, seam_ref, coarse_ref, even_ref, odd_ref, rest, marks_ref, upper_got, lower_got, lines, left_out, right_out,
):
    chans, tiles, height, _ = source_ref.shape
    rows = height - 2 * HALO
    row_even, col_even = even_at("group"), even_at("blk")
    active = cover_ref[0, 0].astype(jnp.float32)
    marked = label_ref[0, 0].astype(jnp.float32)
    eight = lane_ids(8)

    place = eight & (QUARTER - 1)

    at_coarse, at_seam, at_marks = strip_rows(chans, tiles)

    def take(top, got):
        near = HALO - 8 if top else HALO + rows
        mine = lines[0 if top else 1]
        edge = HALO if top else HALO + rows - 1
        other = edge - 1 if top else edge + 1
        their_active = got[at_marks + 2 * chans : at_marks + 2 * chans + 1, :]
        their_mark = got[at_marks + 2 * chans + 1 : at_marks + 2 * chans + 2, :]
        band = 0 if top else 2
        marks_ref[band : band + 1, :] = their_active
        marks_ref[band + 3 : band + 4, :] = their_mark
        half_halo = HALO // 2
        coarse_at = 0 if top else (height - HALO) // 2
        even_cell = (lane_ids(half_halo) & 1) == 0
        for c in range(chans):
            cells = got[at_coarse + c * half_halo : at_coarse + (c + 1) * half_halo, :]
            at = pl.ds(coarse_at, half_halo)
            coarse_ref[c, 0, at, :] = jnp.where(even_cell, cells, roll(cells, 1))
            coarse_ref[c, 1, at, :] = jnp.where(even_cell, roll(cells, -1), cells)
            for k in range(tiles):
                source_ref[c, k, near : near + 8, :] = got[8 * (tiles * c + k) : 8 * (tiles * c + k) + 8, :]
                low = at_marks + 8 * k + 2 * c
                their_a, their_b = got[low : low + 1, :], got[low + 1 : low + 2, :]
                my_a, my_b = mine[k, 2 * c : 2 * c + 1, :], mine[k, 2 * c + 1 : 2 * c + 2, :]
                for_mine = NEAR * active * jnp.where(marked == 1.0, their_b, their_a)
                for_theirs = NEAR * their_active * jnp.where(their_mark == 1.0, my_b, my_a)
                source_ref[c, k, edge : edge + 1, :] = source_ref[c, k, edge : edge + 1, :] - for_mine
                source_ref[c, k, other : other + 1, :] = source_ref[c, k, other : other + 1, :] - for_theirs

        def seam_of(r, cells):
            for c in range(chans):
                base = QUARTER * c
                spot = (eight >= base + LEFT) & (eight < base + LEFT + SEAM)
                cells = jnp.where(spot, roll(source_ref[c, 0, r : r + 8, :], base + LEFT), cells)
                spot = (eight >= base + RIGHT - SEAM) & (eight < base + RIGHT)
                cells = jnp.where(spot, roll(source_ref[c, tiles - 1, r : r + 8, :], base + RIGHT), cells)
            seam_ref[r : r + 8, :] = cells

        in_left = (place >= LEFT - 2) & (place < LEFT + SEAM)
        in_right = (place >= RIGHT - SEAM) & (place < RIGHT + 2)
        for t in range(STRIP // 8):
            packed = got[at_seam + 8 * (t // 2) : at_seam + 8 * (t // 2) + 8, :]
            slot = 2 * (t & 1)
            firsts = jnp.where(in_left, roll(packed, LEFT - 2 - 8 * slot), 0.0)
            cells = jnp.where(in_right, roll(packed, RIGHT - SEAM - 8 * slot - 8), firsts)
            cells = jnp.where(eight < QUARTER * chans, cells, 0.0)
            r = (FIRST if top else HALO + rows) + 8 * t
            if r == near:
                seam_of(r, cells)
            else:
                seam_ref[r : r + 8, :] = cells
        r = edge // 8 * 8
        seam_of(r, seam_ref[r : r + 8, :])

    def arrange(upper, lower, mine_up, mine_low):
        upper_got[...] = upper[...]
        lower_got[...] = lower[...]
        for k in range(tiles):
            at = pl.ds(at_marks + 8 * k, 8)
            lines[0, k], lines[1, k] = mine_up[at, :], mine_low[at, :]

    @pl.when(row_even)
    def _():
        arrange(got_odd, got_even, sent_odd, sent_even)

    @pl.when(jnp.logical_not(row_even))
    def _():
        arrange(got_even, got_odd, sent_even, sent_odd)

    take(True, upper_got)
    take(False, lower_got)
    marks_ref[1:2, :] = jnp.full((1, LANES), active)
    marks_ref[4:5, :] = jnp.full((1, LANES), marked)
    marks_ref[6:8, :] = jnp.zeros((2, LANES), jnp.float32)

    bottom = HALO + rows
    edges = ((HALO - 8, HALO, 0), (HALO, HALO + RIM, 1), (bottom - RIM, bottom, 1), (bottom, bottom + 8, 2))
    spots = [(c, band, r, n) for c in range(chans) for low, high, band in edges for r, n in spans(low, high)]
    for stage in range(2):
        held = (source_ref, once_ref)[stage]

        def edge_sweep(spot, turned):
            c, band, r, n = spot
            scale = [jnp.broadcast_to(marks_ref[band : band + 1, :] * NEAR, (n, LANES))] * tiles
            mids, found = swept(held.at[c], source_ref.at[c], scale, 1, r, n, False, turned)
            for k in range(tiles):
                if stage == 0:
                    once_ref[c, k, r : r + n, :] = found[k]
                else:
                    rest[c, k, r : r + n, :] = found[k] - mids[k]

        staggered(spots, lambda spot: turn(held.at[spot[0]], 1, *spot[2:]), edge_sweep, 0)
    for c in range(chans):
        for low, high in ((HALO - 4, HALO + RIM), (bottom - RIM, bottom + 4)):
            for k in range(tiles):
                coarse_ref[c, k, low // 2 : high // 2, :] = restricted(rest.at[c], k, low, (high - low) // 2, 1)

    cells, units = message_rows(chans, height)
    first_half = eight < HALF
    even_lane = (eight & 1) == 0

    def edge_cells(c, r):
        return jnp.where(first_half, coarse_ref[c, 0, r : r + 8, :], coarse_ref[c, tiles - 1, r : r + 8, :])

    def joined(place):
        c, r, d, s = place
        return jnp.where(even_lane, edge_cells(c, r), edge_cells(d, s))

    def pack(left, right):
        places = column_rows(chans, height)
        for t in range(cells // 8):
            upper, lower = joined(places[t]), joined(places[t + cells // 8])
            left[8 * t : 8 * t + 8, :] = jnp.where(first_half, upper, roll(lower, HALF))
            right[8 * t : 8 * t + 8, :] = jnp.where(first_half, roll(upper, HALF), lower)
        lefts = rights = jnp.zeros((8, LANES), jnp.float32)
        for r, tile, slot in seam_units(height):
            value = seam_ref[r : r + 8, :]
            spot = (place >> 3) == slot
            lefts = jnp.where(spot, roll(value, 8 * slot - (LEFT - 2)), lefts)
            rights = jnp.where(spot, roll(value, 8 * slot - (RIGHT - SEAM)), rights)
            at = cells + 8 * tile
            left[at : at + 8, :], right[at : at + 8, :] = lefts, rights
        for out in (left, right):
            out[cells : cells + 8, :] = jnp.where(eight < LANES - QUARTER, out[cells : cells + 8, :], marks_ref[...])

    pack(left_out, right_out)

    @pl.when(col_even)
    def _():
        odd_ref[...] = left_out[...]
        even_ref[...] = right_out[...]

    @pl.when(jnp.logical_not(col_even))
    def _():
        even_ref[...] = left_out[...]
        odd_ref[...] = right_out[...]


def cycle(
    source_in, once_in, seam_in, coarse_in, sent_even, got_even, got_odd, x_ref, out_hbm,
    out_ref, sems, right_ref, left_ref, seam_source, seam_once, seam_rest, fine, fine_two, fix, *bufs,
):
    chans, own_tiles, height, _ = source_in.shape
    rows = height - 2 * HALO
    tiles = own_tiles + 1
    cells, units = message_rows(chans, height)
    col_even = even_at("blk")
    eight = lane_ids(8)

    @pl.when(col_even)
    def _():
        right_ref[...] = got_even[...]
        left_ref[...] = got_odd[...]

    @pl.when(jnp.logical_not(col_even))
    def _():
        right_ref[...] = got_odd[...]
        left_ref[...] = got_even[...]

    def mark(ref, row):
        cell = ref[cells + row : cells + row + 1, LANES - 1 : LANES]
        return jnp.broadcast_to(cell, (8, LANES))

    own = [mark(sent_even, i) for i in range(6)]
    right = [mark(right_ref, i) for i in range(6)]
    left = [mark(left_ref, i) for i in range(6)]
    first_half = eight < HALF
    place = eight & (QUARTER - 1)

    def mixed(i):
        return jnp.where(place < LEFT, left[i], jnp.where(place < RIGHT, own[i], right[i]))

    seam_scale = [jnp.where(eight < QUARTER * chans, mixed(i), 0.0) * NEAR for i in range(3)]
    seam_mark = [mixed(i + 3) == 1.0 for i in range(3)]
    own_scale = [own[i] * NEAR for i in range(3)]
    side_scale = [jnp.where(first_half, right[i], left[i]) * NEAR for i in range(3)]

    def wide(mask, n):
        return jnp.broadcast_to(mask[:1], (n, LANES))

    def over_rows(kinds, depth, r, n):
        full, halo = height >> depth, HALO >> depth
        ends = ((0, halo), (halo, full - halo), (full - halo, full))
        parts = [(max(a, r), min(b, r + n), kind) for (a, b), kind in zip(ends, kinds)]
        parts = [wide(kind, b - a) for a, b, kind in parts if b > a]
        return parts[0] if len(parts) == 1 else jnp.concatenate(parts, axis=0)

    def scales(depth, r, n):
        return [over_rows(own_scale, depth, r, n)] * own_tiles + [over_rows(side_scale, depth, r, n)]

    inner = ((place >= LEFT) & (place < LEFT + SEAM)) | ((place >= RIGHT - SEAM) & (place < RIGHT))
    outer = ((place >= LEFT - SEAM) & (place < LEFT)) | ((place >= RIGHT) & (place < RIGHT + SEAM))
    from_near = (place == LEFT) | (place == RIGHT - 1)
    from_own = (place == LEFT - 1) | (place == RIGHT)
    up_one = (place == LEFT - 1) | (place == RIGHT - 1)
    near_b = (place == LEFT + 1) | (place == RIGHT - 2)
    right_unit = place >= RIGHT - 2

    def unpack(unit):
        r, tile, slot = unit
        rights = roll(right_ref[cells + 8 * tile : cells + 8 * tile + 8, :], RIGHT - 2 - 8 * slot)
        lefts = roll(left_ref[cells + 8 * tile : cells + 8 * tile + 8, :], LEFT - SEAM - 8 * slot)
        return rights, lefts

    def keep_near(unit, turned):
        r = unit[0]
        seam_rest[0, r : r + 8, :] = jnp.where(right_unit, *turned)

    def second_cells(unit):
        r = unit[0]
        cells_b = jnp.where(near_b, seam_rest[0, r : r + 8, :], seam_in[r : r + 8, :])
        return roll(cells_b, 1), roll(cells_b, -1)

    def put_seam(unit, turned):
        r = unit[0]
        band = 0 if r < HALO else 1 if r < HALO + rows else 2
        near, mine = seam_rest[0, r : r + 8, :], seam_in[r : r + 8, :]
        value = jnp.where(inner, mine, jnp.where(outer, near, 0.0))
        border = jnp.where(seam_mark[band], jnp.where(up_one, *turned), jnp.where(from_near, near, mine))
        border = jnp.where(from_near | from_own, border, 0.0)
        seam_source[0, r : r + 8, :] = value - seam_scale[band] * border

    staggered(seam_units(height), unpack, keep_near, 24)
    staggered(seam_units(height), second_cells, put_seam, 24)
    for r, n in spans(FIRST, height - FIRST, height):
        _, found = swept(
            seam_source, seam_source, [over_rows(seam_scale, 0, r, n)], 1, r, n, True, turn(seam_source, 1, r, n)
        )
        seam_once[0, r : r + n, :] = found[0]
        mids, found = swept(
            seam_once, seam_source, [over_rows(seam_scale, 0, r, n)], 1, r, n, True, turn(seam_once, 1, r, n)
        )
        seam_rest[0, r : r + n, :] = found[0] - mids[0]

    one_src, one_once, one_two = bufs[0:3]
    half_rows = height // 2
    eights = lane_ids(8)
    even_lane = (eights & 1) == 0
    places = column_rows(chans, height)
    for t, (c, r, d, s) in enumerate(places):
        low, upper = (8 * t, True) if t < cells // 8 else (8 * t - cells, False)
        from_right, from_left = right_ref[low : low + 8, :], left_ref[low : low + 8, :]
        if upper:
            value = jnp.where(first_half, from_right, roll(from_left, HALF))
        else:
            value = jnp.where(first_half, roll(from_right, HALF), from_left)
        if c == d:
            one_src[c // 2, own_tiles, 8 + r : 16 + r, :] = jnp.where(even_lane, value, roll(value, 1))
            one_src[c // 2, own_tiles, 8 + s : 16 + s, :] = jnp.where(even_lane, roll(value, -1), value)
        else:
            one_src[c // 2, own_tiles, 8 + r : 16 + r, :] = value

    pairs = [(c, min(c + 1, chans - 1)) for c in range(0, chans, 2)]

    def paired(of, pair, n):
        first, second = pair
        return of(first) if first == second else jnp.where((lane_ids(n) & 1) == 0, of(first), of(second))

    for f, pair in enumerate(pairs):
        for r, n in spans(0, half_rows):
            for k in range(own_tiles):
                one_src[f, k, 8 + r : 8 + r + n, :] = paired(lambda c: coarse_in[c, k, r : r + n, :], pair, n)
    for r, n in spans(FIRST // 2, half_rows - FIRST // 2):
        ids = lane_ids(n)
        seam = restricted(seam_rest, 0, 2 * r, n, 1)
        at = pl.ds(8 + r, n)
        for f, pair in enumerate(pairs):
            by_left = paired(lambda c: roll(seam, -QUARTER * c - LEFT), pair, n)
            by_right = paired(lambda c: roll(seam, -QUARTER * c - RIGHT), pair, n)
            one_src[f, 0, at, :] = jnp.where(ids < 4, by_left, one_src[f, 0, at, :])
            inner_end = one_src[f, own_tiles - 1, at, :]
            one_src[f, own_tiles - 1, at, :] = jnp.where(ids >= LANES - 4, by_right, inner_end)
            side = jnp.where(ids < 4, by_right, one_src[f, own_tiles, at, :])
            one_src[f, own_tiles, at, :] = jnp.where(ids >= LANES - 4, by_left, side)

    def smooth(src, once, fields, depth, into, minus=False):
        def one_sweep(spot, turned):
            f, r, n = spot
            mids, found = swept(once.at[f], src.at[f], scales(depth, r, n), 1 << depth, 8 + r, n, True, turned)
            for k in range(tiles):
                into[f, k, 8 + r : 8 + r + n, :] = found[k] - mids[k] if minus else found[k]

        spots = [(f, r, n) for f in range(fields) for r, n in spans(0, height >> depth)]
        staggered(spots, lambda spot: turn(once.at[spot[0]], 1 << depth, 8 + spot[1], spot[2]), one_sweep, 0)

    def expand(fix, fields, depth, out, low, high, spread):
        for f in range(fields):
            for r, n in spans(low, high):
                scale = scales(depth + 1, r, n)
                for k in range(tiles):
                    value = fix[0 if spread else f, k, 8 + r : 8 + r + n, :]
                    if spread:
                        value = spread(value, f)
                    value = value * (scale[k] * (1.0 / NEAR))
                    out[f, k, pl.ds(8 + 2 * r, n, stride=2), :] = value
                    out[f, k, pl.ds(9 + 2 * r, n, stride=2), :] = value

    def add_fix(once, two, fields, depth, into):
        for f in range(fields):
            for r, n in spans(0, height >> depth):
                for k in range(tiles):
                    at = pl.ds(8 + r, n)
                    into[f, k, at, :] = once[f, k, at, :] + two[f, k, at, :]

    assert chans <= 4 and LEVELS >= 3

    def spread_pair(value, f):
        high = (lane_ids(value.shape[0]) & 2) == 2
        return jnp.where(high, value, roll(value, -2)) if f else jnp.where(high, roll(value, 2), value)

    def level(depth):
        src, once, two = bufs[3 * (depth - 1) : 3 * depth]
        fields = len(pairs) if depth == 1 else 1
        if depth == LEVELS - 1:
            held = src
            for sweep in range(1, COARSE):
                into = (once, two)[sweep % 2]
                smooth(src, held, fields, depth, into)
                held = into
            return held
        smooth(src, src, fields, depth, once)
        smooth(src, once, fields, depth, two, True)
        below = bufs[3 * depth]
        shift = 1 << depth
        for r, n in spans(0, height >> (depth + 1)):
            half = (lane_ids(n) & 2) >> 1
            for k in range(tiles):
                value = None
                for f in range(fields):
                    total = restricted(two.at[f], k, 8 + 2 * r, n, shift)
                    value = total if value is None else jnp.where(half == f, total, value)
                below[0, k, 8 + r : 8 + r + n, :] = value
        fix = level(depth + 1)
        expand(fix, fields, depth, two, 0, height >> (depth + 1), spread_pair if depth == 1 else None)
        add_fix(once, two, fields, depth, once)
        smooth(src, once, fields, depth, two)
        smooth(src, two, fields, depth, once)
        return once

    paired_fix = level(1)
    low, high = HALO - RIM, HALO + rows + RIM
    for f, (even, odd) in enumerate(pairs):
        for r, n in spans(low // 2, high // 2):
            at = pl.ds(8 + r, n)
            odd_lane = (lane_ids(n) & 1) == 1
            for k in range(tiles):
                value = paired_fix[f, k, at, :]
                if even == odd:
                    fix[even, k, at, :] = value
                else:
                    fix[even, k, at, :] = jnp.where(odd_lane, roll(value, 1), value)
                    fix[odd, k, at, :] = jnp.where(odd_lane, value, roll(value, -1))

    def at_borders(seam, c):
        base = QUARTER * c
        return pltpu.roll(seam, LANES - LEFT - base, 1), pltpu.roll(seam, LANES - RIGHT - base, 1)

    def fine_source(c):
        def tile(k, r, n):
            ids = lane_ids(n)
            by_left, by_right = at_borders(seam_source[0, r : r + n, :], c)
            if k == own_tiles:
                return jnp.where(ids < HALF, by_right, by_left)
            value = source_in[c, k, r : r + n, :]
            if k == 0:
                value = jnp.where(ids == 0, by_left, value)
            if k == own_tiles - 1:
                value = jnp.where(ids == LANES - 1, by_right, value)
            return value

        return tile

    for c in range(chans):
        for r, n in spans(low // 2, high // 2):
            scale = scales(1, r, n)
            for k in range(tiles):
                value = fix[c, k, 8 + r : 8 + r + n, :] * (scale[k] * (1.0 / NEAR))
                fine[c, k, pl.ds(8 + 2 * r, n, stride=2), :] = value
                fine[c, k, pl.ds(9 + 2 * r, n, stride=2), :] = value
    for c in range(chans):
        for r, n in spans(low, high):
            ids = lane_ids(n)
            by_left, by_right = at_borders(seam_once[0, r : r + n, :], c)
            at = pl.ds(8 + r, n)
            for k in range(own_tiles):
                value = once_in[c, k, r : r + n, :]
                if k == 0:
                    value = jnp.where(ids < 2, by_left, value)
                if k == own_tiles - 1:
                    value = jnp.where(ids >= LANES - 2, by_right, value)
                fine[c, k, at, :] = fine[c, k, at, :] + value
            fine[c, own_tiles, at, :] = fine[c, own_tiles, at, :] + jnp.where(ids < HALF, by_right, by_left)
    for c in range(chans):
        add, src = fine_source(c), fine.at[c]
        for r, n in spans(low, high):
            _, found = swept(src, add, scales(0, r, n), 1, 8 + r, n, True, turn(src, 1, 8 + r, n))
            for k in range(tiles):
                fine_two[c, k, 8 + r : 8 + r + n, :] = found[k]

    def leave(c):
        return pltpu.make_async_copy(out_ref.at[c], out_hbm.at[c], sems.at[c])

    for c in range(chans):
        add, src = fine_source(c), fine_two.at[c]
        for r, n in spans(HALO, HALO + rows):
            _, found = swept(src, add, scales(0, r, n), 1, 8 + r, n, True, turn(src, 1, 8 + r, n), own_tiles)
            for k in range(own_tiles):
                at = pl.ds(k * LANES, LANES)
                out_ref[c, r - HALO : r - HALO + n, at] = x_ref[c, r - HALO : r - HALO + n, at] + found[k]
        leave(c).start()
    for c in range(chans):
        leave(c).wait()


def swaps(count, odd):
    pairs = [(i, i + 1) for i in range(odd, count - 1, 2)]
    return pairs + [(j, i) for i, j in pairs]


def shards(image_a, image_b, initial, coverage, seam_label):
    chans, rows, cols = image_a.shape
    tiles = cols // LANES
    height = rows + 2 * HALO
    vmem = pl.BlockSpec(memory_space=pltpu.VMEM)
    smem = pl.BlockSpec(memory_space=pltpu.SMEM)
    hbm = pl.BlockSpec(memory_space=pltpu.HBM)
    f32 = jnp.float32
    sds = functools.partial(jax.ShapeDtypeStruct, dtype=f32)
    params = pltpu.CompilerParams(vmem_limit_bytes=40 * 1024 * 1024)
    group, blk = lax.axis_size("group"), lax.axis_size("blk")
    central = sds((chans, tiles, height, LANES))
    assert chans <= 3
    column = sds((height, LANES))
    coarse = sds((chans, tiles, height // 2, LANES))
    upright = sds((strip_rows(chans, tiles)[2] + 8 * tiles, LANES))
    beside = sds((sum(message_rows(chans, height)), LANES))

    sent_even, sent_odd = pl.pallas_call(
        strips,
        out_shape=(upright, upright),
        in_specs=[hbm, hbm, hbm, smem, smem],
        out_specs=(vmem, vmem),
        scratch_shapes=[pltpu.VMEM((2, chans, HALO, cols), f32)] * 3
        + [pltpu.VMEM((chans, tiles, HALO + 16, LANES), f32)]
        + [pltpu.VMEM((chans, tiles, HALO, LANES), f32)] * 2
        + [pltpu.VMEM((chans, tiles, HALO + 16, LANES), f32)] * 3
        + [pltpu.VMEM(upright.shape, f32), pltpu.SemaphoreType.DMA((3, 2))],
        compiler_params=pltpu.CompilerParams(vmem_limit_bytes=56_000_000),
        name="strips",
    )(image_a, image_b, initial, coverage, seam_label)
    got_even = lax.ppermute(sent_even, "group", swaps(group, 0))
    got_odd = lax.ppermute(sent_odd, "group", swaps(group, 1))

    source, once, seam, coarser = pl.pallas_call(
        inside,
        out_shape=(central, central, column, coarse),
        in_specs=[vmem, vmem, vmem, smem, smem],
        out_specs=(vmem,) * 4,
        scratch_shapes=[pltpu.VMEM((tiles, rows + 16, LANES), f32)] * 2 + [pltpu.VMEM((tiles, height, LANES), f32)],
        compiler_params=params,
        cost_estimate=pl.CostEstimate(flops=200_000_000, bytes_accessed=4_000_000, transcendentals=0),
        name="inside",
    )(image_a, image_b, initial, coverage, seam_label)

    source, once, seam, coarser, sent_even, sent_odd = pl.pallas_call(
        join_rows,
        out_shape=(central, central, column, coarse, beside, beside),
        in_specs=[vmem] * 8 + [smem] * 2,
        out_specs=(vmem,) * 6,
        input_output_aliases={0: 0, 1: 1, 2: 2, 3: 3},
        scratch_shapes=[pltpu.VMEM(central.shape, f32), pltpu.VMEM((8, LANES), f32)]
        + [pltpu.VMEM(upright.shape, f32)] * 2
        + [pltpu.VMEM((2, tiles, 8, LANES), f32)]
        + [pltpu.VMEM(beside.shape, f32)] * 2,
        compiler_params=params,
        name="join_rows",
    )(source, once, seam, coarser, sent_even, sent_odd, got_even, got_odd, coverage, seam_label)
    got_even = lax.ppermute(sent_even, "blk", swaps(blk, 0))
    got_odd = lax.ppermute(sent_odd, "blk", swaps(blk, 1))

    scratch = [pltpu.VMEM(image_a.shape, f32), pltpu.SemaphoreType.DMA((chans,))]
    scratch += [pltpu.VMEM(beside.shape, f32)] * 2 + [pltpu.VMEM((1, height, LANES), f32)] * 3
    scratch += [pltpu.VMEM((chans, tiles + 1, height + 16, LANES), f32)] * 2
    scratch += [pltpu.VMEM((chans, tiles + 1, height // 2 + 16, LANES), f32)]
    for depth in range(1, LEVELS):
        fields = (chans + 1) // 2 if depth == 1 else 1
        scratch += [pltpu.VMEM((fields, tiles + 1, (height >> depth) + 16, LANES), f32)] * 3
    return pl.pallas_call(
        cycle,
        out_shape=sds((chans, rows, cols)),
        in_specs=[vmem] * 8,
        out_specs=hbm,
        scratch_shapes=scratch,
        compiler_params=params,
        name="cycle",
    )(source, once, seam, coarser, sent_even, got_even, got_odd, initial)


def solution(mesh):
    placed = (
        P(None, "group", "blk"),
        P(None, "group", "blk"),
        P(None, "group", "blk"),
        P("group", "blk"),
        P("group", "blk"),
    )
    return jax.shard_map(
        shards, mesh=mesh, in_specs=placed, out_specs=P(None, "group", "blk"), check_vma=False
    )
```
